32 devices in a mesh: rows: 8 (over z, y), pairs: 4 (over x, core).
Axes of the slice: x: 2, y: 2, z: 4, core: 2. Of those that a mesh axis runs over, the one named last changes fastest.
Arguments:
- matrix: float32 [16384, 2048], P('rows', 'pairs'), may hold values from -40 to 40
Outputs:
- rotated: float32 [16384, 2048], P('rows', 'pairs')
The draws below stay inside these ranges and needn't reach their ends.
All inputs are finite; a program needn't handle non-finite values.
Results may differ from the reference program's by a relative error of at most 0.0001.
Values sent between devices are 32-bit elements; how exact they have to be, the bound alone decides.
A program may use at most 64 MiB of HBM per device.

```python
import jax
import jax.numpy as jnp
from jax import lax

B = 256
STEPS = 2
PAIRS = 4
ROWS = 16384
COLS = 2048


def draw_matrix(key, part):
    keys = jax.random.split(jax.random.fold_in(key, 17), 4)
    independent = jax.random.normal(keys[0], (ROWS, COLS), jnp.float32)
    shared_scale = 0.05
    factors = jax.random.normal(keys[1], (ROWS, 64), jnp.float32)
    loadings = jax.random.normal(keys[2], (64, COLS), jnp.float32) * shared_scale
    shared = jnp.dot(factors, loadings, preferred_element_type=jnp.float32)
    col_scale = jnp.exp(jax.random.uniform(keys[3], (1, COLS), jnp.float32, jnp.log(0.3), jnp.log(3.0)))
    values = (independent + shared) * col_scale
    return jnp.clip(values, -40.0, 40.0).astype(jnp.float32)


def setup_inputs(seed: int = 0) -> dict:
    key_list = jax.random.split(jax.random.key(seed), 2)
    matrix = draw_matrix(jax.random.fold_in(key_list[1], 71), 0)
    return dict(matrix=matrix)


def spd_solve(system, right_side):
    factor = jnp.linalg.cholesky(system)
    middle = lax.linalg.triangular_solve(factor, right_side, left_side=True, lower=True)
    return lax.linalg.triangular_solve(factor, middle, left_side=True, lower=True, transpose_a=True)

def cayley_rotation(cross_block, norms_first, norms_second, rows_all):
    precise = lax.Precision.HIGHEST
    block_cols = cross_block.shape[0]
    scale_first = lax.rsqrt(norms_first / rows_all + 1e-06)
    scale_second = lax.rsqrt(norms_second / rows_all + 1e-06)
    coupling = 0.5 * cross_block * scale_first[:, None] * scale_second[None, :] / rows_all
    identity = jnp.eye(block_cols, dtype=jnp.float32)
    first_system = identity + jnp.dot(coupling.astype(jnp.float32), coupling.T.astype(jnp.float32), precision=precise, preferred_element_type=jnp.float32)
    first_sol = spd_solve(first_system, jnp.concatenate([identity, coupling], axis=1))
    lower_sol = jnp.dot(coupling.T.astype(jnp.float32), first_sol.astype(jnp.float32), precision=precise, preferred_element_type=jnp.float32)
    upper_rows = jnp.concatenate([2.0 * first_sol[:, :block_cols] - identity, 2.0 * first_sol[:, block_cols:]], axis=1)
    lower_rows = jnp.concatenate([-2.0 * lower_sol[:, :block_cols], identity - 2.0 * lower_sol[:, block_cols:]], axis=1)
    return jnp.concatenate([upper_rows, lower_rows], axis=0)

def reference(matrix):
    precise = lax.Precision.HIGHEST
    grouped = matrix.reshape(ROWS, PAIRS, 2, B)
    first_blocks = jnp.transpose(grouped[:, :, 0, :], (1, 0, 2))
    second_blocks = jnp.transpose(grouped[:, :, 1, :], (1, 0, 2))

    def turn_pair(pair_blocks):
        both = jnp.concatenate([pair_blocks[0], pair_blocks[1]], axis=1)
        gram_pair = lax.dot_general(both.astype(jnp.float32), both.astype(jnp.float32), (((0,), (0,)), ((), ())), precision=precise, preferred_element_type=jnp.float32)
        diag_all = jnp.diagonal(gram_pair)
        rotate = cayley_rotation(gram_pair[:B, B:], diag_all[:B], diag_all[B:], ROWS)
        turned = jnp.dot(both.astype(jnp.float32), rotate.astype(jnp.float32), precision=precise, preferred_element_type=jnp.float32)
        return (turned[:, :B], turned[:, B:])
    for turn_index in range(STEPS):
        first_blocks, second_blocks = lax.map(turn_pair, (first_blocks, second_blocks))
        next_first = jnp.concatenate([first_blocks[:1], second_blocks[:1], first_blocks[1:-1]], axis=0)
        second_blocks = jnp.concatenate([second_blocks[1:], first_blocks[-1:]], axis=0)
        first_blocks = next_first
    stacked = jnp.stack([first_blocks, second_blocks], axis=2)
    return jnp.transpose(stacked, (1, 0, 2, 3)).reshape(ROWS, COLS)
```

```python
import functools

import jax
import jax.numpy as jnp
from jax import lax
from jax.experimental import pallas as pl
from jax.experimental.pallas import tpu as pltpu
from jax.sharding import PartitionSpec as P

CHUNKS = 8
EARLY = 4
F32 = jnp.float32
BF16 = jnp.bfloat16
MESH = pl.DeviceIdType.MESH
DMA = pltpu.SemaphoreType.DMA


def split(value):
    high = value.astype(BF16)
    return high, (value - high.astype(F32)).astype(BF16)


def dot_bf16(left, right, left_dim):
    return lax.dot_general(
        left, right, (((left_dim,), (0,)), ((), ())), preferred_element_type=F32
    )


def dot_three(left, right, left_dim):
    return (
        dot_bf16(left[0], right[1], left_dim)
        + dot_bf16(left[1], right[0], left_dim)
        + dot_bf16(left[0], right[0], left_dim)
    )


def exact_dot(left, right, left_dim=1, right_dim=0):
    return lax.dot_general(
        left,
        right,
        (((left_dim,), (right_dim,)), ((), ())),
        precision=lax.Precision.HIGHEST,
        preferred_element_type=F32,
    )


def rows_copy(src, dst, send, recv, peer):
    return pltpu.make_async_remote_copy(
        src_ref=src,
        dst_ref=dst,
        send_sem=send,
        recv_sem=recv,
        device_id={"rows": peer},
        device_id_type=MESH,
    )


def pairs_copy(src, dst, send, recv, peer):
    return pltpu.make_async_remote_copy(
        src_ref=src,
        dst_ref=dst,
        send_sem=send,
        recv_sem=recv,
        device_id={"pairs": peer},
        device_id_type=MESH,
    )


def greet(barrier, axis, peer):
    pl.semaphore_signal(barrier, inc=1, device_id={axis: peer}, device_id_type=MESH)


def partners(position, length):
    even = position % 2 == 0
    down = jnp.where(position == 0, 1, position - 2)
    up = jnp.where(position == length - 1, length - 2, position + 2)
    lead = jnp.where(even, down, up)
    down = jnp.where(position == 1, 0, position - 2)
    up = jnp.where(position == length - 2, length - 1, position + 2)
    keep = jnp.where(even, up, down)
    return lead, keep


def pack(count, cross, norms, part):
    block = cross.shape[0]
    share = block // count
    half = block // 2
    for slot in range(count):
        part[slot, :share, :] = cross[slot * share : (slot + 1) * share, :half]
        part[slot, share : 2 * share, :] = cross[slot * share : (slot + 1) * share, half:]
        part[slot, 2 * share : 2 * share + 8, :] = norms[:, :half]
        part[slot, 2 * share + 8 : 2 * share + 16, :] = norms[:, half:]


def unpack(total, cross):
    count, depth, half = total.shape
    share = (depth - 16) // 2
    for slot in range(count):
        cross[slot * share : (slot + 1) * share, :half] = total[slot, :share, :]
        cross[slot * share : (slot + 1) * share, half:] = total[slot, share : 2 * share, :]
    return jnp.concatenate(
        [total[0, 2 * share : 2 * share + 8, :], total[0, 2 * share + 8 :, :]], axis=1
    )


def scatter_sum(count, part, recv, mine, send_sems, recv_sems):
    me = lax.axis_index("rows")
    copies = []
    for far in range(1, count):
        peer = lax.rem(me + far, count)
        copy = rows_copy(part.at[peer], recv.at[far], send_sems.at[far], recv_sems.at[far], peer)
        copy.start()
        copies.append(copy)
    acc = part[me]
    for far in range(1, count):
        copies[far - 1].wait_recv()
        acc = acc + recv[far]
    mine[...] = acc
    return copies


def gather_start(count, mine, gathered, send_sems, recv_sems):
    me = lax.axis_index("rows")
    copies = []
    for far in range(1, count):
        peer = lax.rem(me + far, count)
        copy = rows_copy(mine, gathered.at[far], send_sems.at[far], recv_sems.at[far], peer)
        copy.start()
        copies.append(copy)
    return copies


def gather_finish(count, mine, gathered, total, copies):
    me = lax.axis_index("rows")
    total[me] = mine[...]
    for far in range(1, count):
        copies[far - 1].wait_recv()
        total[lax.rem(me + count - far, count)] = gathered[far]


def products_kernel(count, matrix, total, loaded, load_sem, cross, norms, part, recv, mine, gathered, *sems):
    rows, cols = loaded.shape
    block = cols // 2
    step = rows // CHUNKS

    def at(chunk):
        return pl.ds(pl.multiple_of(chunk * step, step), step)

    def load(chunk):
        return pltpu.make_async_copy(
            matrix.at[at(chunk)], loaded.at[at(chunk)], load_sem.at[chunk]
        )

    for chunk in range(CHUNKS):
        load(chunk).start()
    barrier = pltpu.get_barrier_semaphore()
    me = lax.axis_index("rows")
    for far in range(1, count):
        greet(barrier, "rows", lax.rem(me + far, count))
    cross[...] = jnp.zeros_like(cross)
    norms[...] = jnp.zeros_like(norms)

    def take(chunk, carry):
        load(chunk).wait()
        first, second = loaded[at(chunk), :block], loaded[at(chunk), block:]
        cross[...] += dot_three(split(first), split(second), 0)
        norms[0:1, :] += jnp.sum(first * first, axis=0, keepdims=True)
        norms[1:2, :] += jnp.sum(second * second, axis=0, keepdims=True)
        return carry

    lax.fori_loop(0, CHUNKS, take, 0)
    pack(count, cross, norms, part)
    pl.semaphore_wait(barrier, count - 1)
    copies = scatter_sum(count, part, recv, mine, sems[0], sems[1])
    more = gather_start(count, mine, gathered, sems[2], sems[3])
    gather_finish(count, mine, gathered, total, more)
    for copy in copies + more:
        copy.wait_send()


def products(matrix):
    rows, cols = matrix.shape
    block = cols // 2
    count = lax.axis_size("rows")
    slot = (2 * (block // count) + 16, block // 2)
    return pl.pallas_call(
        functools.partial(products_kernel, count),
        out_shape=jax.ShapeDtypeStruct((count,) + slot, F32),
        in_specs=[pl.BlockSpec(memory_space=pl.ANY)],
        out_specs=pl.BlockSpec(memory_space=pltpu.VMEM),
        scratch_shapes=[
            pltpu.VMEM((rows, cols), F32),
            DMA((CHUNKS,)),
            pltpu.VMEM((block, block), F32),
            pltpu.VMEM((8, block), F32),
            pltpu.VMEM((count,) + slot, F32),
            pltpu.VMEM((count,) + slot, F32),
            pltpu.VMEM(slot, F32),
            pltpu.VMEM((count,) + slot, F32),
        ]
        + [DMA((count,))] * 4,
        name="products",
        compiler_params=pltpu.CompilerParams(
            collective_id=0, has_side_effects=True, vmem_limit_bytes=24 * 2**20
        ),
    )(matrix)


def exchange_kernel(
    count, length, matrix, rot_high, rot_low,
    lead, keep, lead_land, keep_land, total_keep, total_lead,
    loaded, cross, norms, part, recv, mine, gathered, passed, gathered_lead,
    load_sem, lead_send, lead_recv, keep_send, keep_recv,
    sum_send, sum_recv, all_send, all_recv, pass_send, pass_recv, more_send, more_recv, go_sem,
):
    rows, cols = loaded.shape
    block = cols // 2
    step = rows // CHUNKS
    me = lax.axis_index("rows")
    position = lax.axis_index("pairs")
    lead_peer, keep_peer = partners(position, length)
    core_peer = position + 1 - 2 * (position % 2)
    near = keep_peer == core_peer
    left_leads = jnp.logical_or(position % 2 == 1, position == 0)
    signals = jnp.logical_and(position > 0, position < length - 1)

    def at(chunk):
        return pl.ds(pl.multiple_of(chunk * step, step), step)

    def load(chunk):
        return pltpu.make_async_copy(
            matrix.at[at(chunk)], loaded.at[at(chunk)], load_sem.at[chunk]
        )

    def send_lead(chunk):
        return pairs_copy(
            lead.at[at(chunk)], keep_land.at[at(chunk)],
            lead_send.at[chunk], lead_recv.at[chunk], lead_peer,
        )

    def send_keep(chunk):
        return pairs_copy(
            keep.at[at(chunk)], lead_land.at[at(chunk)],
            keep_send.at[chunk], keep_recv.at[chunk], keep_peer,
        )

    def loop(low, high, do):
        def body(chunk, carry):
            do(chunk)
            return carry

        lax.fori_loop(low, high, body, 0)

    for chunk in range(CHUNKS):
        load(chunk).start()
    barrier = pltpu.get_barrier_semaphore()
    for far in range(1, count):
        greet(barrier, "rows", lax.rem(me + far, count))
    for peer in (lead_peer, keep_peer, core_peer):
        greet(barrier, "pairs", peer)
    pl.semaphore_wait(barrier, count + 2)

    def turn(chunk):
        load(chunk).wait()
        turned = dot_three(split(loaded[at(chunk), :]), (rot_high[...], rot_low[...]), 1)
        left, right = turned[:, :block], turned[:, block:]
        lead[at(chunk), :] = jnp.where(left_leads, left, right)
        keep[at(chunk), :] = jnp.where(left_leads, right, left)
        send_lead(chunk).start()

        @pl.when(near)
        def _():
            send_keep(chunk).start()

    loop(0, CHUNKS, turn)
    cross[...] = jnp.zeros_like(cross)
    norms[...] = jnp.zeros_like(norms)

    def take(chunk):
        send_lead(chunk).wait_recv()
        mine_rows, theirs = keep[at(chunk), :], keep_land[at(chunk), :]
        cross[...] += dot_three(split(mine_rows), split(theirs), 0)
        norms[0:1, :] += jnp.sum(mine_rows * mine_rows, axis=0, keepdims=True)
        norms[1:2, :] += jnp.sum(theirs * theirs, axis=0, keepdims=True)

    def hand_over():
        loop(0, CHUNKS - 1, lambda chunk: send_lead(chunk).wait_send())

        @pl.when(signals)
        def _():
            pl.semaphore_signal(
                go_sem, inc=1, device_id={"pairs": core_peer}, device_id_type=MESH
            )

    loop(0, CHUNKS - 1, take)

    @pl.when(jnp.logical_not(near))
    def _():
        hand_over()
        pl.semaphore_wait(go_sem, 1)
        loop(0, EARLY, lambda chunk: send_keep(chunk).start())

    take(CHUNKS - 1)
    pack(count, cross, norms, part)
    copies = scatter_sum(count, part, recv, mine, sum_send, sum_recv)
    piece = pairs_copy(mine, passed, pass_send, pass_recv, keep_peer)
    piece.start()
    more = gather_start(count, mine, gathered, all_send, all_recv)

    @pl.when(jnp.logical_not(near))
    def _():
        loop(EARLY, CHUNKS, lambda chunk: send_keep(chunk).start())

    gather_finish(count, mine, gathered, total_keep, more)

    @pl.when(near)
    def _():
        hand_over()

    piece.wait_recv()
    rest = gather_start(count, passed, gathered_lead, more_send, more_recv)
    gather_finish(count, passed, gathered_lead, total_lead, rest)
    for copy in copies + more + rest + [piece]:
        copy.wait_send()
    send_lead(CHUNKS - 1).wait_send()
    loop(0, CHUNKS, lambda chunk: send_keep(chunk).wait())


def exchange(matrix, rotation, slot):
    rows, cols = matrix.shape
    block = cols // 2
    count = lax.axis_size("rows")
    length = lax.axis_size("pairs")
    vmem = pl.BlockSpec(memory_space=pltpu.VMEM)
    pieces = (count,) + slot
    return pl.pallas_call(
        functools.partial(exchange_kernel, count, length),
        out_shape=[jax.ShapeDtypeStruct((rows, block), F32)] * 4
        + [jax.ShapeDtypeStruct(pieces, F32)] * 2,
        in_specs=[pl.BlockSpec(memory_space=pl.ANY), vmem, vmem],
        out_specs=[vmem] * 6,
        scratch_shapes=[
            pltpu.VMEM((rows, cols), F32),
            pltpu.VMEM((block, block), F32),
            pltpu.VMEM((8, block), F32),
            pltpu.VMEM(pieces, F32),
            pltpu.VMEM(pieces, F32),
            pltpu.VMEM(slot, F32),
            pltpu.VMEM(pieces, F32),
            pltpu.VMEM(slot, F32),
            pltpu.VMEM(pieces, F32),
        ]
        + [DMA((CHUNKS,))] * 5
        + [DMA((count,))] * 4
        + [DMA(()), DMA(())]
        + [DMA((count,))] * 2
        + [pltpu.SemaphoreType.REGULAR],
        name="exchange",
        compiler_params=pltpu.CompilerParams(
            collective_id=1, has_side_effects=True, vmem_limit_bytes=32 * 2**20
        ),
    )(matrix, *rotation)


def identity_of(block):
    row = lax.broadcasted_iota(jnp.int32, (block, block), 0)
    col = lax.broadcasted_iota(jnp.int32, (block, block), 1)
    return jnp.where(row == col, 1.0, 0.0).astype(F32)


def couple(rows_all, norms, cross, identity):
    scales = lax.rsqrt(norms / rows_all + 1e-06)
    scale_first = jnp.sum(identity * scales[0:1, :], axis=1, keepdims=True)
    cross[...] = 0.5 * cross[...] * scale_first * scales[1:2, :] / rows_all


def invert(grams, inverses, residuals, identity):
    block = identity.shape[0]
    spreads = [jnp.max(jnp.sum(jnp.abs(gram), axis=1, keepdims=True)) for gram in grams]
    for gram, spread, inverse, residual in zip(grams, spreads, inverses, residuals):
        start = 2.0 / (2.0 + spread)
        first = (1.0 - start) * identity - start * gram
        inverse[...] = start * (identity + first)
        residual[...] = exact_dot(first, first)
    spread = functools.reduce(jnp.maximum, spreads)
    bound = spread / (2.0 + spread)

    def grow(state):
        limit, trips = state
        for inverse, residual in zip(inverses, residuals):
            both = exact_dot(jnp.concatenate([inverse[...], residual[...]], axis=0), residual[...])
            inverse[...] += both[:block]
            residual[...] = both[block:]
        return limit * limit, trips + 1

    lax.while_loop(
        lambda state: jnp.logical_and(state[0] > 1e-07, state[1] < 30),
        grow,
        (bound * bound, jnp.int32(0)),
    )

    def correct(index, carry):
        for gram, inverse, residual in zip(grams, inverses, residuals):
            guess = inverse[...]
            residual[...] = identity - guess - exact_dot(gram, guess)
            inverse[...] = guess + exact_dot(guess, residual[...])
        return carry

    lax.fori_loop(0, jnp.where(spread > 32.0, 4, 0), correct, 0)


def rotation_kernel(rows_all, total, rot_high, rot_low, coupling, inverse, residual):
    block = coupling.shape[0]
    norms = unpack(total, coupling)
    identity = identity_of(block)
    couple(rows_all, norms, coupling, identity)
    turn = coupling[...]
    gram = exact_dot(turn, turn, 1, 1)
    invert([gram], [inverse], [residual], identity)
    upper = exact_dot(inverse[...], turn)
    lower = exact_dot(turn, upper, 0)
    parts = (
        (0, 0, 2.0 * inverse[...] - identity),
        (0, 1, 2.0 * upper),
        (1, 0, -2.0 * upper.T),
        (1, 1, identity - 2.0 * lower),
    )
    for down, across, value in parts:
        high, low = split(value)
        where = (pl.ds(down * block, block), pl.ds(across * block, block))
        rot_high[where] = high
        rot_low[where] = low


def rotation_of(total, rows_all):
    block = 2 * total.shape[2]
    vmem = pl.BlockSpec(memory_space=pltpu.VMEM)
    return pl.pallas_call(
        functools.partial(rotation_kernel, rows_all),
        out_shape=[jax.ShapeDtypeStruct((2 * block, 2 * block), BF16)] * 2,
        in_specs=[vmem],
        out_specs=[vmem, vmem],
        scratch_shapes=[pltpu.VMEM((block, block), F32)] * 3,
        name="rotation",
        compiler_params=pltpu.CompilerParams(vmem_limit_bytes=16 * 2**20),
    )(total)


def final_kernel(
    rows_all, place, lead, keep, lead_land, keep_land, total_keep, total_lead, out,
    turns, inverses, residuals, high, low, staged, sems,
):
    rows, block = lead.shape
    step = rows // CHUNKS
    position, length = place[0], place[1]
    identity = identity_of(block)
    couplings = [turns.at[0], turns.at[1]]
    own_out = [position == 1, position == 0]
    flips = [jnp.logical_not(own_out[0]), own_out[1]]
    odd = position % 2 == 1
    grams = []
    for index, total in enumerate((total_keep, total_lead)):
        norms = unpack(total, couplings[index])
        couple(rows_all, norms, couplings[index], identity)
        value = couplings[index][...]
        couplings[index][...] = jnp.where(flips[index], value.T, value)
        value = couplings[index][...]
        grams.append(exact_dot(value, value, 1, 1))
    invert(
        grams,
        [inverses.at[0], inverses.at[1]],
        [residuals.at[0], residuals.at[1]],
        identity,
    )
    first_slot = [odd, jnp.logical_not(odd)]
    for index in range(2):
        takes_first = jnp.where(
            first_slot[index], position != 1, position == length - 1
        )
        inverse = inverses[index]
        straight = 2.0 * inverse - identity
        sign = jnp.where(takes_first, -2.0, 2.0)
        crossed = sign * exact_dot(couplings[index][...], inverse, 0)
        own = jnp.where(own_out[index], straight, crossed)
        landed = jnp.where(own_out[index], crossed, straight)
        for part, value in enumerate((own, landed)):
            top, bottom = split(value)
            high[index, part] = top
            low[index, part] = bottom

    def at(chunk):
        return pl.ds(pl.multiple_of(chunk * step, step), step)

    def store(chunk, index):
        column = jnp.where(first_slot[index], 0, block)
        return pltpu.make_async_copy(
            staged.at[index, at(chunk)],
            out.at[at(chunk), pl.ds(pl.multiple_of(column, block), block)],
            sems.at[index, chunk],
        )

    def body(chunk, carry):
        for index, (own, landed) in enumerate(((keep, keep_land), (lead, lead_land))):
            staged[index, at(chunk), :] = dot_three(
                split(own[at(chunk), :]), (high[index, 0], low[index, 0]), 1
            ) + dot_three(split(landed[at(chunk), :]), (high[index, 1], low[index, 1]), 1)
            store(chunk, index).start()
        return carry

    lax.fori_loop(0, CHUNKS, body, 0)

    def drain(chunk, carry):
        store(chunk, 0).wait()
        store(chunk, 1).wait()
        return carry

    lax.fori_loop(0, CHUNKS, drain, 0)


def final(rows_all, blocks, totals):
    rows, block = blocks[0].shape
    vmem = pl.BlockSpec(memory_space=pltpu.VMEM)
    place = jnp.stack([lax.axis_index("pairs"), jnp.int32(lax.axis_size("pairs"))])
    return pl.pallas_call(
        functools.partial(final_kernel, rows_all),
        out_shape=jax.ShapeDtypeStruct((rows, 2 * block), F32),
        in_specs=[pl.BlockSpec(memory_space=pltpu.SMEM)] + [vmem] * 6,
        out_specs=pl.BlockSpec(memory_space=pl.ANY),
        scratch_shapes=[
            pltpu.VMEM((2, block, block), F32),
            pltpu.VMEM((2, block, block), F32),
            pltpu.VMEM((2, block, block), F32),
            pltpu.VMEM((2, 2, block, block), BF16),
            pltpu.VMEM((2, 2, block, block), BF16),
            pltpu.VMEM((2, rows, block), F32),
            DMA((2, CHUNKS)),
        ],
        name="final",
        compiler_params=pltpu.CompilerParams(vmem_limit_bytes=32 * 2**20),
    )(place, *blocks, *totals)


def shards(matrix):
    rows_all = matrix.shape[0] * lax.axis_size("rows")
    total = products(matrix)
    rotation = rotation_of(total, rows_all)
    moved = exchange(matrix, rotation, total.shape[1:])
    return final(rows_all, moved[:4], moved[4:])


def solution(mesh):
    return jax.shard_map(
        shards,
        mesh=mesh,
        in_specs=(P("rows", "pairs"),),
        out_specs=P("rows", "pairs"),
        check_vma=False,
    )
```

```python
import functools

import jax
import jax.numpy as jnp
from jax import lax
from jax.experimental import pallas as pl
from jax.experimental.pallas import tpu as pltpu
from jax.sharding import PartitionSpec as P

CHUNKS = 8
EARLY = 4
STORES = 4
F32 = jnp.float32
BF16 = jnp.bfloat16
MESH = pl.DeviceIdType.MESH
DMA = pltpu.SemaphoreType.DMA


def split(value):
    high = value.astype(BF16)
    return high, (value - high.astype(F32)).astype(BF16)


def dot_bf16(left, right, left_dim):
    return lax.dot_general(
        left, right, (((left_dim,), (0,)), ((), ())), preferred_element_type=F32
    )


def dot_three(left, right, left_dim):
    return (
        dot_bf16(left[0], right[1], left_dim)
        + dot_bf16(left[1], right[0], left_dim)
        + dot_bf16(left[0], right[0], left_dim)
    )


def exact_dot(left, right, left_dim=1, right_dim=0):
    return lax.dot_general(
        left,
        right,
        (((left_dim,), (right_dim,)), ((), ())),
        precision=lax.Precision.HIGHEST,
        preferred_element_type=F32,
    )


def rows_copy(src, dst, send, recv, peer):
    return pltpu.make_async_remote_copy(
        src_ref=src,
        dst_ref=dst,
        send_sem=send,
        recv_sem=recv,
        device_id={"rows": peer},
        device_id_type=MESH,
    )


def pairs_copy(src, dst, send, recv, peer):
    return pltpu.make_async_remote_copy(
        src_ref=src,
        dst_ref=dst,
        send_sem=send,
        recv_sem=recv,
        device_id={"pairs": peer},
        device_id_type=MESH,
    )


def greet(barrier, axis, peer):
    pl.semaphore_signal(barrier, inc=1, device_id={axis: peer}, device_id_type=MESH)


def partners(position, length):
    even = position % 2 == 0
    down = jnp.where(position == 0, 1, position - 2)
    up = jnp.where(position == length - 1, length - 2, position + 2)
    lead = jnp.where(even, down, up)
    down = jnp.where(position == 1, 0, position - 2)
    up = jnp.where(position == length - 2, length - 1, position + 2)
    keep = jnp.where(even, up, down)
    return lead, keep


def add_norms(norms, first, second):
    half = norms.shape[1]
    for row, value in ((0, first), (1, second)):
        sums = jnp.sum(value * value, axis=0, keepdims=True)
        norms[row : row + 1, :] += sums[:, :half]
        norms[row + 4 : row + 5, :] += sums[:, half:]


def pack(count, cross, norms, part):
    block = cross.shape[0]
    share = block // count
    half = block // 2
    for slot in range(count):
        part[slot, :share, :] = cross[slot * share : (slot + 1) * share, :half]
        part[slot, share : 2 * share, :] = cross[slot * share : (slot + 1) * share, half:]
        part[slot, 2 * share : 2 * share + 8, :] = norms[...]


def unpack(total, cross):
    count, depth, half = total.shape
    share = (depth - 8) // 2
    for slot in range(count):
        cross[slot * share : (slot + 1) * share, :half] = total[slot, :share, :]
        cross[slot * share : (slot + 1) * share, half:] = total[slot, share : 2 * share, :]
    norms = total[0, 2 * share :, :]
    return jnp.concatenate([norms[0:4], norms[4:8]], axis=1)


def scatter_sum(count, part, recv, mine, send_sems, recv_sems):
    me = lax.axis_index("rows")
    copies = []
    for far in range(1, count):
        peer = lax.rem(me + far, count)
        copy = rows_copy(part.at[peer], recv.at[far], send_sems.at[far], recv_sems.at[far], peer)
        copy.start()
        copies.append(copy)
    acc = part[me]
    for far in range(1, count):
        copies[far - 1].wait_recv()
        acc = acc + recv[far]
    mine[...] = acc
    return copies


def gather_start(count, mine, gathered, send_sems, recv_sems):
    me = lax.axis_index("rows")
    copies = []
    for far in range(1, count):
        peer = lax.rem(me + far, count)
        copy = rows_copy(mine, gathered.at[far], send_sems.at[far], recv_sems.at[far], peer)
        copy.start()
        copies.append(copy)
    return copies


def gather_finish(count, mine, gathered, total, copies):
    me = lax.axis_index("rows")
    total[me] = mine[...]
    for far in range(1, count):
        copies[far - 1].wait_recv()
        total[lax.rem(me + count - far, count)] = gathered[far]


def products_kernel(count, matrix, total, loaded, load_sem, cross, norms, part, recv, mine, gathered, *sems):
    rows, cols = loaded.shape
    block = cols // 2
    step = rows // CHUNKS

    def at(chunk):
        return pl.ds(pl.multiple_of(chunk * step, step), step)

    def load(chunk):
        return pltpu.make_async_copy(
            matrix.at[at(chunk)], loaded.at[at(chunk)], load_sem.at[chunk]
        )

    for chunk in range(CHUNKS):
        load(chunk).start()
    barrier = pltpu.get_barrier_semaphore()
    me = lax.axis_index("rows")
    for far in range(1, count):
        greet(barrier, "rows", lax.rem(me + far, count))
    cross[...] = jnp.zeros_like(cross)
    norms[...] = jnp.zeros_like(norms)

    def take(chunk, carry):
        load(chunk).wait()
        first, second = loaded[at(chunk), :block], loaded[at(chunk), block:]
        cross[...] += dot_three(split(first), split(second), 0)
        add_norms(norms, first, second)
        return carry

    lax.fori_loop(0, CHUNKS, take, 0)
    pack(count, cross, norms, part)
    pl.semaphore_wait(barrier, count - 1)
    copies = scatter_sum(count, part, recv, mine, sems[0], sems[1])
    more = gather_start(count, mine, gathered, sems[2], sems[3])
    gather_finish(count, mine, gathered, total, more)
    for copy in copies + more:
        copy.wait_send()


def products(matrix):
    rows, cols = matrix.shape
    block = cols // 2
    count = lax.axis_size("rows")
    slot = (2 * (block // count) + 8, block // 2)
    return pl.pallas_call(
        functools.partial(products_kernel, count),
        out_shape=[
            jax.ShapeDtypeStruct((count,) + slot, F32),
            jax.ShapeDtypeStruct((rows, cols), F32),
        ],
        in_specs=[pl.BlockSpec(memory_space=pltpu.HBM)],
        out_specs=[pl.BlockSpec(memory_space=pltpu.VMEM)] * 2,
        scratch_shapes=[
            DMA((CHUNKS,)),
            pltpu.VMEM((block, block), F32),
            pltpu.VMEM((8, block // 2), F32),
            pltpu.VMEM((count,) + slot, F32),
            pltpu.VMEM((count,) + slot, F32),
            pltpu.VMEM(slot, F32),
            pltpu.VMEM((count,) + slot, F32),
        ]
        + [DMA((count,))] * 4,
        name="products",
        compiler_params=pltpu.CompilerParams(
            collective_id=0, has_side_effects=True, vmem_limit_bytes=24 * 2**20
        ),
    )(matrix)


def invert_fixed(gram, inverse, residual, identity):
    block = identity.shape[0]
    largest = 0.25 * block * block
    ratio, trips = largest / (2.0 + largest), 0
    while ratio > 1e-08:
        ratio, trips = ratio * ratio / (2.0 - ratio * ratio), trips + 1
    sums = jnp.sum(jnp.abs(gram), axis=1, keepdims=True)
    spread = jnp.max(sums, axis=0, keepdims=True)
    start = 2.0 / (2.0 + spread)
    inverse[...] = start * identity
    residual[...] = (1.0 - start) * identity - start * gram

    def grow(index, ratio):
        square = ratio * ratio
        scale = 2.0 / (2.0 - square)
        both = exact_dot(jnp.concatenate([inverse[...], residual[...]], axis=0), residual[...])
        inverse[...] = scale * (inverse[...] + both[:block])
        residual[...] = (1.0 - scale) * identity + scale * both[block:]
        return square / (2.0 - square)

    lax.fori_loop(0, trips, grow, spread / (2.0 + spread))

    def correct(index, carry):
        guess = inverse[...]
        residual[...] = identity - guess - exact_dot(gram, guess)
        inverse[...] = guess + exact_dot(guess, residual[...])
        return carry

    lax.fori_loop(0, 2, correct, 0)


def exchange_kernel(
    rows_all, count, length, matrix, rot_high, rot_low, out_keep, out_lead,
    lead, keep, lead_land, keep_land, total_keep, total_lead,
    cross, norms, part, recv, mine, gathered, passed, gathered_lead,
    coupling, inverse, residual, high, low,
    lead_send, lead_recv, keep_send, keep_recv,
    sum_send, sum_recv, all_send, all_recv, pass_send, pass_recv, more_send, more_recv, go_sem,
):
    rows, cols = matrix.shape
    block = cols // 2
    step = rows // CHUNKS
    me = lax.axis_index("rows")
    position = lax.axis_index("pairs")
    lead_peer, keep_peer = partners(position, length)
    core_peer = position + 1 - 2 * (position % 2)
    near = keep_peer == core_peer
    even = position % 2 == 0
    left_leads = jnp.logical_or(position % 2 == 1, position == 0)
    signals = jnp.logical_and(position > 0, position < length - 1)

    def at(chunk):
        return pl.ds(pl.multiple_of(chunk * step, step), step)

    def send_lead(chunk):
        return pairs_copy(
            lead.at[at(chunk)], keep_land.at[at(chunk)],
            lead_send.at[chunk], lead_recv.at[chunk], lead_peer,
        )

    def send_keep(chunk):
        return pairs_copy(
            keep.at[at(chunk)], lead_land.at[at(chunk)],
            keep_send.at[chunk], keep_recv.at[chunk], keep_peer,
        )

    def loop(begin, end, do):
        def body(chunk, carry):
            do(chunk)
            return carry

        lax.fori_loop(begin, end, body, 0)

    barrier = pltpu.get_barrier_semaphore()
    for far in range(1, count):
        greet(barrier, "rows", lax.rem(me + far, count))
    for peer in (lead_peer, keep_peer, core_peer):
        greet(barrier, "pairs", peer)
    pl.semaphore_wait(barrier, count + 2)

    def rotate(chunk):
        turned = dot_three(split(matrix[at(chunk), :]), (rot_high[...], rot_low[...]), 1)
        left, right = turned[:, :block], turned[:, block:]
        lead[at(chunk), :] = jnp.where(left_leads, left, right)
        keep[at(chunk), :] = jnp.where(left_leads, right, left)
        send_lead(chunk).start()

        @pl.when(near)
        def _():
            send_keep(chunk).start()

    def take(chunk):
        send_lead(chunk).wait_recv()
        ours, theirs = keep[at(chunk), :], keep_land[at(chunk), :]
        cross[...] += dot_three(split(ours), split(theirs), 0)
        add_norms(norms, ours, theirs)

    def hand_over():
        loop(0, CHUNKS - 1, lambda chunk: send_lead(chunk).wait_send())

        @pl.when(signals)
        def _():
            pl.semaphore_signal(
                go_sem, inc=1, device_id={"pairs": core_peer}, device_id_type=MESH
            )

    def prepare(total, flip, takes_first, own_out):
        scales = unpack(total, coupling)
        identity = identity_of(block)
        couple(rows_all, scales, coupling, identity)
        value = coupling[...]
        coupling[...] = jnp.where(flip, value.T, value)
        value = coupling[...]
        invert_fixed(exact_dot(value, value, 1, 1), inverse, residual, identity)
        straight = 2.0 * inverse[...] - identity
        sign = jnp.where(takes_first, -2.0, 2.0)
        crossed = sign * exact_dot(coupling[...], inverse[...], 0)
        own = jnp.where(own_out, straight, crossed)
        landed = jnp.where(own_out, crossed, straight)
        high[0], low[0] = split(own)
        high[1], low[1] = split(landed)

    def finish(out, own, landed, chunk):
        out[at(chunk), :] = dot_three(split(own[at(chunk), :]), (high[0], low[0]), 1) + dot_three(
            split(landed[at(chunk), :]), (high[1], low[1]), 1
        )

    loop(0, CHUNKS, rotate)
    cross[...] = jnp.zeros_like(cross)
    norms[...] = jnp.zeros_like(norms)
    loop(0, CHUNKS - 1, take)

    @pl.when(jnp.logical_not(near))
    def _():
        hand_over()
        pl.semaphore_wait(go_sem, 1)
        loop(0, EARLY, lambda chunk: send_keep(chunk).start())

    take(CHUNKS - 1)
    pack(count, cross, norms, part)
    copies = scatter_sum(count, part, recv, mine, sum_send, sum_recv)
    piece = pairs_copy(mine, passed, pass_send, pass_recv, keep_peer)
    piece.start()
    more = gather_start(count, mine, gathered, all_send, all_recv)

    @pl.when(jnp.logical_not(near))
    def _():
        loop(EARLY, CHUNKS, lambda chunk: send_keep(chunk).start())
        piece.wait_recv()
        gather_start(count, passed, gathered_lead, more_send, more_recv)

    gather_finish(count, mine, gathered, total_keep, more)
    prepare(
        total_keep,
        position != 1,
        jnp.logical_and(jnp.logical_not(even), position != 1),
        position == 1,
    )

    @pl.when(near)
    def _():
        hand_over()
        piece.wait_recv()
        gather_start(count, passed, gathered_lead, more_send, more_recv)

    loop(0, CHUNKS, lambda chunk: finish(out_keep, keep, keep_land, chunk))
    rest = [
        rows_copy(passed, gathered_lead.at[far], more_send.at[far], more_recv.at[far], lax.rem(me + far, count))
        for far in range(1, count)
    ]
    gather_finish(count, passed, gathered_lead, total_lead, rest)
    prepare(
        total_lead,
        position == 0,
        jnp.logical_or(even, position == length - 1),
        position == 0,
    )

    def last(chunk):
        send_keep(chunk).wait_recv()
        finish(out_lead, lead, lead_land, chunk)

    loop(0, CHUNKS, last)
    for copy in copies + more + rest + [piece]:
        copy.wait_send()
    send_lead(CHUNKS - 1).wait_send()
    loop(0, CHUNKS, lambda chunk: send_keep(chunk).wait_send())


def exchange(rows_all, matrix, rotation, slot):
    rows, cols = matrix.shape
    block = cols // 2
    count = lax.axis_size("rows")
    length = lax.axis_size("pairs")
    vmem = pl.BlockSpec(memory_space=pltpu.VMEM)
    pieces = pltpu.VMEM((count,) + slot, F32)
    return pl.pallas_call(
        functools.partial(exchange_kernel, rows_all, count, length),
        out_shape=[jax.ShapeDtypeStruct((rows, block), F32)] * 2,
        in_specs=[vmem] * 3,
        out_specs=[vmem] * 2,
        scratch_shapes=[pltpu.VMEM((rows, block), F32)] * 4
        + [pieces] * 2
        + [pltpu.VMEM((block, block), F32), pltpu.VMEM((8, block // 2), F32)]
        + [pieces] * 2
        + [pltpu.VMEM(slot, F32), pieces, pltpu.VMEM(slot, F32), pieces]
        + [pltpu.VMEM((block, block), F32)] * 3
        + [pltpu.VMEM((2, block, block), BF16)] * 2
        + [DMA((CHUNKS,))] * 4
        + [DMA((count,))] * 4
        + [DMA(()), DMA(())]
        + [DMA((count,))] * 2
        + [pltpu.SemaphoreType.REGULAR],
        name="exchange",
        compiler_params=pltpu.CompilerParams(
            collective_id=1, has_side_effects=True, vmem_limit_bytes=32 * 2**20
        ),
    )(matrix, *rotation)


def identity_of(block):
    row = lax.broadcasted_iota(jnp.int32, (block, block), 0)
    col = lax.broadcasted_iota(jnp.int32, (block, block), 1)
    return jnp.where(row == col, 1.0, 0.0).astype(F32)


def couple(rows_all, norms, cross, identity):
    scales = lax.rsqrt(norms / rows_all + 1e-06)
    scale_first = jnp.sum(identity * scales[0:1, :], axis=1, keepdims=True)
    cross[...] = 0.5 * cross[...] * scale_first * scales[1:2, :] / rows_all


def invert(grams, inverses, residuals, identity):
    block = identity.shape[0]
    spreads = [jnp.max(jnp.sum(jnp.abs(gram), axis=1, keepdims=True)) for gram in grams]
    for gram, spread, inverse, residual in zip(grams, spreads, inverses, residuals):
        start = 2.0 / (2.0 + spread)
        first = (1.0 - start) * identity - start * gram
        inverse[...] = start * (identity + first)
        residual[...] = exact_dot(first, first)
    spread = functools.reduce(jnp.maximum, spreads)
    bound = spread / (2.0 + spread)

    def grow(state):
        limit, trips = state
        for inverse, residual in zip(inverses, residuals):
            both = exact_dot(jnp.concatenate([inverse[...], residual[...]], axis=0), residual[...])
            inverse[...] += both[:block]
            residual[...] = both[block:]
        return limit * limit, trips + 1

    lax.while_loop(
        lambda state: jnp.logical_and(state[0] > 1e-07, state[1] < 30),
        grow,
        (bound * bound, jnp.int32(0)),
    )

    def correct(index, carry):
        for gram, inverse, residual in zip(grams, inverses, residuals):
            guess = inverse[...]
            residual[...] = identity - guess - exact_dot(gram, guess)
            inverse[...] = guess + exact_dot(guess, residual[...])
        return carry

    lax.fori_loop(0, jnp.where(spread > 32.0, 4, 0), correct, 0)


def rotation_kernel(rows_all, total, rot_high, rot_low, coupling, inverse, residual):
    block = coupling.shape[0]
    norms = unpack(total, coupling)
    identity = identity_of(block)
    couple(rows_all, norms, coupling, identity)
    turn = coupling[...]
    gram = exact_dot(turn, turn, 1, 1)
    invert([gram], [inverse], [residual], identity)
    upper = exact_dot(inverse[...], turn)
    lower = exact_dot(turn, upper, 0)
    parts = (
        (0, 0, 2.0 * inverse[...] - identity),
        (0, 1, 2.0 * upper),
        (1, 0, -2.0 * upper.T),
        (1, 1, identity - 2.0 * lower),
    )
    for down, across, value in parts:
        high, low = split(value)
        where = (pl.ds(down * block, block), pl.ds(across * block, block))
        rot_high[where] = high
        rot_low[where] = low


def rotation_of(total, rows_all):
    block = 2 * total.shape[2]
    vmem = pl.BlockSpec(memory_space=pltpu.VMEM)
    return pl.pallas_call(
        functools.partial(rotation_kernel, rows_all),
        out_shape=[jax.ShapeDtypeStruct((2 * block, 2 * block), BF16)] * 2,
        in_specs=[vmem],
        out_specs=[vmem, vmem],
        scratch_shapes=[pltpu.VMEM((block, block), F32)] * 3,
        name="rotation",
        compiler_params=pltpu.CompilerParams(vmem_limit_bytes=16 * 2**20),
    )(total)


def store_kernel(keep, lead, out, sems):
    rows, block = lead.shape
    step = rows // STORES
    odd = lax.axis_index("pairs") % 2

    def store(chunk, index):
        column = jnp.where(odd == index, block, 0)
        at = pl.ds(chunk * step, step)
        return pltpu.make_async_copy(
            (keep, lead)[index].at[at],
            out.at[at, pl.ds(pl.multiple_of(column, block), block)],
            sems.at[index, chunk],
        )

    copies = [store(chunk, index) for chunk in range(STORES) for index in range(2)]
    for copy in copies:
        copy.start()
    for copy in copies:
        copy.wait()


def store(keep, lead):
    rows, block = lead.shape
    vmem = pl.BlockSpec(memory_space=pltpu.VMEM)
    return pl.pallas_call(
        store_kernel,
        out_shape=jax.ShapeDtypeStruct((rows, 2 * block), F32),
        in_specs=[vmem] * 2,
        out_specs=pl.BlockSpec(memory_space=pl.ANY),
        scratch_shapes=[DMA((2, STORES))],
        name="store",
        compiler_params=pltpu.CompilerParams(vmem_limit_bytes=16 * 2**20),
    )(keep, lead)


def shards(matrix):
    rows_all = matrix.shape[0] * lax.axis_size("rows")
    total, loaded = products(pltpu.with_memory_space_constraint(matrix, pltpu.HBM))
    rotation = rotation_of(total, rows_all)
    return store(*exchange(rows_all, loaded, rotation, total.shape[1:]))


def solution(mesh):
    return jax.shard_map(
        shards,
        mesh=mesh,
        in_specs=(P("rows", "pairs"),),
        out_specs=P("rows", "pairs"),
        check_vma=False,
    )
```

```python
import functools

import jax
import jax.numpy as jnp
from jax import lax
from jax.experimental import pallas as pl
from jax.experimental.pallas import tpu as pltpu
from jax.sharding import PartitionSpec as P

LOADS = 4
CHUNKS = 8
SENDS = 16
EARLY = 6
RELAY = 10
STORES = 4
F32 = jnp.float32
BF16 = jnp.bfloat16
MESH = pl.DeviceIdType.MESH
DMA = pltpu.SemaphoreType.DMA


def split(value):
    high = value.astype(BF16)
    return high, (value - high.astype(F32)).astype(BF16)


def dot_bf16(left, right, left_dim):
    return lax.dot_general(
        left, right, (((left_dim,), (0,)), ((), ())), preferred_element_type=F32
    )


def dot_three(left, right, left_dim):
    return (
        dot_bf16(left[0], right[1], left_dim)
        + dot_bf16(left[1], right[0], left_dim)
        + dot_bf16(left[0], right[0], left_dim)
    )


def exact_dot(left, right, left_dim=1, right_dim=0):
    return lax.dot_general(
        left,
        right,
        (((left_dim,), (right_dim,)), ((), ())),
        precision=lax.Precision.HIGHEST,
        preferred_element_type=F32,
    )


def rows_copy(src, dst, send, recv, peer):
    return pltpu.make_async_remote_copy(
        src_ref=src,
        dst_ref=dst,
        send_sem=send,
        recv_sem=recv,
        device_id={"rows": peer},
        device_id_type=MESH,
    )


def pairs_copy(src, dst, send, recv, peer):
    return pltpu.make_async_remote_copy(
        src_ref=src,
        dst_ref=dst,
        send_sem=send,
        recv_sem=recv,
        device_id={"pairs": peer},
        device_id_type=MESH,
    )


def greet(barrier, axis, peer):
    pl.semaphore_signal(barrier, inc=1, device_id={axis: peer}, device_id_type=MESH)


def partners(position, length):
    even = position % 2 == 0
    down = jnp.where(position == 0, 1, position - 2)
    up = jnp.where(position == length - 1, length - 2, position + 2)
    lead = jnp.where(even, down, up)
    down = jnp.where(position == 1, 0, position - 2)
    up = jnp.where(position == length - 2, length - 1, position + 2)
    keep = jnp.where(even, up, down)
    return lead, keep


def add_norms(norms, first, second):
    half = norms.shape[1]
    for row, value in ((0, first), (1, second)):
        sums = jnp.sum(value * value, axis=0, keepdims=True)
        norms[row : row + 1, :] += sums[:, :half]
        norms[row + 4 : row + 5, :] += sums[:, half:]


def pack(count, cross, norms, part):
    block = cross.shape[0]
    share = block // count
    half = block // 2
    for slot in range(count):
        part[slot, :share, :] = cross[slot * share : (slot + 1) * share, :half]
        part[slot, share : 2 * share, :] = cross[slot * share : (slot + 1) * share, half:]
        part[slot, 2 * share : 2 * share + 8, :] = norms[...]


def unpack(total, cross):
    count, depth, half = total.shape
    share = (depth - 8) // 2
    for slot in range(count):
        cross[slot * share : (slot + 1) * share, :half] = total[slot, :share, :]
        cross[slot * share : (slot + 1) * share, half:] = total[slot, share : 2 * share, :]
    norms = total[0, 2 * share :, :]
    return jnp.concatenate([norms[0:4], norms[4:8]], axis=1)


def scatter_sum(count, part, recv, mine, send_sems, recv_sems):
    me = lax.axis_index("rows")
    copies = []
    for far in range(1, count):
        peer = lax.rem(me + far, count)
        copy = rows_copy(part.at[peer], recv.at[far], send_sems.at[far], recv_sems.at[far], peer)
        copy.start()
        copies.append(copy)
    acc = part[me]
    for far in range(1, count):
        copies[far - 1].wait_recv()
        acc = acc + recv[far]
    mine[...] = acc
    return copies


def gather_start(count, mine, gathered, send_sems, recv_sems):
    me = lax.axis_index("rows")
    copies = []
    for far in range(1, count):
        peer = lax.rem(me + far, count)
        copy = rows_copy(mine, gathered.at[far], send_sems.at[far], recv_sems.at[far], peer)
        copy.start()
        copies.append(copy)
    return copies


def gather_finish(count, mine, gathered, total, copies):
    me = lax.axis_index("rows")
    total[me] = mine[...]
    for far in range(1, count):
        copies[far - 1].wait_recv()
        total[lax.rem(me + count - far, count)] = gathered[far]


def products_kernel(count, matrix, total, loaded, load_sem, cross, norms, part, recv, mine, gathered, *sems):
    rows, cols = loaded.shape
    block = cols // 2
    step = rows // LOADS

    def at(chunk):
        return pl.ds(pl.multiple_of(chunk * step, step), step)

    def load(chunk):
        return pltpu.make_async_copy(
            matrix.at[at(chunk)], loaded.at[at(chunk)], load_sem.at[chunk]
        )

    for chunk in range(LOADS):
        load(chunk).start()
    barrier = pltpu.get_barrier_semaphore()
    me = lax.axis_index("rows")
    for far in range(1, count):
        greet(barrier, "rows", lax.rem(me + far, count))
    cross[...] = jnp.zeros_like(cross)
    norms[...] = jnp.zeros_like(norms)

    def take(chunk, carry):
        load(chunk).wait()
        first, second = loaded[at(chunk), :block], loaded[at(chunk), block:]
        cross[...] += dot_three(split(first), split(second), 0)
        add_norms(norms, first, second)
        return carry

    lax.fori_loop(0, LOADS, take, 0)
    pack(count, cross, norms, part)
    pl.semaphore_wait(barrier, count - 1)
    copies = scatter_sum(count, part, recv, mine, sems[0], sems[1])
    more = gather_start(count, mine, gathered, sems[2], sems[3])
    gather_finish(count, mine, gathered, total, more)
    for copy in copies + more:
        copy.wait_send()


def products(matrix):
    rows, cols = matrix.shape
    block = cols // 2
    count = lax.axis_size("rows")
    slot = (2 * (block // count) + 8, block // 2)
    return pl.pallas_call(
        functools.partial(products_kernel, count),
        out_shape=[
            jax.ShapeDtypeStruct((count,) + slot, F32),
            jax.ShapeDtypeStruct((rows, cols), F32),
        ],
        in_specs=[pl.BlockSpec(memory_space=pltpu.HBM)],
        out_specs=[pl.BlockSpec(memory_space=pltpu.VMEM)] * 2,
        scratch_shapes=[
            DMA((LOADS,)),
            pltpu.VMEM((block, block), F32),
            pltpu.VMEM((8, block // 2), F32),
            pltpu.VMEM((count,) + slot, F32),
            pltpu.VMEM((count,) + slot, F32),
            pltpu.VMEM(slot, F32),
            pltpu.VMEM((count,) + slot, F32),
        ]
        + [DMA((count,))] * 4,
        name="products",
        compiler_params=pltpu.CompilerParams(
            collective_id=0, has_side_effects=True, vmem_limit_bytes=24 * 2**20
        ),
    )(matrix)


def invert_fixed(gram, inverse, residual, identity):
    block = identity.shape[0]
    largest = 0.25 * block * block
    ratio, trips = largest / (2.0 + largest), 0
    while ratio > 0.01:
        ratio, trips = ratio * ratio / (2.0 - ratio * ratio), trips + 1
    sums = jnp.sum(jnp.abs(gram), axis=1, keepdims=True)
    spread = jnp.max(sums, axis=0, keepdims=True)
    start = 2.0 / (2.0 + spread)
    inverse[...] = start * identity
    residual[...] = (1.0 - start) * identity - start * gram

    def grow(index, ratio):
        square = ratio * ratio
        scale = 2.0 / (2.0 - square)
        power = split(residual[...])
        more = dot_three(split(inverse[...]), power, 1)
        inverse[...] = scale * (inverse[...] + more)
        residual[...] = (1.0 - scale) * identity + scale * dot_three(power, power, 1)
        return square / (2.0 - square)

    lax.fori_loop(0, trips, grow, spread / (2.0 + spread))

    def correct(index, carry):
        guess = inverse[...]
        error = identity - guess - exact_dot(gram, guess)
        inverse[...] = guess + dot_three(split(guess), split(error), 1)
        return carry

    lax.fori_loop(0, 2, correct, 0)


def exchange_kernel(
    rows_all, count, length, matrix, rot_high, rot_low, out_keep, out_lead,
    lead, keep, lead_land, keep_land, total_keep, total_lead,
    cross, norms, part, recv, mine, gathered, passed, gathered_lead,
    coupling, inverse, residual, high, low,
    lead_send, lead_recv, keep_send, keep_recv,
    sum_send, sum_recv, all_send, all_recv, pass_send, pass_recv, more_send, more_recv, go_sem,
):
    rows, cols = matrix.shape
    block = cols // 2
    step = rows // SENDS
    group = SENDS // CHUNKS
    me = lax.axis_index("rows")
    position = lax.axis_index("pairs")
    lead_peer, keep_peer = partners(position, length)
    core_peer = position + 1 - 2 * (position % 2)
    near_keep = keep_peer == core_peer
    near_lead = lead_peer == core_peer
    even = position % 2 == 0
    left_leads = jnp.logical_or(position % 2 == 1, position == 0)
    signals = jnp.logical_and(position > 0, position < length - 1)

    def at(send, sends=1):
        return pl.ds(pl.multiple_of(send * step, step), sends * step)

    def send_lead(send):
        return pairs_copy(
            lead.at[at(send)], keep_land.at[at(send)],
            lead_send.at[send], lead_recv.at[send], lead_peer,
        )

    def send_keep(send):
        return pairs_copy(
            keep.at[at(send)], lead_land.at[at(send)],
            keep_send.at[send], keep_recv.at[send], keep_peer,
        )

    def loop(begin, end, do):
        def body(index, carry):
            do(index)
            return carry

        lax.fori_loop(begin, end, body, 0)

    barrier = pltpu.get_barrier_semaphore()
    for far in range(1, count):
        greet(barrier, "rows", lax.rem(me + far, count))
    for peer in (lead_peer, keep_peer, core_peer):
        greet(barrier, "pairs", peer)

    def turn(chunk):
        where = at(chunk * group, group)
        turned = dot_three(split(matrix[where, :]), (rot_high[...], rot_low[...]), 1)
        left, right = turned[:, :block], turned[:, block:]
        lead[where, :] = jnp.where(left_leads, left, right)
        keep[where, :] = jnp.where(left_leads, right, left)

    def send(chunk):
        for offset in range(group):
            send_lead(chunk * group + offset).start()

        @pl.when(near_keep)
        def _():
            for offset in range(group):
                send_keep(chunk * group + offset).start()

    def turn_and_send(chunk):
        turn(chunk)
        send(chunk)

    def take(send):
        send_lead(send).wait_recv()
        ours, theirs = keep[at(send), :], keep_land[at(send), :]
        cross[...] += dot_three(split(ours), split(theirs), 0)
        add_norms(norms, ours, theirs)

    def hand_over():
        loop(0, SENDS - 1, lambda send: send_lead(send).wait_send())

        @pl.when(signals)
        def _():
            pl.semaphore_signal(
                go_sem, inc=1, device_id={"pairs": core_peer}, device_id_type=MESH
            )

    def relay():
        pairs_copy(mine, passed, pass_send, pass_recv, keep_peer).wait_recv()
        gather_start(count, passed, gathered_lead, more_send, more_recv)

    def prepare(total, flip, takes_first, own_out):
        scales = unpack(total, coupling)
        identity = identity_of(block)
        couple(rows_all, scales, coupling, identity)
        value = coupling[...]
        coupling[...] = jnp.where(flip, value.T, value)
        value = coupling[...]
        invert_fixed(exact_dot(value, value, 1, 1), inverse, residual, identity)
        straight = 2.0 * inverse[...] - identity
        sign = jnp.where(takes_first, -2.0, 2.0)
        crossed = sign * exact_dot(coupling[...], inverse[...], 0)
        own = jnp.where(own_out, straight, crossed)
        landed = jnp.where(own_out, crossed, straight)
        high[0], low[0] = split(own)
        high[1], low[1] = split(landed)

    def finish(out, own, landed, chunk):
        where = at(chunk * group, group)
        out[where, :] = dot_three(split(own[where, :]), (high[0], low[0]), 1) + dot_three(
            split(landed[where, :]), (high[1], low[1]), 1
        )

    def finish_lead():
        gather_finish(count, passed, gathered_lead, total_lead, rest)
        prepare(
            total_lead,
            position == 0,
            jnp.logical_or(even, position == length - 1),
            position == 0,
        )

        def last(chunk):
            for offset in range(group):
                send_keep(chunk * group + offset).wait_recv()
            finish(out_lead, lead, lead_land, chunk)

        loop(0, CHUNKS, last)

    rest = [
        rows_copy(
            passed, gathered_lead.at[far], more_send.at[far], more_recv.at[far],
            lax.rem(me + far, count),
        )
        for far in range(1, count)
    ]
    turn(0)
    cross[...] = jnp.zeros_like(cross)
    norms[...] = jnp.zeros_like(norms)
    pl.semaphore_wait(barrier, count + 2)
    send(0)
    loop(1, CHUNKS, turn_and_send)
    loop(0, RELAY, take)

    @pl.when(near_lead)
    def _():
        relay()

    loop(RELAY, SENDS - 1, take)

    @pl.when(jnp.logical_not(near_keep))
    def _():
        hand_over()
        pl.semaphore_wait(go_sem, 1)
        loop(0, EARLY, lambda send: send_keep(send).start())

    take(SENDS - 1)
    pack(count, cross, norms, part)
    copies = scatter_sum(count, part, recv, mine, sum_send, sum_recv)
    piece = pairs_copy(mine, passed, pass_send, pass_recv, keep_peer)
    piece.start()
    more = gather_start(count, mine, gathered, all_send, all_recv)

    @pl.when(jnp.logical_not(near_keep))
    def _():
        loop(EARLY, SENDS, lambda send: send_keep(send).start())

    @pl.when(near_lead)
    def _():
        finish_lead()

    gather_finish(count, mine, gathered, total_keep, more)

    @pl.when(near_keep)
    def _():
        hand_over()

    prepare(
        total_keep,
        position != 1,
        jnp.logical_and(jnp.logical_not(even), position != 1),
        position == 1,
    )
    loop(0, CHUNKS, lambda chunk: finish(out_keep, keep, keep_land, chunk))

    @pl.when(jnp.logical_not(near_lead))
    def _():
        relay()
        finish_lead()

    for copy in copies + more + rest + [piece]:
        copy.wait_send()
    send_lead(SENDS - 1).wait_send()
    loop(0, SENDS, lambda send: send_keep(send).wait_send())


def exchange(rows_all, matrix, rotation, slot):
    rows, cols = matrix.shape
    block = cols // 2
    count = lax.axis_size("rows")
    length = lax.axis_size("pairs")
    vmem = pl.BlockSpec(memory_space=pltpu.VMEM)
    pieces = pltpu.VMEM((count,) + slot, F32)
    return pl.pallas_call(
        functools.partial(exchange_kernel, rows_all, count, length),
        out_shape=[jax.ShapeDtypeStruct((rows, block), F32)] * 2,
        in_specs=[vmem] * 3,
        out_specs=[vmem] * 2,
        scratch_shapes=[pltpu.VMEM((rows, block), F32)] * 4
        + [pieces] * 2
        + [pltpu.VMEM((block, block), F32), pltpu.VMEM((8, block // 2), F32)]
        + [pieces] * 2
        + [pltpu.VMEM(slot, F32), pieces, pltpu.VMEM(slot, F32), pieces]
        + [pltpu.VMEM((block, block), F32)] * 3
        + [pltpu.VMEM((2, block, block), BF16)] * 2
        + [DMA((SENDS,))] * 4
        + [DMA((count,))] * 4
        + [DMA(()), DMA(())]
        + [DMA((count,))] * 2
        + [pltpu.SemaphoreType.REGULAR],
        name="exchange",
        compiler_params=pltpu.CompilerParams(
            collective_id=1, has_side_effects=True, vmem_limit_bytes=32 * 2**20
        ),
    )(matrix, *rotation)


def identity_of(block):
    row = lax.broadcasted_iota(jnp.int32, (block, block), 0)
    col = lax.broadcasted_iota(jnp.int32, (block, block), 1)
    return jnp.where(row == col, 1.0, 0.0).astype(F32)


def couple(rows_all, norms, cross, identity):
    scales = lax.rsqrt(norms / rows_all + 1e-06)
    scale_first = jnp.sum(identity * scales[0:1, :], axis=1, keepdims=True)
    cross[...] = 0.5 * cross[...] * scale_first * scales[1:2, :] / rows_all


def invert(grams, inverses, residuals, identity):
    block = identity.shape[0]
    spreads = [jnp.max(jnp.sum(jnp.abs(gram), axis=1, keepdims=True)) for gram in grams]
    for gram, spread, inverse, residual in zip(grams, spreads, inverses, residuals):
        start = 2.0 / (2.0 + spread)
        first = (1.0 - start) * identity - start * gram
        inverse[...] = start * (identity + first)
        residual[...] = exact_dot(first, first)
    spread = functools.reduce(jnp.maximum, spreads)
    bound = spread / (2.0 + spread)

    def grow(state):
        limit, trips = state
        for inverse, residual in zip(inverses, residuals):
            both = exact_dot(jnp.concatenate([inverse[...], residual[...]], axis=0), residual[...])
            inverse[...] += both[:block]
            residual[...] = both[block:]
        return limit * limit, trips + 1

    lax.while_loop(
        lambda state: jnp.logical_and(state[0] > 1e-07, state[1] < 30),
        grow,
        (bound * bound, jnp.int32(0)),
    )

    def correct(index, carry):
        for gram, inverse, residual in zip(grams, inverses, residuals):
            guess = inverse[...]
            residual[...] = identity - guess - exact_dot(gram, guess)
            inverse[...] = guess + exact_dot(guess, residual[...])
        return carry

    lax.fori_loop(0, jnp.where(spread > 32.0, 4, 0), correct, 0)


def rotation_kernel(rows_all, total, rot_high, rot_low, coupling, inverse, residual):
    block = coupling.shape[0]
    norms = unpack(total, coupling)
    identity = identity_of(block)
    couple(rows_all, norms, coupling, identity)
    turn = coupling[...]
    gram = exact_dot(turn, turn, 1, 1)
    invert([gram], [inverse], [residual], identity)
    upper = exact_dot(inverse[...], turn)
    lower = exact_dot(turn, upper, 0)
    parts = (
        (0, 0, 2.0 * inverse[...] - identity),
        (0, 1, 2.0 * upper),
        (1, 0, -2.0 * upper.T),
        (1, 1, identity - 2.0 * lower),
    )
    for down, across, value in parts:
        high, low = split(value)
        where = (pl.ds(down * block, block), pl.ds(across * block, block))
        rot_high[where] = high
        rot_low[where] = low


def rotation_of(total, rows_all):
    block = 2 * total.shape[2]
    vmem = pl.BlockSpec(memory_space=pltpu.VMEM)
    return pl.pallas_call(
        functools.partial(rotation_kernel, rows_all),
        out_shape=[jax.ShapeDtypeStruct((2 * block, 2 * block), BF16)] * 2,
        in_specs=[vmem],
        out_specs=[vmem, vmem],
        scratch_shapes=[pltpu.VMEM((block, block), F32)] * 3,
        name="rotation",
        compiler_params=pltpu.CompilerParams(vmem_limit_bytes=16 * 2**20),
    )(total)


def store_kernel(keep, lead, out, sems):
    rows, block = lead.shape
    step = rows // STORES
    odd = lax.axis_index("pairs") % 2

    def store(chunk, index):
        column = jnp.where(odd == index, block, 0)
        at = pl.ds(chunk * step, step)
        return pltpu.make_async_copy(
            (keep, lead)[index].at[at],
            out.at[at, pl.ds(pl.multiple_of(column, block), block)],
            sems.at[index, chunk],
        )

    copies = [store(chunk, index) for chunk in range(STORES) for index in range(2)]
    for copy in copies:
        copy.start()
    for copy in copies:
        copy.wait()


def store(keep, lead):
    rows, block = lead.shape
    vmem = pl.BlockSpec(memory_space=pltpu.VMEM)
    return pl.pallas_call(
        store_kernel,
        out_shape=jax.ShapeDtypeStruct((rows, 2 * block), F32),
        in_specs=[vmem] * 2,
        out_specs=pl.BlockSpec(memory_space=pl.ANY),
        scratch_shapes=[DMA((2, STORES))],
        name="store",
        compiler_params=pltpu.CompilerParams(vmem_limit_bytes=16 * 2**20),
    )(keep, lead)


def shards(matrix):
    rows_all = matrix.shape[0] * lax.axis_size("rows")
    total, loaded = products(pltpu.with_memory_space_constraint(matrix, pltpu.HBM))
    rotation = rotation_of(total, rows_all)
    return store(*exchange(rows_all, loaded, rotation, total.shape[1:]))


def solution(mesh):
    return jax.shard_map(
        shards,
        mesh=mesh,
        in_specs=(P("rows", "pairs"),),
        out_specs=P("rows", "pairs"),
        check_vma=False,
    )
```

```python
import functools

import jax
import jax.numpy as jnp
from jax import lax
from jax.experimental import pallas as pl
from jax.experimental.pallas import tpu as pltpu
from jax.sharding import PartitionSpec as P

LOADS = 4
CHUNKS = 8
SENDS = 16
EARLY = 6
RAW = 6
RAW_FIRST = 3
STORES = 4
F32 = jnp.float32
BF16 = jnp.bfloat16
MESH = pl.DeviceIdType.MESH
DMA = pltpu.SemaphoreType.DMA


def split(value):
    high = value.astype(BF16)
    return high, (value - high.astype(F32)).astype(BF16)


def dot_bf16(left, right, left_dim):
    return lax.dot_general(
        left, right, (((left_dim,), (0,)), ((), ())), preferred_element_type=F32
    )


def dot_three(left, right, left_dim):
    return (
        dot_bf16(left[0], right[1], left_dim)
        + dot_bf16(left[1], right[0], left_dim)
        + dot_bf16(left[0], right[0], left_dim)
    )


def exact_dot(left, right, left_dim=1, right_dim=0):
    return lax.dot_general(
        left,
        right,
        (((left_dim,), (right_dim,)), ((), ())),
        precision=lax.Precision.HIGHEST,
        preferred_element_type=F32,
    )


def rows_copy(src, dst, send, recv, peer):
    return pltpu.make_async_remote_copy(
        src_ref=src,
        dst_ref=dst,
        send_sem=send,
        recv_sem=recv,
        device_id={"rows": peer},
        device_id_type=MESH,
    )


def pairs_copy(src, dst, send, recv, peer):
    return pltpu.make_async_remote_copy(
        src_ref=src,
        dst_ref=dst,
        send_sem=send,
        recv_sem=recv,
        device_id={"pairs": peer},
        device_id_type=MESH,
    )


def greet(barrier, axis, peer):
    pl.semaphore_signal(barrier, inc=1, device_id={axis: peer}, device_id_type=MESH)


def partners(position, length):
    even = position % 2 == 0
    down = jnp.where(position == 0, 1, position - 2)
    up = jnp.where(position == length - 1, length - 2, position + 2)
    lead = jnp.where(even, down, up)
    down = jnp.where(position == 1, 0, position - 2)
    up = jnp.where(position == length - 2, length - 1, position + 2)
    keep = jnp.where(even, up, down)
    return lead, keep


def add_norms(norms, first, second):
    half = norms.shape[1]
    for row, value in ((0, first), (1, second)):
        sums = jnp.sum(value * value, axis=0, keepdims=True)
        norms[row : row + 1, :] += sums[:, :half]
        norms[row + 4 : row + 5, :] += sums[:, half:]


def pack(count, cross, norms, part):
    block = cross.shape[0]
    share = block // count
    half = block // 2
    for slot in range(count):
        part[slot, :share, :] = cross[slot * share : (slot + 1) * share, :half]
        part[slot, share : 2 * share, :] = cross[slot * share : (slot + 1) * share, half:]
        part[slot, 2 * share : 2 * share + 8, :] = norms[...]


def unpack(total, cross):
    count, depth, half = total.shape
    share = (depth - 8) // 2
    for slot in range(count):
        cross[slot * share : (slot + 1) * share, :half] = total[slot, :share, :]
        cross[slot * share : (slot + 1) * share, half:] = total[slot, share : 2 * share, :]
    norms = total[0, 2 * share :, :]
    return jnp.concatenate([norms[0:4], norms[4:8]], axis=1)


def scatter_sum(count, part, recv, mine, send_sems, recv_sems):
    me = lax.axis_index("rows")
    copies = []
    for far in range(1, count):
        peer = lax.rem(me + far, count)
        copy = rows_copy(part.at[peer], recv.at[far], send_sems.at[far], recv_sems.at[far], peer)
        copy.start()
        copies.append(copy)
    acc = part[me]
    for far in range(1, count):
        copies[far - 1].wait_recv()
        acc = acc + recv[far]
    mine[...] = acc
    return copies


def gather_start(count, mine, gathered, send_sems, recv_sems):
    me = lax.axis_index("rows")
    copies = []
    for far in range(1, count):
        peer = lax.rem(me + far, count)
        copy = rows_copy(mine, gathered.at[far], send_sems.at[far], recv_sems.at[far], peer)
        copy.start()
        copies.append(copy)
    return copies


def gather_finish(count, mine, gathered, total, copies):
    me = lax.axis_index("rows")
    total[me] = mine[...]
    for far in range(1, count):
        copies[far - 1].wait_recv()
        total[lax.rem(me + count - far, count)] = gathered[far]


def products_kernel(
    count, length, matrix, total, loaded, raw, raw_piece,
    load_sem, cross, norms, part, recv, mine, gathered,
    sum_send, sum_recv, all_send, all_recv, raw_send, raw_recv, piece_send, piece_recv,
):
    rows, cols = loaded.shape
    block = cols // 2
    step = rows // LOADS
    send_rows = rows // SENDS
    raw_start = rows - RAW * send_rows
    me = lax.axis_index("rows")
    position = lax.axis_index("pairs")
    lead_peer, keep_peer = partners(position, length)
    core_peer = position + 1 - 2 * (position % 2)
    sends_raw = lead_peer != core_peer
    takes_raw = keep_peer != core_peer

    def at(chunk):
        return pl.ds(pl.multiple_of(chunk * step, step), step)

    def load(chunk):
        return pltpu.make_async_copy(
            matrix.at[at(chunk)], loaded.at[at(chunk)], load_sem.at[chunk]
        )

    def raw_copy(index):
        return pairs_copy(
            matrix.at[pl.ds(raw_start + index * send_rows, send_rows)],
            raw.at[pl.ds(index * send_rows, send_rows)],
            raw_send.at[index], raw_recv.at[index], lead_peer,
        )

    for chunk in range(LOADS):
        load(chunk).start()
    barrier = pltpu.get_barrier_semaphore()
    for far in range(1, count):
        greet(barrier, "rows", lax.rem(me + far, count))
    greet(barrier, "pairs", lead_peer)
    greet(barrier, "pairs", keep_peer)
    cross[...] = jnp.zeros_like(cross)
    norms[...] = jnp.zeros_like(norms)
    pl.semaphore_wait(barrier, count + 1)

    @pl.when(sends_raw)
    def _():
        for index in range(RAW_FIRST):
            raw_copy(index).start()

    def take(chunk, carry):
        load(chunk).wait()
        first, second = loaded[at(chunk), :block], loaded[at(chunk), block:]
        cross[...] += dot_three(split(first), split(second), 0)
        add_norms(norms, first, second)
        return carry

    lax.fori_loop(0, LOADS, take, 0)
    pack(count, cross, norms, part)
    copies = scatter_sum(count, part, recv, mine, sum_send, sum_recv)
    more = gather_start(count, mine, gathered, all_send, all_recv)
    piece = pairs_copy(mine, raw_piece, piece_send, piece_recv, lead_peer)

    @pl.when(sends_raw)
    def _():
        piece.start()
        for index in range(RAW_FIRST, RAW):
            raw_copy(index).start()

    gather_finish(count, mine, gathered, total, more)
    for copy in copies + more:
        copy.wait_send()

    @pl.when(sends_raw)
    def _():
        piece.wait_send()
        for index in range(RAW):
            raw_copy(index).wait_send()

    @pl.when(takes_raw)
    def _():
        piece.wait_recv()
        for index in range(RAW):
            raw_copy(index).wait_recv()


def products(matrix):
    rows, cols = matrix.shape
    block = cols // 2
    count = lax.axis_size("rows")
    length = lax.axis_size("pairs")
    slot = (2 * (block // count) + 8, block // 2)
    return pl.pallas_call(
        functools.partial(products_kernel, count, length),
        out_shape=[
            jax.ShapeDtypeStruct((count,) + slot, F32),
            jax.ShapeDtypeStruct((rows, cols), F32),
            jax.ShapeDtypeStruct((RAW * (rows // SENDS), cols), F32),
            jax.ShapeDtypeStruct(slot, F32),
        ],
        in_specs=[pl.BlockSpec(memory_space=pltpu.HBM)],
        out_specs=[pl.BlockSpec(memory_space=pltpu.VMEM)] * 4,
        scratch_shapes=[
            DMA((LOADS,)),
            pltpu.VMEM((block, block), F32),
            pltpu.VMEM((8, block // 2), F32),
            pltpu.VMEM((count,) + slot, F32),
            pltpu.VMEM((count,) + slot, F32),
            pltpu.VMEM(slot, F32),
            pltpu.VMEM((count,) + slot, F32),
        ]
        + [DMA((count,))] * 4
        + [DMA((RAW,))] * 2
        + [DMA(())] * 2,
        name="products",
        compiler_params=pltpu.CompilerParams(
            collective_id=0, has_side_effects=True, vmem_limit_bytes=24 * 2**20
        ),
    )(matrix)


def invert_fixed(gram, inverse, residual, identity):
    block = identity.shape[0]
    largest = 0.25 * block * block
    ratio, trips = largest / (2.0 + largest), 0
    while ratio > 0.01:
        ratio, trips = ratio * ratio / (2.0 - ratio * ratio), trips + 1
    sums = jnp.sum(jnp.abs(gram), axis=1, keepdims=True)
    spread = jnp.max(sums, axis=0, keepdims=True)
    start = 2.0 / (2.0 + spread)
    inverse[...] = start * identity
    residual[...] = (1.0 - start) * identity - start * gram

    def grow(index, ratio):
        square = ratio * ratio
        scale = 2.0 / (2.0 - square)
        power = split(residual[...])
        more = dot_three(split(inverse[...]), power, 1)
        inverse[...] = scale * (inverse[...] + more)
        residual[...] = (1.0 - scale) * identity + scale * dot_three(power, power, 1)
        return square / (2.0 - square)

    lax.fori_loop(0, trips, grow, spread / (2.0 + spread))

    def correct(index, carry):
        guess = inverse[...]
        error = identity - guess - exact_dot(gram, guess)
        inverse[...] = guess + dot_three(split(guess), split(error), 1)
        return carry

    lax.fori_loop(0, 2, correct, 0)


def exchange_kernel(
    rows_all, count, length, matrix, rot_high, rot_low, raw, raw_piece, out_keep, out_lead,
    lead, keep, lead_land, keep_land, total_keep, total_lead,
    cross, norms, part, recv, mine, gathered, passed, gathered_lead, total_raw, gathered_raw,
    coupling, inverse, residual, high, low,
    lead_send, lead_recv, keep_send, keep_recv,
    sum_send, sum_recv, all_send, all_recv, pass_send, pass_recv, more_send, more_recv, raw_send, raw_recv, go_sem,
):
    rows, cols = matrix.shape
    block = cols // 2
    step = rows // SENDS
    group = SENDS // CHUNKS
    me = lax.axis_index("rows")
    position = lax.axis_index("pairs")
    lead_peer, keep_peer = partners(position, length)
    core_peer = position + 1 - 2 * (position % 2)
    near_keep = keep_peer == core_peer
    near_lead = lead_peer == core_peer
    even = position % 2 == 0
    left_leads = jnp.logical_or(position % 2 == 1, position == 0)
    signals = jnp.logical_and(position > 0, position < length - 1)
    sent = jnp.where(near_lead, SENDS, SENDS - RAW)
    landing = jnp.where(near_keep, SENDS, SENDS - RAW)

    def at(send, sends=1):
        return pl.ds(pl.multiple_of(send * step, step), sends * step)

    def send_lead(send):
        return pairs_copy(
            lead.at[at(send)], keep_land.at[at(send)],
            lead_send.at[send], lead_recv.at[send], lead_peer,
        )

    def send_keep(send):
        return pairs_copy(
            keep.at[at(send)], lead_land.at[at(send)],
            keep_send.at[send], keep_recv.at[send], keep_peer,
        )

    def loop(begin, end, do):
        def body(index, carry):
            do(index)
            return carry

        lax.fori_loop(begin, end, body, 0)

    barrier = pltpu.get_barrier_semaphore()
    for far in range(1, count):
        greet(barrier, "rows", lax.rem(me + far, count))
    for peer in (lead_peer, keep_peer, core_peer):
        greet(barrier, "pairs", peer)

    def turn(chunk):
        where = at(chunk * group, group)
        turned = dot_three(split(matrix[where, :]), (rot_high[...], rot_low[...]), 1)
        left, right = turned[:, :block], turned[:, block:]
        lead[where, :] = jnp.where(left_leads, left, right)
        keep[where, :] = jnp.where(left_leads, right, left)

    def send(chunk):
        for offset in range(group):
            @pl.when(chunk * group + offset < sent)
            def _():
                send_lead(chunk * group + offset).start()

        @pl.when(near_keep)
        def _():
            for offset in range(group):
                send_keep(chunk * group + offset).start()

    def turn_and_send(chunk):
        turn(chunk)
        send(chunk)

    def multiply(send):
        ours, theirs = keep[at(send), :], keep_land[at(send), :]
        cross[...] += dot_three(split(ours), split(theirs), 0)
        add_norms(norms, ours, theirs)

    def take(send):
        send_lead(send).wait_recv()
        multiply(send)

    def turn_raw():
        gather_finish(count, raw_piece, gathered_raw, total_raw, raw_copies)
        left = jnp.logical_or(keep_peer % 2 == 1, keep_peer == 0)
        prepare(total_raw, jnp.logical_not(left), left, left)

        def body(index):
            source = pl.ds(pl.multiple_of(index * step, step), step)
            send = SENDS - RAW + index
            keep_land[at(send), :] = dot_three(
                split(raw[source, :block]), (high[0], low[0]), 1
            ) + dot_three(split(raw[source, block:]), (high[1], low[1]), 1)
            multiply(send)

        loop(0, RAW, body)

    def hand_over():
        loop(0, sent - 1, lambda send: send_lead(send).wait_send())

        @pl.when(signals)
        def _():
            pl.semaphore_signal(
                go_sem, inc=1, device_id={"pairs": core_peer}, device_id_type=MESH
            )

    def relay():
        pairs_copy(mine, passed, pass_send, pass_recv, keep_peer).wait_recv()
        gather_start(count, passed, gathered_lead, more_send, more_recv)

    def prepare(total, flip, takes_first, own_out):
        scales = unpack(total, coupling)
        identity = identity_of(block)
        couple(rows_all, scales, coupling, identity)
        value = coupling[...]
        coupling[...] = jnp.where(flip, value.T, value)
        value = coupling[...]
        invert_fixed(exact_dot(value, value, 1, 1), inverse, residual, identity)
        straight = 2.0 * inverse[...] - identity
        sign = jnp.where(takes_first, -2.0, 2.0)
        crossed = sign * exact_dot(coupling[...], inverse[...], 0)
        own = jnp.where(own_out, straight, crossed)
        landed = jnp.where(own_out, crossed, straight)
        high[0], low[0] = split(own)
        high[1], low[1] = split(landed)

    def finish(out, own, landed, chunk):
        where = at(chunk * group, group)
        out[where, :] = dot_three(split(own[where, :]), (high[0], low[0]), 1) + dot_three(
            split(landed[where, :]), (high[1], low[1]), 1
        )

    def finish_lead():
        gather_finish(count, passed, gathered_lead, total_lead, rest)
        prepare(
            total_lead,
            position == 0,
            jnp.logical_or(even, position == length - 1),
            position == 0,
        )

        def last(chunk):
            for offset in range(group):
                send_keep(chunk * group + offset).wait_recv()
            finish(out_lead, lead, lead_land, chunk)

        loop(0, CHUNKS, last)

    rest = [
        rows_copy(
            passed, gathered_lead.at[far], more_send.at[far], more_recv.at[far],
            lax.rem(me + far, count),
        )
        for far in range(1, count)
    ]
    raw_copies = [
        rows_copy(
            raw_piece, gathered_raw.at[far], raw_send.at[far], raw_recv.at[far],
            lax.rem(me + far, count),
        )
        for far in range(1, count)
    ]
    turn(0)
    cross[...] = jnp.zeros_like(cross)
    norms[...] = jnp.zeros_like(norms)
    pl.semaphore_wait(barrier, count + 2)
    send(0)

    @pl.when(jnp.logical_not(near_keep))
    def _():
        for copy in raw_copies:
            copy.start()

    loop(1, CHUNKS, turn_and_send)

    @pl.when(jnp.logical_not(near_keep))
    def _():
        turn_raw()

    loop(0, landing - 1, take)

    @pl.when(jnp.logical_not(near_keep))
    def _():
        hand_over()
        pl.semaphore_wait(go_sem, 1)
        loop(0, EARLY, lambda send: send_keep(send).start())

    @pl.when(near_lead)
    def _():
        relay()

    take(landing - 1)
    pack(count, cross, norms, part)
    copies = scatter_sum(count, part, recv, mine, sum_send, sum_recv)
    piece = pairs_copy(mine, passed, pass_send, pass_recv, keep_peer)
    piece.start()
    more = gather_start(count, mine, gathered, all_send, all_recv)

    @pl.when(jnp.logical_not(near_keep))
    def _():
        loop(EARLY, SENDS, lambda send: send_keep(send).start())

    @pl.when(near_keep)
    def _():
        hand_over()

    @pl.when(near_lead)
    def _():
        finish_lead()

    gather_finish(count, mine, gathered, total_keep, more)
    prepare(
        total_keep,
        position != 1,
        jnp.logical_and(jnp.logical_not(even), position != 1),
        position == 1,
    )
    loop(0, CHUNKS, lambda chunk: finish(out_keep, keep, keep_land, chunk))

    @pl.when(jnp.logical_not(near_lead))
    def _():
        relay()
        finish_lead()

    for copy in copies + more + rest + [piece]:
        copy.wait_send()
    send_lead(sent - 1).wait_send()

    @pl.when(jnp.logical_not(near_keep))
    def _():
        for copy in raw_copies:
            copy.wait_send()

    loop(0, SENDS, lambda send: send_keep(send).wait_send())


def exchange(rows_all, matrix, rotation, raw, raw_piece):
    rows, cols = matrix.shape
    block = cols // 2
    count = lax.axis_size("rows")
    length = lax.axis_size("pairs")
    vmem = pl.BlockSpec(memory_space=pltpu.VMEM)
    slot = raw_piece.shape
    pieces = pltpu.VMEM((count,) + slot, F32)
    return pl.pallas_call(
        functools.partial(exchange_kernel, rows_all, count, length),
        out_shape=[jax.ShapeDtypeStruct((rows, block), F32)] * 2,
        in_specs=[vmem] * 5,
        out_specs=[vmem] * 2,
        scratch_shapes=[pltpu.VMEM((rows, block), F32)] * 4
        + [pieces] * 2
        + [pltpu.VMEM((block, block), F32), pltpu.VMEM((8, block // 2), F32)]
        + [pieces] * 2
        + [pltpu.VMEM(slot, F32), pieces, pltpu.VMEM(slot, F32)]
        + [pieces] * 3
        + [pltpu.VMEM((block, block), F32)] * 3
        + [pltpu.VMEM((2, block, block), BF16)] * 2
        + [DMA((SENDS,))] * 4
        + [DMA((count,))] * 4
        + [DMA(()), DMA(())]
        + [DMA((count,))] * 4
        + [pltpu.SemaphoreType.REGULAR],
        name="exchange",
        compiler_params=pltpu.CompilerParams(
            collective_id=1, has_side_effects=True, vmem_limit_bytes=32 * 2**20
        ),
    )(matrix, *rotation, raw, raw_piece)


def identity_of(block):
    row = lax.broadcasted_iota(jnp.int32, (block, block), 0)
    col = lax.broadcasted_iota(jnp.int32, (block, block), 1)
    return jnp.where(row == col, 1.0, 0.0).astype(F32)


def couple(rows_all, norms, cross, identity):
    scales = lax.rsqrt(norms / rows_all + 1e-06)
    scale_first = jnp.sum(identity * scales[0:1, :], axis=1, keepdims=True)
    cross[...] = 0.5 * cross[...] * scale_first * scales[1:2, :] / rows_all


def invert(grams, inverses, residuals, identity):
    block = identity.shape[0]
    spreads = [jnp.max(jnp.sum(jnp.abs(gram), axis=1, keepdims=True)) for gram in grams]
    for gram, spread, inverse, residual in zip(grams, spreads, inverses, residuals):
        start = 2.0 / (2.0 + spread)
        first = (1.0 - start) * identity - start * gram
        inverse[...] = start * (identity + first)
        residual[...] = exact_dot(first, first)
    spread = functools.reduce(jnp.maximum, spreads)
    bound = spread / (2.0 + spread)

    def grow(state):
        limit, trips = state
        for inverse, residual in zip(inverses, residuals):
            both = exact_dot(jnp.concatenate([inverse[...], residual[...]], axis=0), residual[...])
            inverse[...] += both[:block]
            residual[...] = both[block:]
        return limit * limit, trips + 1

    lax.while_loop(
        lambda state: jnp.logical_and(state[0] > 1e-07, state[1] < 30),
        grow,
        (bound * bound, jnp.int32(0)),
    )

    def correct(index, carry):
        for gram, inverse, residual in zip(grams, inverses, residuals):
            guess = inverse[...]
            residual[...] = identity - guess - exact_dot(gram, guess)
            inverse[...] = guess + exact_dot(guess, residual[...])
        return carry

    lax.fori_loop(0, jnp.where(spread > 32.0, 4, 0), correct, 0)


def rotation_kernel(rows_all, total, rot_high, rot_low, coupling, inverse, residual):
    block = coupling.shape[0]
    norms = unpack(total, coupling)
    identity = identity_of(block)
    couple(rows_all, norms, coupling, identity)
    turn = coupling[...]
    gram = exact_dot(turn, turn, 1, 1)
    invert([gram], [inverse], [residual], identity)
    upper = exact_dot(inverse[...], turn)
    lower = exact_dot(turn, upper, 0)
    parts = (
        (0, 0, 2.0 * inverse[...] - identity),
        (0, 1, 2.0 * upper),
        (1, 0, -2.0 * upper.T),
        (1, 1, identity - 2.0 * lower),
    )
    for down, across, value in parts:
        high, low = split(value)
        where = (pl.ds(down * block, block), pl.ds(across * block, block))
        rot_high[where] = high
        rot_low[where] = low


def rotation_of(total, rows_all):
    block = 2 * total.shape[2]
    vmem = pl.BlockSpec(memory_space=pltpu.VMEM)
    return pl.pallas_call(
        functools.partial(rotation_kernel, rows_all),
        out_shape=[jax.ShapeDtypeStruct((2 * block, 2 * block), BF16)] * 2,
        in_specs=[vmem],
        out_specs=[vmem, vmem],
        scratch_shapes=[pltpu.VMEM((block, block), F32)] * 3,
        name="rotation",
        compiler_params=pltpu.CompilerParams(vmem_limit_bytes=16 * 2**20),
    )(total)


def store_kernel(keep, lead, out, sems):
    rows, block = lead.shape
    step = rows // STORES
    odd = lax.axis_index("pairs") % 2

    def store(chunk, index):
        column = jnp.where(odd == index, block, 0)
        at = pl.ds(chunk * step, step)
        return pltpu.make_async_copy(
            (keep, lead)[index].at[at],
            out.at[at, pl.ds(pl.multiple_of(column, block), block)],
            sems.at[index, chunk],
        )

    copies = [store(chunk, index) for chunk in range(STORES) for index in range(2)]
    for copy in copies:
        copy.start()
    for copy in copies:
        copy.wait()


def store(keep, lead):
    rows, block = lead.shape
    vmem = pl.BlockSpec(memory_space=pltpu.VMEM)
    return pl.pallas_call(
        store_kernel,
        out_shape=jax.ShapeDtypeStruct((rows, 2 * block), F32),
        in_specs=[vmem] * 2,
        out_specs=pl.BlockSpec(memory_space=pl.ANY),
        scratch_shapes=[DMA((2, STORES))],
        name="store",
        compiler_params=pltpu.CompilerParams(vmem_limit_bytes=16 * 2**20),
    )(keep, lead)


def shards(matrix):
    rows_all = matrix.shape[0] * lax.axis_size("rows")
    total, loaded, raw, raw_piece = products(pltpu.with_memory_space_constraint(matrix, pltpu.HBM))
    rotation = rotation_of(total, rows_all)
    return store(*exchange(rows_all, loaded, rotation, raw, raw_piece))


def solution(mesh):
    return jax.shard_map(
        shards,
        mesh=mesh,
        in_specs=(P("rows", "pairs"),),
        out_specs=P("rows", "pairs"),
        check_vma=False,
    )
```

```python
import functools

import jax
import jax.numpy as jnp
from jax import lax
from jax.experimental import pallas as pl
from jax.experimental.pallas import tpu as pltpu
from jax.sharding import PartitionSpec as P

LOADS = 4
CHUNKS = 8
SENDS = 16
OUTS = 4
EARLY = 6
RAW = 8
RAW_FIRST = 3
STORES = 4
F32 = jnp.float32
BF16 = jnp.bfloat16
MESH = pl.DeviceIdType.MESH
DMA = pltpu.SemaphoreType.DMA


def split(value):
    high = value.astype(BF16)
    return high, (value - high.astype(F32)).astype(BF16)


def dot_bf16(left, right, left_dim):
    return lax.dot_general(
        left, right, (((left_dim,), (0,)), ((), ())), preferred_element_type=F32
    )


def dot_three(left, right, left_dim):
    return (
        dot_bf16(left[0], right[1], left_dim)
        + dot_bf16(left[1], right[0], left_dim)
        + dot_bf16(left[0], right[0], left_dim)
    )


def exact_dot(left, right, left_dim=1, right_dim=0):
    return lax.dot_general(
        left,
        right,
        (((left_dim,), (right_dim,)), ((), ())),
        precision=lax.Precision.HIGHEST,
        preferred_element_type=F32,
    )


def rows_copy(src, dst, send, recv, peer):
    return pltpu.make_async_remote_copy(
        src_ref=src,
        dst_ref=dst,
        send_sem=send,
        recv_sem=recv,
        device_id={"rows": peer},
        device_id_type=MESH,
    )


def pairs_copy(src, dst, send, recv, peer):
    return pltpu.make_async_remote_copy(
        src_ref=src,
        dst_ref=dst,
        send_sem=send,
        recv_sem=recv,
        device_id={"pairs": peer},
        device_id_type=MESH,
    )


def greet(barrier, axis, peer):
    pl.semaphore_signal(barrier, inc=1, device_id={axis: peer}, device_id_type=MESH)


def partners(position, length):
    even = position % 2 == 0
    down = jnp.where(position == 0, 1, position - 2)
    up = jnp.where(position == length - 1, length - 2, position + 2)
    lead = jnp.where(even, down, up)
    down = jnp.where(position == 1, 0, position - 2)
    up = jnp.where(position == length - 2, length - 1, position + 2)
    keep = jnp.where(even, up, down)
    return lead, keep


def add_norms(norms, first, second):
    half = norms.shape[1]
    for row, value in ((0, first), (1, second)):
        sums = jnp.sum(value * value, axis=0, keepdims=True)
        norms[row : row + 1, :] += sums[:, :half]
        norms[row + 4 : row + 5, :] += sums[:, half:]


def pack(count, cross, norms, part):
    block = cross.shape[0]
    share = block // count
    half = block // 2
    for slot in range(count):
        part[slot, :share, :] = cross[slot * share : (slot + 1) * share, :half]
        part[slot, share : 2 * share, :] = cross[slot * share : (slot + 1) * share, half:]
        part[slot, 2 * share : 2 * share + 8, :] = norms[...]


def unpack(total, cross):
    count, depth, half = total.shape
    share = (depth - 8) // 2
    for slot in range(count):
        cross[slot * share : (slot + 1) * share, :half] = total[slot, :share, :]
        cross[slot * share : (slot + 1) * share, half:] = total[slot, share : 2 * share, :]
    norms = total[0, 2 * share :, :]
    return jnp.concatenate([norms[0:4], norms[4:8]], axis=1)


def scatter_sum(count, part, recv, mine, send_sems, recv_sems):
    me = lax.axis_index("rows")
    copies = []
    for far in range(1, count):
        peer = lax.rem(me + far, count)
        copy = rows_copy(part.at[peer], recv.at[far], send_sems.at[far], recv_sems.at[far], peer)
        copy.start()
        copies.append(copy)
    acc = part[me]
    for far in range(1, count):
        copies[far - 1].wait_recv()
        acc = acc + recv[far]
    mine[...] = acc
    return copies


def gather_start(count, mine, gathered, send_sems, recv_sems):
    me = lax.axis_index("rows")
    copies = []
    for far in range(1, count):
        peer = lax.rem(me + far, count)
        copy = rows_copy(mine, gathered.at[far], send_sems.at[far], recv_sems.at[far], peer)
        copy.start()
        copies.append(copy)
    return copies


def gather_finish(count, mine, gathered, total, copies):
    me = lax.axis_index("rows")
    total[me] = mine[...]
    for far in range(1, count):
        copies[far - 1].wait_recv()
        total[lax.rem(me + count - far, count)] = gathered[far]


def invert_fixed(gram, inverse, residual, identity):
    block = identity.shape[0]
    largest = 0.25 * block * block
    ratio, trips = largest / (2.0 + largest), 0
    while ratio > 0.05:
        ratio, trips = ratio * ratio / (2.0 - ratio * ratio), trips + 1
    sums = jnp.sum(jnp.abs(gram), axis=1, keepdims=True)
    spread = jnp.max(sums, axis=0, keepdims=True)
    start = 2.0 / (2.0 + spread)
    inverse[...] = start * identity
    residual[...] = (1.0 - start) * identity - start * gram

    def grow(index, ratio):
        square = ratio * ratio
        scale = 2.0 / (2.0 - square)
        power = split(residual[...])
        more = dot_three(split(inverse[...]), power, 1)
        inverse[...] = scale * (inverse[...] + more)
        residual[...] = (1.0 - scale) * identity + scale * dot_three(power, power, 1)
        return square / (2.0 - square)

    lax.fori_loop(0, trips, grow, spread / (2.0 + spread))

    def correct(index, carry):
        guess = inverse[...]
        error = identity - guess - exact_dot(gram, guess)
        inverse[...] = guess + dot_three(split(guess), split(error), 1)
        return carry

    lax.fori_loop(0, 2, correct, 0)


def identity_of(block):
    row = lax.broadcasted_iota(jnp.int32, (block, block), 0)
    col = lax.broadcasted_iota(jnp.int32, (block, block), 1)
    return jnp.where(row == col, 1.0, 0.0).astype(F32)


def couple(rows_all, norms, cross, identity):
    scales = lax.rsqrt(norms / rows_all + 1e-06)
    scale_first = jnp.sum(identity * scales[0:1, :], axis=1, keepdims=True)
    cross[...] = 0.5 * cross[...] * scale_first * scales[1:2, :] / rows_all


def sweep_kernel(
    rows_all, count, length, matrix, out_keep, out_lead,
    loaded, raw, lead, keep, lead_land, keep_land,
    cross, norms, part, recv, mine, gathered, total,
    cross_two, norms_two, part_two, recv_two, mine_two, gathered_two, total_keep,
    passed, gathered_lead, total_lead, raw_piece, gathered_raw, total_raw,
    coupling, inverse, residual, high, low, rot_high, rot_low,
    load_sem, lead_send, lead_recv, keep_send, keep_recv, raw_send, raw_recv,
    sum_send, sum_recv, all_send, all_recv, sum_two_send, sum_two_recv, all_two_send, all_two_recv,
    more_send, more_recv, rest_send, rest_recv,
    pass_send, pass_recv, piece_send, piece_recv, go_sem,
):
    rows, cols = loaded.shape
    block = cols // 2
    step = rows // SENDS
    group = SENDS // CHUNKS
    me = lax.axis_index("rows")
    position = lax.axis_index("pairs")
    lead_peer, keep_peer = partners(position, length)
    core_peer = position + 1 - 2 * (position % 2)
    near_keep = keep_peer == core_peer
    near_lead = lead_peer == core_peer
    far_keep = jnp.logical_not(near_keep)
    far_lead = jnp.logical_not(near_lead)
    even = position % 2 == 0
    left_leads = jnp.logical_or(position % 2 == 1, position == 0)
    signals = jnp.logical_and(position > 0, position < length - 1)
    sent = jnp.where(near_lead, SENDS, SENDS - RAW)
    landing = jnp.where(near_keep, SENDS, SENDS - RAW)

    def at(send, sends=1):
        return pl.ds(pl.multiple_of(send * step, step), sends * step)

    def load(chunk):
        where = at(chunk * (SENDS // LOADS), SENDS // LOADS)
        return pltpu.make_async_copy(matrix.at[where], loaded.at[where], load_sem.at[chunk])

    def send_raw(index):
        return pairs_copy(
            matrix.at[at(SENDS - RAW + index)], raw.at[at(index)],
            raw_send.at[index], raw_recv.at[index], lead_peer,
        )

    def send_lead(send):
        return pairs_copy(
            lead.at[at(send)], keep_land.at[at(send)],
            lead_send.at[send], lead_recv.at[send], lead_peer,
        )

    def send_keep(send):
        return pairs_copy(
            keep.at[at(send)], lead_land.at[at(send)],
            keep_send.at[send], keep_recv.at[send], keep_peer,
        )

    def loop(begin, end, do):
        def body(index, carry):
            do(index)
            return carry

        lax.fori_loop(begin, end, body, 0)

    def relay_copies(source, target, send_sems, recv_sems):
        return [
            rows_copy(
                source, target.at[far], send_sems.at[far], recv_sems.at[far],
                lax.rem(me + far, count),
            )
            for far in range(1, count)
        ]

    piece = pairs_copy(mine, raw_piece, piece_send, piece_recv, lead_peer)
    piece_two = pairs_copy(mine_two, passed, pass_send, pass_recv, keep_peer)
    raw_copies = relay_copies(raw_piece, gathered_raw, rest_send, rest_recv)
    lead_copies = relay_copies(passed, gathered_lead, more_send, more_recv)

    def turn(chunk):
        where = at(chunk * group, group)
        turned = dot_three(split(loaded[where, :]), (rot_high[...], rot_low[...]), 1)
        left, right = turned[:, :block], turned[:, block:]
        lead[where, :] = jnp.where(left_leads, left, right)
        keep[where, :] = jnp.where(left_leads, right, left)
        for offset in range(group):
            send = chunk * group + offset

            @pl.when(send < sent)
            def _():
                send_lead(send).start()

            @pl.when(near_keep)
            def _():
                send_keep(send).start()

    def multiply(chunk):
        where = at(chunk * group, group)
        ours, theirs = keep[where, :], keep_land[where, :]
        cross_two[...] += dot_three(split(ours), split(theirs), 0)
        add_norms(norms_two, ours, theirs)

    def take(chunk):
        for offset in range(group):
            send_lead(chunk * group + offset).wait_recv()
        multiply(chunk)

    def hand_over():
        loop(0, sent - 1, lambda send: send_lead(send).wait_send())

        @pl.when(signals)
        def _():
            pl.semaphore_signal(
                go_sem, inc=1, device_id={"pairs": core_peer}, device_id_type=MESH
            )

    def relay_lead():
        piece_two.wait_recv()
        for copy in lead_copies:
            copy.start()

    def couple_and_invert(sums, flip):
        scales = unpack(sums, coupling)
        identity = identity_of(block)
        couple(rows_all, scales, coupling, identity)
        if flip is not None:
            value = coupling[...]
            coupling[...] = jnp.where(flip, value.T, value)
        value = coupling[...]
        invert_fixed(exact_dot(value, value, 1, 1), inverse, residual, identity)
        return 2.0 * inverse[...] - identity, identity

    def prepare_both():
        straight, identity = couple_and_invert(total, None)
        upper = exact_dot(inverse[...], coupling[...])
        lower = exact_dot(coupling[...], upper, 0)
        parts = (
            (0, 0, straight),
            (0, 1, 2.0 * upper),
            (1, 0, -2.0 * upper.T),
            (1, 1, identity - 2.0 * lower),
        )
        for down, across, value in parts:
            where = (pl.ds(down * block, block), pl.ds(across * block, block))
            rot_high[where], rot_low[where] = split(value)

    def prepare(sums, flip, takes_first, own_out):
        straight, identity = couple_and_invert(sums, flip)
        sign = jnp.where(takes_first, -2.0, 2.0)
        crossed = sign * exact_dot(coupling[...], inverse[...], 0)
        own = jnp.where(own_out, straight, crossed)
        landed = jnp.where(own_out, crossed, straight)
        high[0], low[0] = split(own)
        high[1], low[1] = split(landed)

    def turn_raw():
        gather_finish(count, raw_piece, gathered_raw, total_raw, raw_copies)
        left = jnp.logical_or(keep_peer % 2 == 1, keep_peer == 0)
        prepare(total_raw, jnp.logical_not(left), left, left)

        def body(chunk):
            for offset in range(group):
                send_raw(chunk * group + offset).wait_recv()
            source = at(chunk * group, group)
            keep_land[at(SENDS - RAW + chunk * group, group), :] = dot_three(
                split(raw[source, :block]), (high[0], low[0]), 1
            ) + dot_three(split(raw[source, block:]), (high[1], low[1]), 1)
            multiply(CHUNKS - RAW // group + chunk)

        loop(0, RAW // group, body)

    def finish(out, own, landed, chunk):
        where = at(chunk * (SENDS // OUTS), SENDS // OUTS)
        out[where, :] = dot_three(split(own[where, :]), (high[0], low[0]), 1) + dot_three(
            split(landed[where, :]), (high[1], low[1]), 1
        )

    def finish_lead():
        gather_finish(count, passed, gathered_lead, total_lead, lead_copies)
        prepare(
            total_lead,
            position == 0,
            jnp.logical_or(even, position == length - 1),
            position == 0,
        )

        def last(chunk):
            for offset in range(SENDS // OUTS):
                send_keep(chunk * (SENDS // OUTS) + offset).wait_recv()
            finish(out_lead, lead, lead_land, chunk)

        loop(0, OUTS, last)

    for chunk in range(LOADS):
        load(chunk).start()
    barrier = pltpu.get_barrier_semaphore()
    for far in range(1, count):
        greet(barrier, "rows", lax.rem(me + far, count))
    for peer in (lead_peer, keep_peer, core_peer):
        greet(barrier, "pairs", peer)
    for ref in (cross, norms, cross_two, norms_two):
        ref[...] = jnp.zeros_like(ref)
    pl.semaphore_wait(barrier, count + 2)

    @pl.when(far_lead)
    def _():
        loop(0, RAW_FIRST, lambda index: send_raw(index).start())

    def take_first(chunk):
        where = at(chunk * (SENDS // LOADS), SENDS // LOADS)
        load(chunk).wait()
        first, second = loaded[where, :block], loaded[where, block:]
        cross[...] += dot_three(split(first), split(second), 0)
        add_norms(norms, first, second)

    loop(0, LOADS, take_first)
    pack(count, cross, norms, part)
    sums = scatter_sum(count, part, recv, mine, sum_send, sum_recv)

    @pl.when(far_lead)
    def _():
        piece.start()
        loop(RAW_FIRST, RAW, lambda index: send_raw(index).start())

    alls = gather_start(count, mine, gathered, all_send, all_recv)

    @pl.when(far_keep)
    def _():
        piece.wait_recv()
        for copy in raw_copies:
            copy.start()

    gather_finish(count, mine, gathered, total, alls)
    prepare_both()
    loop(0, CHUNKS, turn)

    @pl.when(far_keep)
    def _():
        turn_raw()

    loop(0, landing // group - 1, take)

    @pl.when(far_keep)
    def _():
        hand_over()
        pl.semaphore_wait(go_sem, 1)
        loop(0, EARLY, lambda send: send_keep(send).start())

    @pl.when(near_lead)
    def _():
        relay_lead()

    take(landing // group - 1)
    pack(count, cross_two, norms_two, part_two)
    sums += scatter_sum(count, part_two, recv_two, mine_two, sum_two_send, sum_two_recv)
    piece_two.start()
    alls_two = gather_start(count, mine_two, gathered_two, all_two_send, all_two_recv)

    @pl.when(far_keep)
    def _():
        loop(EARLY, SENDS, lambda send: send_keep(send).start())

    @pl.when(near_keep)
    def _():
        hand_over()

    @pl.when(near_lead)
    def _():
        finish_lead()

    gather_finish(count, mine_two, gathered_two, total_keep, alls_two)
    prepare(
        total_keep,
        position != 1,
        jnp.logical_and(jnp.logical_not(even), position != 1),
        position == 1,
    )
    loop(0, OUTS, lambda chunk: finish(out_keep, keep, keep_land, chunk))

    @pl.when(far_lead)
    def _():
        relay_lead()
        finish_lead()

    for copy in sums + alls + alls_two + lead_copies + [piece_two]:
        copy.wait_send()
    send_lead(sent - 1).wait_send()

    @pl.when(far_keep)
    def _():
        for copy in raw_copies:
            copy.wait_send()

    @pl.when(far_lead)
    def _():
        piece.wait_send()
        loop(0, RAW, lambda index: send_raw(index).wait_send())

    loop(0, SENDS, lambda send: send_keep(send).wait_send())


def sweep(matrix):
    rows, cols = matrix.shape
    block = cols // 2
    count = lax.axis_size("rows")
    length = lax.axis_size("pairs")
    shape = (2 * (block // count) + 8, block // 2)
    slot, slots = pltpu.VMEM(shape, F32), pltpu.VMEM((count,) + shape, F32)
    square = pltpu.VMEM((block, block), F32)
    sums = [square, pltpu.VMEM((8, block // 2), F32), slots, slots, slot, slots, slots]
    vmem = pl.BlockSpec(memory_space=pltpu.VMEM)
    return pl.pallas_call(
        functools.partial(sweep_kernel, rows * count, count, length),
        out_shape=[jax.ShapeDtypeStruct((rows, block), F32)] * 2,
        in_specs=[pl.BlockSpec(memory_space=pltpu.HBM)],
        out_specs=[vmem] * 2,
        scratch_shapes=[pltpu.VMEM((rows, cols), F32)]
        + [pltpu.VMEM((RAW * (rows // SENDS), cols), F32)]
        + [pltpu.VMEM((rows, block), F32)] * 4
        + sums * 2
        + [slot, slots, slots] * 2
        + [square] * 3
        + [pltpu.VMEM((2, block, block), BF16)] * 2
        + [pltpu.VMEM((cols, cols), BF16)] * 2
        + [DMA((LOADS,))]
        + [DMA((SENDS,))] * 4
        + [DMA((RAW,))] * 2
        + [DMA((count,))] * 12
        + [DMA(())] * 4
        + [pltpu.SemaphoreType.REGULAR],
        name="sweep",
        compiler_params=pltpu.CompilerParams(
            collective_id=0, has_side_effects=True, vmem_limit_bytes=40 * 2**20
        ),
    )(pltpu.with_memory_space_constraint(matrix, pltpu.HBM))


def store_kernel(keep, lead, out, sems):
    rows, block = lead.shape
    step = rows // STORES
    odd = lax.axis_index("pairs") % 2

    def store(chunk, index):
        column = jnp.where(odd == index, block, 0)
        at = pl.ds(chunk * step, step)
        return pltpu.make_async_copy(
            (keep, lead)[index].at[at],
            out.at[at, pl.ds(pl.multiple_of(column, block), block)],
            sems.at[index, chunk],
        )

    copies = [store(chunk, index) for chunk in range(STORES) for index in range(2)]
    for copy in copies:
        copy.start()
    for copy in copies:
        copy.wait()


def store(keep, lead):
    rows, block = lead.shape
    vmem = pl.BlockSpec(memory_space=pltpu.VMEM)
    return pl.pallas_call(
        store_kernel,
        out_shape=jax.ShapeDtypeStruct((rows, 2 * block), F32),
        in_specs=[vmem] * 2,
        out_specs=pl.BlockSpec(memory_space=pl.ANY),
        scratch_shapes=[DMA((2, STORES))],
        name="store",
        compiler_params=pltpu.CompilerParams(vmem_limit_bytes=16 * 2**20),
    )(keep, lead)


def shards(matrix):
    return store(*sweep(matrix))


def solution(mesh):
    return jax.shard_map(
        shards,
        mesh=mesh,
        in_specs=(P("rows", "pairs"),),
        out_specs=P("rows", "pairs"),
        check_vma=False,
    )
```

```python
import functools

import jax
import jax.numpy as jnp
from jax import lax
from jax.experimental import pallas as pl
from jax.experimental.pallas import tpu as pltpu
from jax.sharding import PartitionSpec as P

LOADS = 4
CHUNKS = 8
SENDS = 16
OUTS = 4
EARLY = 5
RAW = 8
RAW_FIRST = 3
F32 = jnp.float32
BF16 = jnp.bfloat16
MESH = pl.DeviceIdType.MESH
DMA = pltpu.SemaphoreType.DMA


def split(value):
    high = value.astype(BF16)
    return high, (value - high.astype(F32)).astype(BF16)


def dot_bf16(left, right, left_dim):
    return lax.dot_general(
        left, right, (((left_dim,), (0,)), ((), ())), preferred_element_type=F32
    )


def dot_three(left, right, left_dim):
    return (
        dot_bf16(left[0], right[1], left_dim)
        + dot_bf16(left[1], right[0], left_dim)
        + dot_bf16(left[0], right[0], left_dim)
    )


def exact_dot(left, right, left_dim=1, right_dim=0):
    return lax.dot_general(
        left,
        right,
        (((left_dim,), (right_dim,)), ((), ())),
        precision=lax.Precision.HIGHEST,
        preferred_element_type=F32,
    )


def rows_copy(src, dst, send, recv, peer):
    return pltpu.make_async_remote_copy(
        src_ref=src,
        dst_ref=dst,
        send_sem=send,
        recv_sem=recv,
        device_id={"rows": peer},
        device_id_type=MESH,
    )


def pairs_copy(src, dst, send, recv, peer):
    return pltpu.make_async_remote_copy(
        src_ref=src,
        dst_ref=dst,
        send_sem=send,
        recv_sem=recv,
        device_id={"pairs": peer},
        device_id_type=MESH,
    )


def greet(barrier, axis, peer):
    pl.semaphore_signal(barrier, inc=1, device_id={axis: peer}, device_id_type=MESH)


def partners(position, length):
    even = position % 2 == 0
    down = jnp.where(position == 0, 1, position - 2)
    up = jnp.where(position == length - 1, length - 2, position + 2)
    lead = jnp.where(even, down, up)
    down = jnp.where(position == 1, 0, position - 2)
    up = jnp.where(position == length - 2, length - 1, position + 2)
    keep = jnp.where(even, up, down)
    return lead, keep


def add_norms(norms, first, second):
    half = norms.shape[1]
    for row, value in ((0, first), (1, second)):
        sums = jnp.sum(value * value, axis=0, keepdims=True)
        norms[row : row + 1, :] += sums[:, :half]
        norms[row + 4 : row + 5, :] += sums[:, half:]


def pack(count, cross, norms, part):
    block = cross.shape[0]
    share = block // count
    half = block // 2
    for slot in range(count):
        part[slot, :share, :] = cross[slot * share : (slot + 1) * share, :half]
        part[slot, share : 2 * share, :] = cross[slot * share : (slot + 1) * share, half:]
        part[slot, 2 * share : 2 * share + 8, :] = norms[...]


def unpack(total, cross):
    count, depth, half = total.shape
    share = (depth - 8) // 2
    for slot in range(count):
        cross[slot * share : (slot + 1) * share, :half] = total[slot, :share, :]
        cross[slot * share : (slot + 1) * share, half:] = total[slot, share : 2 * share, :]
    norms = total[0, 2 * share :, :]
    return jnp.concatenate([norms[0:4], norms[4:8]], axis=1)


def scatter_start(count, part, recv, send_sems, recv_sems):
    me = lax.axis_index("rows")
    copies = []
    for far in range(1, count):
        peer = lax.rem(me + far, count)
        copy = rows_copy(part.at[peer], recv.at[far], send_sems.at[far], recv_sems.at[far], peer)
        copy.start()
        copies.append(copy)
    return copies


def scatter_finish(count, part, recv, mine, copies):
    acc = part[lax.axis_index("rows")]
    for far in range(1, count):
        copies[far - 1].wait_recv()
        acc = acc + recv[far]
    mine[...] = acc


def gather_start(count, mine, gathered, send_sems, recv_sems):
    me = lax.axis_index("rows")
    copies = []
    for far in range(1, count):
        peer = lax.rem(me + far, count)
        copy = rows_copy(mine, gathered.at[far], send_sems.at[far], recv_sems.at[far], peer)
        copy.start()
        copies.append(copy)
    return copies


def gather_finish(count, mine, gathered, total, copies):
    me = lax.axis_index("rows")
    total[me] = mine[...]
    for far in range(1, count):
        copies[far - 1].wait_recv()
        total[lax.rem(me + count - far, count)] = gathered[far]


def invert_fixed(gram, inverse, residual, identity):
    block = identity.shape[0]
    largest = 0.25 * block * block
    ratio, trips = largest / (2.0 + largest), 0
    while ratio > 0.01:
        ratio, trips = ratio * ratio / (2.0 - ratio * ratio), trips + 1
    sums = jnp.sum(jnp.abs(gram), axis=1, keepdims=True)
    spread = jnp.max(sums, axis=0, keepdims=True)
    start = 2.0 / (2.0 + spread)
    inverse[...] = start * identity
    residual[...] = (1.0 - start) * identity - start * gram

    def grow(index, ratio):
        square = ratio * ratio
        scale = 2.0 / (2.0 - square)
        power = split(residual[...])
        more = dot_three(split(inverse[...]), power, 1)
        inverse[...] = scale * (inverse[...] + more)
        residual[...] = (1.0 - scale) * identity + scale * dot_three(power, power, 1)
        return square / (2.0 - square)

    lax.fori_loop(0, trips, grow, spread / (2.0 + spread))

    guess = inverse[...]
    error = identity - guess - exact_dot(gram, guess)
    inverse[...] = guess + dot_three(split(guess), split(error), 1)


def identity_of(block):
    row = lax.broadcasted_iota(jnp.int32, (block, block), 0)
    col = lax.broadcasted_iota(jnp.int32, (block, block), 1)
    return jnp.where(row == col, 1.0, 0.0).astype(F32)


def couple(rows_all, norms, cross, identity):
    scales = lax.rsqrt(norms / rows_all + 1e-06)
    scale_first = jnp.sum(identity * scales[0:1, :], axis=1, keepdims=True)
    cross[...] = 0.5 * cross[...] * scale_first * scales[1:2, :] / rows_all


def two_blocks(own, landed, high, low, place):
    return dot_three(split(own), (high[place, 0], low[place, 0]), 1) + dot_three(
        split(landed), (high[place, 1], low[place, 1]), 1
    )


def sweep_kernel(
    rows_all, count, length, matrix, out, lead, keep, lead_land, keep_land, high, low,
    loaded, raw,
    cross, norms, part, recv, mine, gathered, total,
    cross_two, norms_two, part_two, recv_two, mine_two, gathered_two, total_keep,
    passed, gathered_lead, total_lead, raw_piece, gathered_raw, total_raw,
    coupling, inverse, residual, rot_high, rot_low,
    load_sem, lead_send, lead_recv, keep_send, keep_recv, raw_send, raw_recv,
    sum_send, sum_recv, all_send, all_recv, sum_two_send, sum_two_recv, all_two_send, all_two_recv,
    more_send, more_recv, rest_send, rest_recv,
    pass_send, pass_recv, piece_send, piece_recv, totals_send, totals_recv,
):
    rows, cols = loaded.shape
    block = cols // 2
    step = rows // SENDS
    group = SENDS // CHUNKS
    me = lax.axis_index("rows")
    position = lax.axis_index("pairs")
    lead_peer, keep_peer = partners(position, length)
    core_peer = position + 1 - 2 * (position % 2)
    near_keep = keep_peer == core_peer
    near_lead = lead_peer == core_peer
    far_keep = jnp.logical_not(near_keep)
    far_lead = jnp.logical_not(near_lead)
    even = position % 2 == 0
    left_leads = jnp.logical_or(position % 2 == 1, position == 0)
    sent = jnp.where(near_lead, SENDS, SENDS - RAW)
    landing = SENDS - RAW

    def at(send, sends=1):
        return pl.ds(pl.multiple_of(send * step, step), sends * step)

    def load(chunk):
        where = at(chunk * (SENDS // LOADS), SENDS // LOADS)
        return pltpu.make_async_copy(matrix.at[where], loaded.at[where], load_sem.at[chunk])

    def send_raw(index):
        return pairs_copy(
            matrix.at[at(SENDS - RAW + index)], raw.at[at(index)],
            raw_send.at[index], raw_recv.at[index], lead_peer,
        )

    def send_lead(send):
        return pairs_copy(
            lead.at[at(send)], keep_land.at[at(send)],
            lead_send.at[send], lead_recv.at[send], lead_peer,
        )

    def send_keep(send):
        return pairs_copy(
            keep.at[at(send)], lead_land.at[at(send)],
            keep_send.at[send], keep_recv.at[send], keep_peer,
        )

    def loop(begin, end, do):
        def body(index, carry):
            do(index)
            return carry

        lax.fori_loop(begin, end, body, 0)

    def relay_copies(source, target, send_sems, recv_sems):
        return [
            rows_copy(
                source, target.at[far], send_sems.at[far], recv_sems.at[far],
                lax.rem(me + far, count),
            )
            for far in range(1, count)
        ]

    piece = pairs_copy(mine, raw_piece, piece_send, piece_recv, lead_peer)
    piece_two = pairs_copy(mine_two, passed, pass_send, pass_recv, keep_peer)
    totals = pairs_copy(total_keep, total_lead, totals_send, totals_recv, keep_peer)
    raw_copies = relay_copies(raw_piece, gathered_raw, rest_send, rest_recv)
    lead_copies = relay_copies(passed, gathered_lead, more_send, more_recv)

    def turn(chunk):
        where = at(chunk * group, group)
        turned = dot_three(split(loaded[where, :]), (rot_high[...], rot_low[...]), 1)
        left, right = turned[:, :block], turned[:, block:]
        lead[where, :] = jnp.where(left_leads, left, right)
        keep[where, :] = jnp.where(left_leads, right, left)
        for offset in range(group):
            send = chunk * group + offset

            @pl.when(send < sent)
            def _():
                send_lead(send).start()

            @pl.when(near_keep)
            def _():
                send_keep(send).start()

    def multiply(chunk):
        where = at(chunk * group, group)
        ours, theirs = keep[where, :], keep_land[where, :]
        cross_two[...] += dot_three(split(ours), split(theirs), 0)
        add_norms(norms_two, ours, theirs)

    def take(chunk):
        for offset in range(group):
            send_lead(chunk * group + offset).wait_recv()
        multiply(chunk)

    def couple_and_invert(sums, flip):
        scales = unpack(sums, coupling)
        identity = identity_of(block)
        couple(rows_all, scales, coupling, identity)
        if flip is not None:
            value = coupling[...]
            coupling[...] = jnp.where(flip, value.T, value)
        value = coupling[...]
        invert_fixed(exact_dot(value, value, 1, 1), inverse, residual, identity)
        return 2.0 * inverse[...] - identity, identity

    def prepare_both():
        straight, identity = couple_and_invert(total, None)
        upper = exact_dot(inverse[...], coupling[...])
        lower = exact_dot(coupling[...], upper, 0)
        parts = (
            (0, 0, straight),
            (0, 1, 2.0 * upper),
            (1, 0, -2.0 * upper.T),
            (1, 1, identity - 2.0 * lower),
        )
        for down, across, value in parts:
            where = (pl.ds(down * block, block), pl.ds(across * block, block))
            rot_high[where], rot_low[where] = split(value)

    def prepare(place, sums, flip, takes_first, own_out):
        straight, identity = couple_and_invert(sums, flip)
        sign = jnp.where(takes_first, -2.0, 2.0)
        crossed = sign * dot_three(split(coupling[...]), split(inverse[...]), 0)
        own = jnp.where(own_out, straight, crossed)
        landed = jnp.where(own_out, crossed, straight)
        high[place, 0], low[place, 0] = split(own)
        high[place, 1], low[place, 1] = split(landed)

    def turn_raw():
        gather_finish(count, raw_piece, gathered_raw, total_raw, raw_copies)
        left = jnp.logical_or(keep_peer % 2 == 1, keep_peer == 0)
        prepare(0, total_raw, jnp.logical_not(left), left, left)
        loop(0, RAW, lambda index: send_raw(index).wait_recv())

        def body(chunk):
            source = at(chunk * group, group)
            keep_land[at(landing + chunk * group, group), :] = dot_three(
                split(raw[source, :block]), (high[0, 0], low[0, 0]), 1
            ) + dot_three(split(raw[source, block:]), (high[0, 1], low[0, 1]), 1)
            multiply(landing // group + chunk)

        loop(0, RAW // group, body)

    def prepare_lead(place):
        prepare(
            place,
            total_lead,
            position == 0,
            jnp.logical_or(even, position == length - 1),
            position == 0,
        )
        loop(0, SENDS, lambda send: send_keep(send).wait_recv())

    def finish(own, landed):
        def body(chunk):
            where = at(chunk * (SENDS // OUTS), SENDS // OUTS)
            out[where, :] = two_blocks(own[where, :], landed[where, :], high, low, 0)

        loop(0, OUTS, body)

    for chunk in range(LOADS):
        load(chunk).start()
    barrier = pltpu.get_barrier_semaphore()
    for far in range(1, count):
        greet(barrier, "rows", lax.rem(me + far, count))
    for peer in (lead_peer, keep_peer, core_peer):
        greet(barrier, "pairs", peer)
    for ref in (cross, norms, cross_two, norms_two):
        ref[...] = jnp.zeros_like(ref)

    def take_first(chunk):
        where = at(chunk * (SENDS // LOADS), SENDS // LOADS)
        load(chunk).wait()
        first, second = loaded[where, :block], loaded[where, block:]
        cross[...] += dot_three(split(first), split(second), 0)
        add_norms(norms, first, second)

    loop(0, LOADS, take_first)
    pl.semaphore_wait(barrier, count + 2)

    @pl.when(far_lead)
    def _():
        loop(0, RAW_FIRST, lambda index: send_raw(index).start())

    pack(count, cross, norms, part)
    sums = scatter_start(count, part, recv, sum_send, sum_recv)
    scatter_finish(count, part, recv, mine, sums)

    @pl.when(far_lead)
    def _():
        piece.start()
        loop(RAW_FIRST, RAW, lambda index: send_raw(index).start())

    alls = gather_start(count, mine, gathered, all_send, all_recv)
    gather_finish(count, mine, gathered, total, alls)

    @pl.when(far_keep)
    def _():
        piece.wait_recv()
        for copy in raw_copies:
            copy.start()

    prepare_both()
    loop(0, CHUNKS, turn)

    @pl.when(far_keep)
    def _():
        turn_raw()

    @pl.when(far_keep)
    def _():
        loop(0, landing // group - 1, take)
        send_lead(landing - group).wait_recv()
        loop(0, EARLY, lambda send: send_keep(send).start())
        for offset in range(1, group):
            send_lead(landing - group + offset).wait_recv()
        multiply(landing // group - 1)

    @pl.when(near_keep)
    def _():
        loop(0, CHUNKS, take)

    pack(count, cross_two, norms_two, part_two)
    sums_two = scatter_start(count, part_two, recv_two, sum_two_send, sum_two_recv)
    scatter_finish(count, part_two, recv_two, mine_two, sums_two)

    @pl.when(far_keep)
    def _():
        piece_two.start()

    alls_two = gather_start(count, mine_two, gathered_two, all_two_send, all_two_recv)

    @pl.when(far_keep)
    def _():
        loop(EARLY, SENDS, lambda send: send_keep(send).start())

    @pl.when(near_lead)
    def _():
        totals.wait_recv()
        prepare_lead(0)
        finish(lead, lead_land)

    gather_finish(count, mine_two, gathered_two, total_keep, alls_two)

    @pl.when(near_keep)
    def _():
        totals.start()

    prepare(
        jnp.where(near_lead, 1, 0),
        total_keep,
        position != 1,
        jnp.logical_and(jnp.logical_not(even), position != 1),
        position == 1,
    )

    @pl.when(far_lead)
    def _():
        finish(keep, keep_land)
        piece_two.wait_recv()
        for copy in lead_copies:
            copy.start()
        gather_finish(count, passed, gathered_lead, total_lead, lead_copies)
        prepare_lead(1)
        for copy in lead_copies:
            copy.wait_send()

    for copy in sums + alls + sums_two + alls_two:
        copy.wait_send()

    @pl.when(near_keep)
    def _():
        totals.wait_send()

    @pl.when(far_keep)
    def _():
        piece_two.wait_send()

    loop(0, sent, lambda send: send_lead(send).wait_send())

    @pl.when(far_keep)
    def _():
        for copy in raw_copies:
            copy.wait_send()

    @pl.when(far_lead)
    def _():
        piece.wait_send()
        loop(0, RAW, lambda index: send_raw(index).wait_send())

    loop(0, SENDS, lambda send: send_keep(send).wait_send())


def sweep(matrix):
    rows, cols = matrix.shape
    block = cols // 2
    count = lax.axis_size("rows")
    length = lax.axis_size("pairs")
    shape = (2 * (block // count) + 8, block // 2)
    slot, slots = pltpu.VMEM(shape, F32), pltpu.VMEM((count,) + shape, F32)
    square = pltpu.VMEM((block, block), F32)
    sums = [square, pltpu.VMEM((8, block // 2), F32), slots, slots, slot, slots, slots]
    vmem = pl.BlockSpec(memory_space=pltpu.VMEM)
    return pl.pallas_call(
        functools.partial(sweep_kernel, rows * count, count, length),
        out_shape=[jax.ShapeDtypeStruct((rows, block), F32)] * 5
        + [jax.ShapeDtypeStruct((2, 2, block, block), BF16)] * 2,
        in_specs=[pl.BlockSpec(memory_space=pltpu.HBM)],
        out_specs=[vmem] * 7,
        scratch_shapes=[pltpu.VMEM((rows, cols), F32)]
        + [pltpu.VMEM((RAW * (rows // SENDS), cols), F32)]
        + sums * 2
        + [slot, slots, slots] * 2
        + [square] * 3
        + [pltpu.VMEM((cols, cols), BF16)] * 2
        + [DMA((LOADS,))]
        + [DMA((SENDS,))] * 4
        + [DMA((RAW,))] * 2
        + [DMA((count,))] * 12
        + [DMA(())] * 6,
        name="sweep",
        compiler_params=pltpu.CompilerParams(
            collective_id=0, has_side_effects=True, vmem_limit_bytes=24 * 2**20
        ),
    )(pltpu.with_memory_space_constraint(matrix, pltpu.HBM))


def final_kernel(length, done, lead, keep, lead_land, keep_land, high, low, out, staged, sems):
    rows, block = lead.shape
    step = rows // OUTS
    position = lax.axis_index("pairs")
    near_lead = jnp.logical_or(position == 0, position == length - 1)
    even = position % 2 == 0

    def store(chunk, source, takes_lead, sem):
        column = jnp.where(takes_lead == even, 0, block)
        where = pl.ds(pl.multiple_of(chunk * step, step), step)
        return pltpu.make_async_copy(
            source.at[where],
            out.at[where, pl.ds(pl.multiple_of(column, block), block)],
            sems.at[sem, chunk],
        )

    def loop(do):
        def body(chunk, carry):
            do(chunk)
            return carry

        lax.fori_loop(0, OUTS, body, 0)

    loop(lambda chunk: store(chunk, done, near_lead, 0).start())

    def finish(own, landed):
        def body(chunk):
            where = pl.ds(pl.multiple_of(chunk * step, step), step)
            staged[where, :] = two_blocks(own[where, :], landed[where, :], high, low, 1)
            store(chunk, staged, jnp.logical_not(near_lead), 1).start()

        loop(body)

    @pl.when(near_lead)
    def _():
        finish(keep, keep_land)

    @pl.when(jnp.logical_not(near_lead))
    def _():
        finish(lead, lead_land)

    def drain(chunk):
        store(chunk, done, near_lead, 0).wait()
        store(chunk, staged, near_lead, 1).wait()

    loop(drain)


def final(done, *blocks):
    rows, block = done.shape
    return pl.pallas_call(
        functools.partial(final_kernel, lax.axis_size("pairs")),
        out_shape=jax.ShapeDtypeStruct((rows, 2 * block), F32),
        in_specs=[pl.BlockSpec(memory_space=pltpu.VMEM)] * 7,
        out_specs=pl.BlockSpec(memory_space=pl.ANY),
        scratch_shapes=[pltpu.VMEM((rows, block), F32), DMA((2, OUTS))],
        name="final",
        compiler_params=pltpu.CompilerParams(vmem_limit_bytes=16 * 2**20),
    )(done, *blocks)


def shards(matrix):
    return final(*sweep(matrix))


def solution(mesh):
    return jax.shard_map(
        shards,
        mesh=mesh,
        in_specs=(P("rows", "pairs"),),
        out_specs=P("rows", "pairs"),
        check_vma=False,
    )
```

```python
import functools

import jax
import jax.numpy as jnp
from jax import lax
from jax.experimental import pallas as pl
from jax.experimental.pallas import tpu as pltpu
from jax.sharding import PartitionSpec as P

LOADS = 4
CHUNKS = 8
SENDS = 16
OUTS = 4
EARLY = 7
RAW = 8
RAW_FIRST = 3
F32 = jnp.float32
BF16 = jnp.bfloat16
MESH = pl.DeviceIdType.MESH
DMA = pltpu.SemaphoreType.DMA


def split(value):
    high = value.astype(BF16)
    return high, (value - high.astype(F32)).astype(BF16)


def dot_bf16(left, right, left_dim):
    return lax.dot_general(
        left, right, (((left_dim,), (0,)), ((), ())), preferred_element_type=F32
    )


def dot_three(left, right, left_dim):
    return (
        dot_bf16(left[0], right[1], left_dim)
        + dot_bf16(left[1], right[0], left_dim)
        + dot_bf16(left[0], right[0], left_dim)
    )


def exact_dot(left, right, left_dim=1, right_dim=0):
    return lax.dot_general(
        left,
        right,
        (((left_dim,), (right_dim,)), ((), ())),
        precision=lax.Precision.HIGHEST,
        preferred_element_type=F32,
    )


def rows_copy(src, dst, send, recv, peer):
    return pltpu.make_async_remote_copy(
        src_ref=src,
        dst_ref=dst,
        send_sem=send,
        recv_sem=recv,
        device_id={"rows": peer},
        device_id_type=MESH,
    )


def pairs_copy(src, dst, send, recv, peer):
    return pltpu.make_async_remote_copy(
        src_ref=src,
        dst_ref=dst,
        send_sem=send,
        recv_sem=recv,
        device_id={"pairs": peer},
        device_id_type=MESH,
    )


def greet(barrier, axis, peer):
    pl.semaphore_signal(barrier, inc=1, device_id={axis: peer}, device_id_type=MESH)


def partners(position, length):
    even = position % 2 == 0
    down = jnp.where(position == 0, 1, position - 2)
    up = jnp.where(position == length - 1, length - 2, position + 2)
    lead = jnp.where(even, down, up)
    down = jnp.where(position == 1, 0, position - 2)
    up = jnp.where(position == length - 2, length - 1, position + 2)
    keep = jnp.where(even, up, down)
    return lead, keep


def add_norms(norms, first, second):
    half = norms.shape[1]
    for row, value in ((0, first), (1, second)):
        sums = jnp.sum(value * value, axis=0, keepdims=True)
        norms[row : row + 1, :] += sums[:, :half]
        norms[row + 2 : row + 3, :] += sums[:, half:]


def pack(count, cross, norms, part):
    block = cross.shape[0]
    share = block // count
    half = block // 2
    for slot in range(count):
        part[slot, :share, :] = cross[slot * share : (slot + 1) * share, :half]
        part[slot, share : 2 * share, :] = cross[slot * share : (slot + 1) * share, half:]
        part[slot, 2 * share :, :] = norms[...]


def unpack(total, cross):
    count, depth, half = total.shape
    share = (depth - 4) // 2
    for slot in range(count):
        cross[slot * share : (slot + 1) * share, :half] = total[slot, :share, :]
        cross[slot * share : (slot + 1) * share, half:] = total[slot, share : 2 * share, :]
    norms = total[0, 2 * share :, :]
    return jnp.concatenate([norms[0:2], norms[2:4]], axis=1)


def scatter_start(count, part, recv, send_sems, recv_sems):
    me = lax.axis_index("rows")
    copies = []
    for far in range(1, count):
        peer = lax.rem(me + far, count)
        copy = rows_copy(part.at[peer], recv.at[far], send_sems.at[far], recv_sems.at[far], peer)
        copy.start()
        copies.append(copy)
    return copies


def scatter_finish(count, part, recv, mine, copies):
    acc = part[lax.axis_index("rows")]
    for far in range(1, count):
        copies[far - 1].wait_recv()
        acc = acc + recv[far]
    mine[...] = acc


def gather_start(count, mine, gathered, send_sems, recv_sems):
    me = lax.axis_index("rows")
    copies = []
    for far in range(1, count):
        peer = lax.rem(me + far, count)
        copy = rows_copy(mine, gathered.at[far], send_sems.at[far], recv_sems.at[far], peer)
        copy.start()
        copies.append(copy)
    return copies


def gather_finish(count, mine, gathered, total, copies):
    me = lax.axis_index("rows")
    total[me] = mine[...]
    for far in range(1, count):
        copies[far - 1].wait_recv()
        total[lax.rem(me + count - far, count)] = gathered[far]


def invert_fixed(gram, inverse, residual, identity):
    block = identity.shape[0]
    largest = 0.25 * block * block
    ratio, trips = largest / (2.0 + largest), 0
    while ratio > 0.01:
        ratio, trips = ratio * ratio / (2.0 - ratio * ratio), trips + 1
    sums = jnp.sum(jnp.abs(gram), axis=1, keepdims=True)
    spread = jnp.max(sums, axis=0, keepdims=True)
    start = 2.0 / (2.0 + spread)
    inverse[...] = start * identity
    residual[...] = (1.0 - start) * identity - start * gram

    def grow(index, ratio):
        square = ratio * ratio
        scale = 2.0 / (2.0 - square)
        power = split(residual[...])
        more = dot_three(split(inverse[...]), power, 1)
        inverse[...] = scale * (inverse[...] + more)
        residual[...] = (1.0 - scale) * identity + scale * dot_three(power, power, 1)
        return square / (2.0 - square)

    lax.fori_loop(0, trips, grow, spread / (2.0 + spread))

    guess = inverse[...]
    error = identity - guess - exact_dot(gram, guess)
    inverse[...] = guess + dot_three(split(guess), split(error), 1)


def identity_of(block):
    row = lax.broadcasted_iota(jnp.int32, (block, block), 0)
    col = lax.broadcasted_iota(jnp.int32, (block, block), 1)
    return jnp.where(row == col, 1.0, 0.0).astype(F32)


def couple(rows_all, norms, cross, identity):
    scales = lax.rsqrt(norms / rows_all + 1e-06)
    scale_first = jnp.sum(identity * scales[0:1, :], axis=1, keepdims=True)
    cross[...] = 0.5 * cross[...] * scale_first * scales[1:2, :] / rows_all


def two_blocks(own, landed, high, low, place):
    return dot_three(split(own), (high[place, 0], low[place, 0]), 1) + dot_three(
        split(landed), (high[place, 1], low[place, 1]), 1
    )


def sweep_kernel(
    rows_all, count, length, matrix, out, lead, keep, lead_land, keep_land, high, low,
    loaded, raw,
    cross, norms, part, recv, mine, gathered, total,
    cross_two, norms_two, part_two, recv_two, mine_two, gathered_two, total_keep,
    passed, gathered_lead, total_lead, raw_piece, gathered_raw, total_raw,
    coupling, inverse, residual, rot_high, rot_low,
    load_sem, lead_send, lead_recv, keep_send, keep_recv, raw_send, raw_recv,
    sum_send, sum_recv, all_send, all_recv, sum_two_send, sum_two_recv, all_two_send, all_two_recv,
    more_send, more_recv, rest_send, rest_recv,
    pass_send, pass_recv, piece_send, piece_recv, totals_send, totals_recv, go_sem,
):
    rows, cols = loaded.shape
    block = cols // 2
    step = rows // SENDS
    group = SENDS // CHUNKS
    me = lax.axis_index("rows")
    position = lax.axis_index("pairs")
    lead_peer, keep_peer = partners(position, length)
    core_peer = position + 1 - 2 * (position % 2)
    near_keep = keep_peer == core_peer
    near_lead = lead_peer == core_peer
    far_keep = jnp.logical_not(near_keep)
    far_lead = jnp.logical_not(near_lead)
    even = position % 2 == 0
    left_leads = jnp.logical_or(position % 2 == 1, position == 0)
    sent = jnp.where(near_lead, SENDS, SENDS - RAW)
    landing = SENDS - RAW
    signals = jnp.logical_and(position > 0, position < length - 1)

    def at(send, sends=1):
        return pl.ds(pl.multiple_of(send * step, step), sends * step)

    def load(chunk):
        where = at(chunk * (SENDS // LOADS), SENDS // LOADS)
        return pltpu.make_async_copy(matrix.at[where], loaded.at[where], load_sem.at[chunk])

    def send_raw(index):
        return pairs_copy(
            matrix.at[at(SENDS - RAW + index)], raw.at[at(index)],
            raw_send.at[index], raw_recv.at[index], lead_peer,
        )

    def send_lead(send):
        return pairs_copy(
            lead.at[at(send)], keep_land.at[at(send)],
            lead_send.at[send], lead_recv.at[send], lead_peer,
        )

    def send_keep(send):
        return pairs_copy(
            keep.at[at(send)], lead_land.at[at(send)],
            keep_send.at[send], keep_recv.at[send], keep_peer,
        )

    def loop(begin, end, do):
        def body(index, carry):
            do(index)
            return carry

        lax.fori_loop(begin, end, body, 0)

    def relay_copies(source, target, send_sems, recv_sems):
        return [
            rows_copy(
                source, target.at[far], send_sems.at[far], recv_sems.at[far],
                lax.rem(me + far, count),
            )
            for far in range(1, count)
        ]

    piece = pairs_copy(mine, raw_piece, piece_send, piece_recv, lead_peer)
    piece_two = pairs_copy(mine_two, passed, pass_send, pass_recv, keep_peer)
    totals = pairs_copy(total_keep, total_lead, totals_send, totals_recv, keep_peer)
    raw_copies = relay_copies(raw_piece, gathered_raw, rest_send, rest_recv)
    lead_copies = relay_copies(passed, gathered_lead, more_send, more_recv)

    def turn(chunk):
        where = at(chunk * group, group)
        turned = dot_three(split(loaded[where, :]), (rot_high[...], rot_low[...]), 1)
        left, right = turned[:, :block], turned[:, block:]
        lead[where, :] = jnp.where(left_leads, left, right)
        keep[where, :] = jnp.where(left_leads, right, left)
        for offset in range(group):
            send = chunk * group + offset

            @pl.when(send < sent)
            def _():
                send_lead(send).start()

            @pl.when(near_keep)
            def _():
                send_keep(send).start()

    def multiply(chunk):
        where = at(chunk * group, group)
        ours, theirs = keep[where, :], keep_land[where, :]
        cross_two[...] += dot_three(split(ours), split(theirs), 0)
        add_norms(norms_two, ours, theirs)

    def take(chunk):
        for offset in range(group):
            send_lead(chunk * group + offset).wait_recv()
        multiply(chunk)

    def hand_over():
        loop(0, sent, lambda send: send_lead(send).wait_send())

        @pl.when(signals)
        def _():
            pl.semaphore_signal(
                go_sem, inc=1, device_id={"pairs": core_peer}, device_id_type=MESH
            )

    def couple_and_invert(sums, flip):
        scales = unpack(sums, coupling)
        identity = identity_of(block)
        couple(rows_all, scales, coupling, identity)
        if flip is not None:
            value = coupling[...]
            coupling[...] = jnp.where(flip, value.T, value)
        value = coupling[...]
        invert_fixed(exact_dot(value, value, 1, 1), inverse, residual, identity)
        return 2.0 * inverse[...] - identity, identity

    def prepare_both():
        straight, identity = couple_and_invert(total, None)
        upper = exact_dot(inverse[...], coupling[...])
        lower = exact_dot(coupling[...], upper, 0)
        parts = (
            (0, 0, straight),
            (0, 1, 2.0 * upper),
            (1, 0, -2.0 * upper.T),
            (1, 1, identity - 2.0 * lower),
        )
        for down, across, value in parts:
            where = (pl.ds(down * block, block), pl.ds(across * block, block))
            rot_high[where], rot_low[where] = split(value)

    def prepare(place, sums, flip, takes_first, own_out):
        straight, identity = couple_and_invert(sums, flip)
        sign = jnp.where(takes_first, -2.0, 2.0)
        crossed = sign * dot_three(split(coupling[...]), split(inverse[...]), 0)
        own = jnp.where(own_out, straight, crossed)
        landed = jnp.where(own_out, crossed, straight)
        high[place, 0], low[place, 0] = split(own)
        high[place, 1], low[place, 1] = split(landed)

    def turn_raw():
        gather_finish(count, raw_piece, gathered_raw, total_raw, raw_copies)
        left = jnp.logical_or(keep_peer % 2 == 1, keep_peer == 0)
        prepare(0, total_raw, jnp.logical_not(left), left, left)
        loop(0, RAW, lambda index: send_raw(index).wait_recv())

        def body(chunk):
            source = at(chunk * group, group)
            keep_land[at(landing + chunk * group, group), :] = dot_three(
                split(raw[source, :block]), (high[0, 0], low[0, 0]), 1
            ) + dot_three(split(raw[source, block:]), (high[0, 1], low[0, 1]), 1)
            multiply(landing // group + chunk)

        loop(0, RAW // group, body)

    def prepare_lead(place):
        prepare(
            place,
            total_lead,
            position == 0,
            jnp.logical_or(even, position == length - 1),
            position == 0,
        )
        loop(0, SENDS, lambda send: send_keep(send).wait_recv())

    def finish(own, landed):
        def body(chunk):
            where = at(chunk * (SENDS // OUTS), SENDS // OUTS)
            out[where, :] = two_blocks(own[where, :], landed[where, :], high, low, 0)

        loop(0, OUTS, body)

    for chunk in range(LOADS):
        load(chunk).start()
    barrier = pltpu.get_barrier_semaphore()
    for far in range(1, count):
        greet(barrier, "rows", lax.rem(me + far, count))
    for peer in (lead_peer, keep_peer, core_peer):
        greet(barrier, "pairs", peer)
    for ref in (cross, norms, cross_two, norms_two):
        ref[...] = jnp.zeros_like(ref)

    def take_first(chunk):
        where = at(chunk * (SENDS // LOADS), SENDS // LOADS)
        load(chunk).wait()
        first, second = loaded[where, :block], loaded[where, block:]
        cross[...] += dot_three(split(first), split(second), 0)
        add_norms(norms, first, second)

    loop(0, LOADS, take_first)
    pl.semaphore_wait(barrier, count + 2)

    @pl.when(far_lead)
    def _():
        loop(0, RAW_FIRST, lambda index: send_raw(index).start())

    pack(count, cross, norms, part)
    sums = scatter_start(count, part, recv, sum_send, sum_recv)
    scatter_finish(count, part, recv, mine, sums)

    @pl.when(far_lead)
    def _():
        piece.start()
        loop(RAW_FIRST, RAW, lambda index: send_raw(index).start())

    alls = gather_start(count, mine, gathered, all_send, all_recv)
    gather_finish(count, mine, gathered, total, alls)

    @pl.when(far_keep)
    def _():
        piece.wait_recv()
        for copy in raw_copies:
            copy.start()

    prepare_both()
    loop(0, CHUNKS, turn)

    @pl.when(far_keep)
    def _():
        turn_raw()

    @pl.when(far_keep)
    def _():
        loop(0, landing // group - 1, take)
        hand_over()
        pl.semaphore_wait(go_sem, 1)
        loop(0, EARLY, lambda send: send_keep(send).start())
        take(landing // group - 1)

    @pl.when(near_keep)
    def _():
        loop(0, CHUNKS, take)

    pack(count, cross_two, norms_two, part_two)
    sums_two = scatter_start(count, part_two, recv_two, sum_two_send, sum_two_recv)

    @pl.when(near_keep)
    def _():
        hand_over()

    scatter_finish(count, part_two, recv_two, mine_two, sums_two)

    @pl.when(far_keep)
    def _():
        piece_two.start()

    alls_two = gather_start(count, mine_two, gathered_two, all_two_send, all_two_recv)

    @pl.when(far_keep)
    def _():
        loop(EARLY, SENDS, lambda send: send_keep(send).start())

    @pl.when(near_lead)
    def _():
        totals.wait_recv()
        prepare_lead(0)
        finish(lead, lead_land)

    gather_finish(count, mine_two, gathered_two, total_keep, alls_two)

    @pl.when(near_keep)
    def _():
        totals.start()

    prepare(
        jnp.where(near_lead, 1, 0),
        total_keep,
        position != 1,
        jnp.logical_and(jnp.logical_not(even), position != 1),
        position == 1,
    )

    @pl.when(far_lead)
    def _():
        piece_two.wait_recv()
        for copy in lead_copies:
            copy.start()
        finish(keep, keep_land)
        gather_finish(count, passed, gathered_lead, total_lead, lead_copies)
        prepare_lead(1)
        for copy in lead_copies:
            copy.wait_send()

    for copy in sums + alls + sums_two + alls_two:
        copy.wait_send()

    @pl.when(near_keep)
    def _():
        totals.wait_send()

    @pl.when(far_keep)
    def _():
        piece_two.wait_send()


    @pl.when(far_keep)
    def _():
        for copy in raw_copies:
            copy.wait_send()

    @pl.when(far_lead)
    def _():
        piece.wait_send()
        loop(0, RAW, lambda index: send_raw(index).wait_send())

    loop(0, SENDS, lambda send: send_keep(send).wait_send())


def sweep(matrix):
    rows, cols = matrix.shape
    block = cols // 2
    count = lax.axis_size("rows")
    length = lax.axis_size("pairs")
    shape = (2 * (block // count) + 4, block // 2)
    slot, slots = pltpu.VMEM(shape, F32), pltpu.VMEM((count,) + shape, F32)
    square = pltpu.VMEM((block, block), F32)
    sums = [square, pltpu.VMEM((4, block // 2), F32), slots, slots, slot, slots, slots]
    vmem = pl.BlockSpec(memory_space=pltpu.VMEM)
    return pl.pallas_call(
        functools.partial(sweep_kernel, rows * count, count, length),
        out_shape=[jax.ShapeDtypeStruct((rows, block), F32)] * 5
        + [jax.ShapeDtypeStruct((2, 2, block, block), BF16)] * 2,
        in_specs=[pl.BlockSpec(memory_space=pltpu.HBM)],
        out_specs=[vmem] * 7,
        scratch_shapes=[pltpu.VMEM((rows, cols), F32)]
        + [pltpu.VMEM((RAW * (rows // SENDS), cols), F32)]
        + sums * 2
        + [slot, slots, slots] * 2
        + [square] * 3
        + [pltpu.VMEM((cols, cols), BF16)] * 2
        + [DMA((LOADS,))]
        + [DMA((SENDS,))] * 4
        + [DMA((RAW,))] * 2
        + [DMA((count,))] * 12
        + [DMA(())] * 6
        + [pltpu.SemaphoreType.REGULAR],
        name="sweep",
        compiler_params=pltpu.CompilerParams(
            collective_id=0, has_side_effects=True, vmem_limit_bytes=24 * 2**20
        ),
    )(pltpu.with_memory_space_constraint(matrix, pltpu.HBM))


def final_kernel(length, done, lead, keep, lead_land, keep_land, high, low, out, staged, sems):
    rows, block = lead.shape
    step = rows // OUTS
    position = lax.axis_index("pairs")
    near_lead = jnp.logical_or(position == 0, position == length - 1)
    even = position % 2 == 0

    def store(chunk, source, takes_lead, sem):
        column = jnp.where(takes_lead == even, 0, block)
        where = pl.ds(pl.multiple_of(chunk * step, step), step)
        return pltpu.make_async_copy(
            source.at[where],
            out.at[where, pl.ds(pl.multiple_of(column, block), block)],
            sems.at[sem, chunk],
        )

    def loop(do):
        def body(chunk, carry):
            do(chunk)
            return carry

        lax.fori_loop(0, OUTS, body, 0)

    loop(lambda chunk: store(chunk, done, near_lead, 0).start())

    def finish(own, landed):
        def body(chunk):
            where = pl.ds(pl.multiple_of(chunk * step, step), step)
            staged[where, :] = two_blocks(own[where, :], landed[where, :], high, low, 1)
            store(chunk, staged, jnp.logical_not(near_lead), 1).start()

        loop(body)

    @pl.when(near_lead)
    def _():
        finish(keep, keep_land)

    @pl.when(jnp.logical_not(near_lead))
    def _():
        finish(lead, lead_land)

    def drain(chunk):
        store(chunk, done, near_lead, 0).wait()
        store(chunk, staged, near_lead, 1).wait()

    loop(drain)


def final(done, *blocks):
    rows, block = done.shape
    return pl.pallas_call(
        functools.partial(final_kernel, lax.axis_size("pairs")),
        out_shape=jax.ShapeDtypeStruct((rows, 2 * block), F32),
        in_specs=[pl.BlockSpec(memory_space=pltpu.VMEM)] * 7,
        out_specs=pl.BlockSpec(memory_space=pl.ANY),
        scratch_shapes=[pltpu.VMEM((rows, block), F32), DMA((2, OUTS))],
        name="final",
        compiler_params=pltpu.CompilerParams(vmem_limit_bytes=16 * 2**20),
    )(done, *blocks)


def shards(matrix):
    return final(*sweep(matrix))


def solution(mesh):
    return jax.shard_map(
        shards,
        mesh=mesh,
        in_specs=(P("rows", "pairs"),),
        out_specs=P("rows", "pairs"),
        check_vma=False,
    )
```

```python
import functools

import jax
import jax.numpy as jnp
from jax import lax
from jax.experimental import pallas as pl
from jax.experimental.pallas import tpu as pltpu
from jax.sharding import PartitionSpec as P

LOADS = 4
CHUNKS = 8
SENDS = 16
OUTS = 4
EARLY = 6
RAW = 8
RAW_FIRST = 3
F32 = jnp.float32
BF16 = jnp.bfloat16
MESH = pl.DeviceIdType.MESH
DMA = pltpu.SemaphoreType.DMA


def split(value):
    high = value.astype(BF16)
    return high, (value - high.astype(F32)).astype(BF16)


def dot_bf16(left, right, left_dim):
    return lax.dot_general(
        left, right, (((left_dim,), (0,)), ((), ())), preferred_element_type=F32
    )


def dot_three(left, right, left_dim):
    return (
        dot_bf16(left[0], right[1], left_dim)
        + dot_bf16(left[1], right[0], left_dim)
        + dot_bf16(left[0], right[0], left_dim)
    )


def exact_dot(left, right, left_dim=1, right_dim=0):
    return lax.dot_general(
        left,
        right,
        (((left_dim,), (right_dim,)), ((), ())),
        precision=lax.Precision.HIGHEST,
        preferred_element_type=F32,
    )


def rows_copy(src, dst, send, recv, peer):
    return pltpu.make_async_remote_copy(
        src_ref=src,
        dst_ref=dst,
        send_sem=send,
        recv_sem=recv,
        device_id={"rows": peer},
        device_id_type=MESH,
    )


def pairs_copy(src, dst, send, recv, peer):
    return pltpu.make_async_remote_copy(
        src_ref=src,
        dst_ref=dst,
        send_sem=send,
        recv_sem=recv,
        device_id={"pairs": peer},
        device_id_type=MESH,
    )


def greet(barrier, axis, peer):
    pl.semaphore_signal(barrier, inc=1, device_id={axis: peer}, device_id_type=MESH)


def partners(position, length):
    even = position % 2 == 0
    down = jnp.where(position == 0, 1, position - 2)
    up = jnp.where(position == length - 1, length - 2, position + 2)
    lead = jnp.where(even, down, up)
    down = jnp.where(position == 1, 0, position - 2)
    up = jnp.where(position == length - 2, length - 1, position + 2)
    keep = jnp.where(even, up, down)
    return lead, keep


def add_norms(norms, first, second):
    half = norms.shape[1]
    for row, value in ((0, first), (1, second)):
        sums = jnp.sum(value * value, axis=0, keepdims=True)
        norms[row : row + 1, :] += sums[:, :half]
        norms[row + 2 : row + 3, :] += sums[:, half:]


def pack(count, cross, norms, part):
    block = cross.shape[0]
    share = block // count
    half = block // 2
    for slot in range(count):
        part[slot, :share, :] = cross[slot * share : (slot + 1) * share, :half]
        part[slot, share : 2 * share, :] = cross[slot * share : (slot + 1) * share, half:]
        part[slot, 2 * share :, :] = norms[...]


def unpack(total, cross):
    count, depth, half = total.shape
    share = (depth - 4) // 2
    for slot in range(count):
        cross[slot * share : (slot + 1) * share, :half] = total[slot, :share, :]
        cross[slot * share : (slot + 1) * share, half:] = total[slot, share : 2 * share, :]
    norms = total[0, 2 * share :, :]
    return jnp.concatenate([norms[0:2], norms[2:4]], axis=1)


def scatter_start(count, part, recv, send_sems, recv_sems):
    me = lax.axis_index("rows")
    copies = []
    for far in range(1, count):
        peer = lax.rem(me + far, count)
        copy = rows_copy(part.at[peer], recv.at[far], send_sems.at[far], recv_sems.at[far], peer)
        copy.start()
        copies.append(copy)
    return copies


def scatter_finish(count, part, recv, mine, copies):
    acc = part[lax.axis_index("rows")]
    for far in range(1, count):
        copies[far - 1].wait_recv()
        acc = acc + recv[far]
    mine[...] = acc


def gather_start(count, mine, gathered, send_sems, recv_sems):
    me = lax.axis_index("rows")
    copies = []
    for far in range(1, count):
        peer = lax.rem(me + far, count)
        copy = rows_copy(mine, gathered.at[far], send_sems.at[far], recv_sems.at[far], peer)
        copy.start()
        copies.append(copy)
    return copies


def gather_finish(count, mine, gathered, total, copies):
    me = lax.axis_index("rows")
    total[me] = mine[...]
    for far in range(1, count):
        copies[far - 1].wait_recv()
        total[lax.rem(me + count - far, count)] = gathered[far]


def invert_fixed(gram, inverse, residual, identity):
    block = identity.shape[0]
    largest = 0.25 * block * block
    ratio, trips = largest / (2.0 + largest), 0
    while ratio > 0.01:
        ratio, trips = ratio * ratio / (2.0 - ratio * ratio), trips + 1
    sums = jnp.sum(jnp.abs(gram), axis=1, keepdims=True)
    spread = jnp.max(sums, axis=0, keepdims=True)
    start = 2.0 / (2.0 + spread)
    inverse[...] = start * identity
    residual[...] = (1.0 - start) * identity - start * gram

    def grow(index, ratio):
        square = ratio * ratio
        scale = 2.0 / (2.0 - square)
        power = split(residual[...])
        more = dot_three(split(inverse[...]), power, 1)
        inverse[...] = scale * (inverse[...] + more)
        residual[...] = (1.0 - scale) * identity + scale * dot_three(power, power, 1)
        return square / (2.0 - square)

    lax.fori_loop(0, trips, grow, spread / (2.0 + spread))

    guess = inverse[...]
    error = identity - guess - exact_dot(gram, guess)
    inverse[...] = guess + dot_three(split(guess), split(error), 1)


def identity_of(block):
    row = lax.broadcasted_iota(jnp.int32, (block, block), 0)
    col = lax.broadcasted_iota(jnp.int32, (block, block), 1)
    return jnp.where(row == col, 1.0, 0.0).astype(F32)


def couple(rows_all, norms, cross, identity):
    scales = lax.rsqrt(norms / rows_all + 1e-06)
    scale_first = jnp.sum(identity * scales[0:1, :], axis=1, keepdims=True)
    cross[...] = 0.5 * cross[...] * scale_first * scales[1:2, :] / rows_all


def two_blocks(own, landed, high, low, place):
    return dot_three(split(own), (high[place, 0], low[place, 0]), 1) + dot_three(
        split(landed), (high[place, 1], low[place, 1]), 1
    )


def sweep_kernel(
    rows_all, count, length, matrix, out, lead, keep, lead_land, keep_land, high, low,
    loaded, raw,
    cross, norms, part, recv, mine, gathered, total,
    cross_two, norms_two, part_two, recv_two, mine_two, gathered_two, total_keep,
    passed, gathered_lead, total_lead, raw_piece, gathered_raw, total_raw,
    coupling, inverse, residual, rot_high, rot_low,
    load_sem, lead_send, lead_recv, keep_send, keep_recv, raw_send, raw_recv,
    sum_send, sum_recv, all_send, all_recv, sum_two_send, sum_two_recv, all_two_send, all_two_recv,
    more_send, more_recv, rest_send, rest_recv,
    pass_send, pass_recv, piece_send, piece_recv, totals_send, totals_recv, go_sem,
):
    rows, cols = loaded.shape
    block = cols // 2
    step = rows // SENDS
    group = SENDS // CHUNKS
    me = lax.axis_index("rows")
    position = lax.axis_index("pairs")
    lead_peer, keep_peer = partners(position, length)
    core_peer = position + 1 - 2 * (position % 2)
    near_keep = keep_peer == core_peer
    near_lead = lead_peer == core_peer
    far_keep = jnp.logical_not(near_keep)
    far_lead = jnp.logical_not(near_lead)
    even = position % 2 == 0
    left_leads = jnp.logical_or(position % 2 == 1, position == 0)
    sent = jnp.where(near_lead, SENDS, SENDS - RAW)
    landing = SENDS - RAW
    signals = jnp.logical_and(position > 0, position < length - 1)

    def at(send, sends=1):
        return pl.ds(pl.multiple_of(send * step, step), sends * step)

    def load(chunk):
        where = at(chunk * (SENDS // LOADS), SENDS // LOADS)
        return pltpu.make_async_copy(matrix.at[where], loaded.at[where], load_sem.at[chunk])

    def send_raw(index):
        return pairs_copy(
            loaded.at[at(SENDS - RAW + index)], raw.at[at(index)],
            raw_send.at[index], raw_recv.at[index], lead_peer,
        )

    def send_lead(send):
        return pairs_copy(
            lead.at[at(send)], keep_land.at[at(send)],
            lead_send.at[send], lead_recv.at[send], lead_peer,
        )

    def send_keep(send):
        return pairs_copy(
            keep.at[at(send)], lead_land.at[at(send)],
            keep_send.at[send], keep_recv.at[send], keep_peer,
        )

    def loop(begin, end, do):
        def body(index, carry):
            do(index)
            return carry

        lax.fori_loop(begin, end, body, 0)

    def relay_copies(source, target, send_sems, recv_sems):
        return [
            rows_copy(
                source, target.at[far], send_sems.at[far], recv_sems.at[far],
                lax.rem(me + far, count),
            )
            for far in range(1, count)
        ]

    piece = pairs_copy(mine, raw_piece, piece_send, piece_recv, lead_peer)
    piece_two = pairs_copy(mine_two, passed, pass_send, pass_recv, keep_peer)
    totals = pairs_copy(total_keep, total_lead, totals_send, totals_recv, keep_peer)
    raw_copies = relay_copies(raw_piece, gathered_raw, rest_send, rest_recv)
    lead_copies = relay_copies(passed, gathered_lead, more_send, more_recv)

    def turn(chunk):
        where = at(chunk * group, group)
        turned = dot_three(split(loaded[where, :]), (rot_high[...], rot_low[...]), 1)
        left, right = turned[:, :block], turned[:, block:]
        lead[where, :] = jnp.where(left_leads, left, right)
        keep[where, :] = jnp.where(left_leads, right, left)
        for offset in range(group):
            send = chunk * group + offset

            @pl.when(send < sent)
            def _():
                send_lead(send).start()

            @pl.when(near_keep)
            def _():
                send_keep(send).start()

    def multiply(chunk):
        where = at(chunk * group, group)
        ours, theirs = keep[where, :], keep_land[where, :]
        cross_two[...] += dot_three(split(ours), split(theirs), 0)
        add_norms(norms_two, ours, theirs)

    def take(chunk):
        for offset in range(group):
            send_lead(chunk * group + offset).wait_recv()
        multiply(chunk)

    def hand_over():
        loop(0, sent, lambda send: send_lead(send).wait_send())

        @pl.when(signals)
        def _():
            pl.semaphore_signal(
                go_sem, inc=1, device_id={"pairs": core_peer}, device_id_type=MESH
            )

    def couple_and_invert(sums, flip):
        scales = unpack(sums, coupling)
        identity = identity_of(block)
        couple(rows_all, scales, coupling, identity)
        if flip is not None:
            value = coupling[...]
            coupling[...] = jnp.where(flip, value.T, value)
        value = coupling[...]
        invert_fixed(exact_dot(value, value, 1, 1), inverse, residual, identity)
        return 2.0 * inverse[...] - identity, identity

    def prepare_both():
        straight, identity = couple_and_invert(total, None)
        upper = exact_dot(inverse[...], coupling[...])
        lower = exact_dot(coupling[...], upper, 0)
        parts = (
            (0, 0, straight),
            (0, 1, 2.0 * upper),
            (1, 0, -2.0 * upper.T),
            (1, 1, identity - 2.0 * lower),
        )
        for down, across, value in parts:
            where = (pl.ds(down * block, block), pl.ds(across * block, block))
            rot_high[where], rot_low[where] = split(value)

    def prepare(place, sums, flip, takes_first, own_out):
        straight, identity = couple_and_invert(sums, flip)
        sign = jnp.where(takes_first, -2.0, 2.0)
        crossed = sign * dot_three(split(coupling[...]), split(inverse[...]), 0)
        own = jnp.where(own_out, straight, crossed)
        landed = jnp.where(own_out, crossed, straight)
        high[place, 0], low[place, 0] = split(own)
        high[place, 1], low[place, 1] = split(landed)

    def turn_raw():
        gather_finish(count, raw_piece, gathered_raw, total_raw, raw_copies)
        left = jnp.logical_or(keep_peer % 2 == 1, keep_peer == 0)
        prepare(0, total_raw, jnp.logical_not(left), left, left)
        loop(0, RAW, lambda index: send_raw(index).wait_recv())

        def body(chunk):
            source = at(chunk * group, group)
            keep_land[at(landing + chunk * group, group), :] = dot_three(
                split(raw[source, :block]), (high[0, 0], low[0, 0]), 1
            ) + dot_three(split(raw[source, block:]), (high[0, 1], low[0, 1]), 1)
            multiply(landing // group + chunk)

        loop(0, RAW // group, body)

    def prepare_lead(place):
        prepare(
            place,
            total_lead,
            position == 0,
            jnp.logical_or(even, position == length - 1),
            position == 0,
        )

    def finish(own, landed):
        def body(chunk):
            where = at(chunk * (SENDS // OUTS), SENDS // OUTS)
            out[where, :] = two_blocks(own[where, :], landed[where, :], high, low, 0)

        loop(0, OUTS, body)

    for chunk in range(LOADS):
        load(chunk).start()
    barrier = pltpu.get_barrier_semaphore()
    for far in range(1, count):
        greet(barrier, "rows", lax.rem(me + far, count))
    for peer in (lead_peer, keep_peer, core_peer):
        greet(barrier, "pairs", peer)
    for ref in (cross, norms, cross_two, norms_two):
        ref[...] = jnp.zeros_like(ref)

    def take_first(chunk):
        where = at(chunk * (SENDS // LOADS), SENDS // LOADS)
        load(chunk).wait()
        first, second = loaded[where, :block], loaded[where, block:]
        cross[...] += dot_three(split(first), split(second), 0)
        add_norms(norms, first, second)

    loop(0, LOADS, take_first)
    pl.semaphore_wait(barrier, count + 2)

    @pl.when(far_lead)
    def _():
        loop(0, RAW_FIRST, lambda index: send_raw(index).start())

    pack(count, cross, norms, part)
    sums = scatter_start(count, part, recv, sum_send, sum_recv)
    scatter_finish(count, part, recv, mine, sums)

    @pl.when(far_lead)
    def _():
        piece.start()
        loop(RAW_FIRST, RAW, lambda index: send_raw(index).start())

    alls = gather_start(count, mine, gathered, all_send, all_recv)
    gather_finish(count, mine, gathered, total, alls)

    @pl.when(far_keep)
    def _():
        piece.wait_recv()
        for copy in raw_copies:
            copy.start()

    prepare_both()
    loop(0, CHUNKS, turn)

    @pl.when(far_keep)
    def _():
        turn_raw()

    @pl.when(far_keep)
    def _():
        loop(0, landing // group - 1, take)
        hand_over()
        pl.semaphore_wait(go_sem, 1)
        loop(0, EARLY, lambda send: send_keep(send).start())
        take(landing // group - 1)

    @pl.when(near_keep)
    def _():
        loop(0, CHUNKS, take)

    pack(count, cross_two, norms_two, part_two)
    sums_two = scatter_start(count, part_two, recv_two, sum_two_send, sum_two_recv)

    @pl.when(near_keep)
    def _():
        hand_over()

    scatter_finish(count, part_two, recv_two, mine_two, sums_two)

    @pl.when(far_keep)
    def _():
        piece_two.start()

    alls_two = gather_start(count, mine_two, gathered_two, all_two_send, all_two_recv)

    @pl.when(far_keep)
    def _():
        loop(EARLY, SENDS, lambda send: send_keep(send).start())

    @pl.when(near_lead)
    def _():
        totals.wait_recv()
        prepare_lead(0)
        loop(0, SENDS, lambda send: send_keep(send).wait_recv())
        finish(lead, lead_land)

    gather_finish(count, mine_two, gathered_two, total_keep, alls_two)

    @pl.when(near_keep)
    def _():
        totals.start()

    @pl.when(far_lead)
    def _():
        piece_two.wait_recv()
        for copy in lead_copies:
            copy.start()

    prepare(
        jnp.where(near_lead, 1, 0),
        total_keep,
        position != 1,
        jnp.logical_and(jnp.logical_not(even), position != 1),
        position == 1,
    )

    @pl.when(far_lead)
    def _():
        gather_finish(count, passed, gathered_lead, total_lead, lead_copies)
        prepare_lead(1)
        finish(keep, keep_land)
        loop(0, SENDS, lambda send: send_keep(send).wait_recv())
        for copy in lead_copies:
            copy.wait_send()

    for copy in sums + alls + sums_two + alls_two:
        copy.wait_send()

    @pl.when(near_keep)
    def _():
        totals.wait_send()

    @pl.when(far_keep)
    def _():
        piece_two.wait_send()


    @pl.when(far_keep)
    def _():
        for copy in raw_copies:
            copy.wait_send()

    @pl.when(far_lead)
    def _():
        piece.wait_send()
        loop(0, RAW, lambda index: send_raw(index).wait_send())

    loop(0, SENDS, lambda send: send_keep(send).wait_send())


def sweep(matrix):
    rows, cols = matrix.shape
    block = cols // 2
    count = lax.axis_size("rows")
    length = lax.axis_size("pairs")
    shape = (2 * (block // count) + 4, block // 2)
    slot, slots = pltpu.VMEM(shape, F32), pltpu.VMEM((count,) + shape, F32)
    square = pltpu.VMEM((block, block), F32)
    sums = [square, pltpu.VMEM((4, block // 2), F32), slots, slots, slot, slots, slots]
    vmem = pl.BlockSpec(memory_space=pltpu.VMEM)
    return pl.pallas_call(
        functools.partial(sweep_kernel, rows * count, count, length),
        out_shape=[jax.ShapeDtypeStruct((rows, block), F32)] * 5
        + [jax.ShapeDtypeStruct((2, 2, block, block), BF16)] * 2,
        in_specs=[pl.BlockSpec(memory_space=pltpu.HBM)],
        out_specs=[vmem] * 7,
        scratch_shapes=[pltpu.VMEM((rows, cols), F32)]
        + [pltpu.VMEM((RAW * (rows // SENDS), cols), F32)]
        + sums * 2
        + [slot, slots, slots] * 2
        + [square] * 3
        + [pltpu.VMEM((cols, cols), BF16)] * 2
        + [DMA((LOADS,))]
        + [DMA((SENDS,))] * 4
        + [DMA((RAW,))] * 2
        + [DMA((count,))] * 12
        + [DMA(())] * 6
        + [pltpu.SemaphoreType.REGULAR],
        name="sweep",
        compiler_params=pltpu.CompilerParams(
            collective_id=0, has_side_effects=True, vmem_limit_bytes=24 * 2**20
        ),
    )(pltpu.with_memory_space_constraint(matrix, pltpu.HBM))


def final_kernel(length, done, lead, keep, lead_land, keep_land, high, low, out, staged, sems):
    rows, block = lead.shape
    step = rows // OUTS
    position = lax.axis_index("pairs")
    near_lead = jnp.logical_or(position == 0, position == length - 1)
    even = position % 2 == 0

    def store(chunk, source, takes_lead, sem):
        column = jnp.where(takes_lead == even, 0, block)
        where = pl.ds(pl.multiple_of(chunk * step, step), step)
        return pltpu.make_async_copy(
            source.at[where],
            out.at[where, pl.ds(pl.multiple_of(column, block), block)],
            sems.at[sem, chunk],
        )

    def loop(do):
        def body(chunk, carry):
            do(chunk)
            return carry

        lax.fori_loop(0, OUTS, body, 0)

    loop(lambda chunk: store(chunk, done, near_lead, 0).start())

    def finish(own, landed):
        def body(chunk):
            where = pl.ds(pl.multiple_of(chunk * step, step), step)
            staged[where, :] = two_blocks(own[where, :], landed[where, :], high, low, 1)
            store(chunk, staged, jnp.logical_not(near_lead), 1).start()

        loop(body)

    @pl.when(near_lead)
    def _():
        finish(keep, keep_land)

    @pl.when(jnp.logical_not(near_lead))
    def _():
        finish(lead, lead_land)

    def drain(chunk):
        store(chunk, done, near_lead, 0).wait()
        store(chunk, staged, near_lead, 1).wait()

    loop(drain)


def final(done, *blocks):
    rows, block = done.shape
    return pl.pallas_call(
        functools.partial(final_kernel, lax.axis_size("pairs")),
        out_shape=jax.ShapeDtypeStruct((rows, 2 * block), F32),
        in_specs=[pl.BlockSpec(memory_space=pltpu.VMEM)] * 7,
        out_specs=pl.BlockSpec(memory_space=pl.ANY),
        scratch_shapes=[pltpu.VMEM((rows, block), F32), DMA((2, OUTS))],
        name="final",
        compiler_params=pltpu.CompilerParams(vmem_limit_bytes=16 * 2**20),
    )(done, *blocks)


def shards(matrix):
    return final(*sweep(matrix))


def solution(mesh):
    return jax.shard_map(
        shards,
        mesh=mesh,
        in_specs=(P("rows", "pairs"),),
        out_specs=P("rows", "pairs"),
        check_vma=False,
    )
```

```python
import functools

import jax
import jax.numpy as jnp
from jax import lax
from jax.experimental import pallas as pl
from jax.experimental.pallas import tpu as pltpu
from jax.sharding import PartitionSpec as P

LOADS = 4
CHUNKS = 8
SENDS = 16
OUTS = 2
EARLY = 6
RAW = 8
RAW_FIRST = 3
F32 = jnp.float32
BF16 = jnp.bfloat16
MESH = pl.DeviceIdType.MESH
DMA = pltpu.SemaphoreType.DMA


def split(value):
    high = value.astype(BF16)
    return high, (value - high.astype(F32)).astype(BF16)


def dot_bf16(left, right, left_dim):
    return lax.dot_general(
        left, right, (((left_dim,), (0,)), ((), ())), preferred_element_type=F32
    )


def dot_three(left, right, left_dim):
    return (
        dot_bf16(left[0], right[1], left_dim)
        + dot_bf16(left[1], right[0], left_dim)
        + dot_bf16(left[0], right[0], left_dim)
    )


def exact_dot(left, right, left_dim=1, right_dim=0):
    return lax.dot_general(
        left,
        right,
        (((left_dim,), (right_dim,)), ((), ())),
        precision=lax.Precision.HIGHEST,
        preferred_element_type=F32,
    )


def rows_copy(src, dst, send, recv, peer):
    return pltpu.make_async_remote_copy(
        src_ref=src,
        dst_ref=dst,
        send_sem=send,
        recv_sem=recv,
        device_id={"rows": peer},
        device_id_type=MESH,
    )


def pairs_copy(src, dst, send, recv, peer):
    return pltpu.make_async_remote_copy(
        src_ref=src,
        dst_ref=dst,
        send_sem=send,
        recv_sem=recv,
        device_id={"pairs": peer},
        device_id_type=MESH,
    )


def greet(barrier, axis, peer):
    pl.semaphore_signal(barrier, inc=1, device_id={axis: peer}, device_id_type=MESH)


def partners(position, length):
    even = position % 2 == 0
    down = jnp.where(position == 0, 1, position - 2)
    up = jnp.where(position == length - 1, length - 2, position + 2)
    lead = jnp.where(even, down, up)
    down = jnp.where(position == 1, 0, position - 2)
    up = jnp.where(position == length - 2, length - 1, position + 2)
    keep = jnp.where(even, up, down)
    return lead, keep


def add_norms(norms, first, second):
    half = norms.shape[1]
    for row, value in ((0, first), (1, second)):
        sums = jnp.sum(value * value, axis=0, keepdims=True)
        norms[row : row + 1, :] += sums[:, :half]
        norms[row + 2 : row + 3, :] += sums[:, half:]


def pack(count, cross, norms, part):
    block = cross.shape[0]
    share = block // count
    half = block // 2
    for slot in range(count):
        part[slot, :share, :] = cross[slot * share : (slot + 1) * share, :half]
        part[slot, share : 2 * share, :] = cross[slot * share : (slot + 1) * share, half:]
        part[slot, 2 * share :, :] = norms[...]


def unpack(total, cross):
    count, depth, half = total.shape
    share = (depth - 4) // 2
    for slot in range(count):
        cross[slot * share : (slot + 1) * share, :half] = total[slot, :share, :]
        cross[slot * share : (slot + 1) * share, half:] = total[slot, share : 2 * share, :]
    norms = total[0, 2 * share :, :]
    return jnp.concatenate([norms[0:2], norms[2:4]], axis=1)


def scatter_start(count, part, recv, send_sems, recv_sems):
    me = lax.axis_index("rows")
    copies = []
    for far in range(1, count):
        peer = lax.rem(me + far, count)
        copy = rows_copy(part.at[peer], recv.at[far], send_sems.at[far], recv_sems.at[far], peer)
        copy.start()
        copies.append(copy)
    return copies


def scatter_finish(count, part, recv, mine, copies):
    acc = part[lax.axis_index("rows")]
    for far in range(1, count):
        copies[far - 1].wait_recv()
        acc = acc + recv[far]
    mine[...] = acc


def gather_start(count, mine, gathered, send_sems, recv_sems):
    me = lax.axis_index("rows")
    copies = []
    for far in range(1, count):
        peer = lax.rem(me + far, count)
        copy = rows_copy(mine, gathered.at[far], send_sems.at[far], recv_sems.at[far], peer)
        copy.start()
        copies.append(copy)
    return copies


def gather_finish(count, mine, gathered, total, copies):
    me = lax.axis_index("rows")
    total[me] = mine[...]
    for far in range(1, count):
        copies[far - 1].wait_recv()
        total[lax.rem(me + count - far, count)] = gathered[far]


def invert_fixed(gram, inverse, residual, identity):
    block = identity.shape[0]
    largest = 0.25 * block * block
    ratio, trips = largest / (2.0 + largest), 0
    while ratio > 0.01:
        ratio, trips = ratio * ratio / (2.0 - ratio * ratio), trips + 1
    sums = jnp.sum(jnp.abs(gram), axis=1, keepdims=True)
    spread = jnp.max(sums, axis=0, keepdims=True)
    start = 2.0 / (2.0 + spread)
    inverse[...] = start * identity
    residual[...] = (1.0 - start) * identity - start * gram

    def grow(index, ratio):
        square = ratio * ratio
        scale = 2.0 / (2.0 - square)
        power = split(residual[...])
        more = dot_three(split(inverse[...]), power, 1)
        inverse[...] = scale * (inverse[...] + more)
        residual[...] = (1.0 - scale) * identity + scale * dot_three(power, power, 1)
        return square / (2.0 - square)

    lax.fori_loop(0, trips, grow, spread / (2.0 + spread))

    guess = inverse[...]
    error = identity - guess - exact_dot(gram, guess)
    inverse[...] = guess + dot_three(split(guess), split(error), 1)


def identity_of(block):
    row = lax.broadcasted_iota(jnp.int32, (block, block), 0)
    col = lax.broadcasted_iota(jnp.int32, (block, block), 1)
    return jnp.where(row == col, 1.0, 0.0).astype(F32)


def couple(rows_all, norms, cross, identity):
    scales = lax.rsqrt(norms / rows_all + 1e-06)
    scale_first = jnp.sum(identity * scales[0:1, :], axis=1, keepdims=True)
    cross[...] = 0.5 * cross[...] * scale_first * scales[1:2, :] / rows_all


def two_blocks(own, landed, high, low, place):
    return dot_three(split(own), (high[place, 0], low[place, 0]), 1) + dot_three(
        split(landed), (high[place, 1], low[place, 1]), 1
    )


def sweep_kernel(
    rows_all, count, length, matrix, out, lead, keep, lead_land, keep_land, high, low,
    loaded, raw,
    cross, norms, part, recv, mine, gathered, total,
    cross_two, norms_two, part_two, recv_two, mine_two, gathered_two, total_keep,
    passed, gathered_lead, total_lead, raw_piece, gathered_raw, total_raw,
    coupling, inverse, residual, rot_high, rot_low,
    load_sem, lead_send, lead_recv, keep_send, keep_recv, raw_send, raw_recv,
    sum_send, sum_recv, all_send, all_recv, sum_two_send, sum_two_recv, all_two_send, all_two_recv,
    more_send, more_recv, rest_send, rest_recv,
    pass_send, pass_recv, piece_send, piece_recv, totals_send, totals_recv, go_sem,
):
    rows, cols = loaded.shape
    block = cols // 2
    step = rows // SENDS
    group = SENDS // CHUNKS
    me = lax.axis_index("rows")
    position = lax.axis_index("pairs")
    lead_peer, keep_peer = partners(position, length)
    core_peer = position + 1 - 2 * (position % 2)
    near_keep = keep_peer == core_peer
    near_lead = lead_peer == core_peer
    far_keep = jnp.logical_not(near_keep)
    far_lead = jnp.logical_not(near_lead)
    even = position % 2 == 0
    left_leads = jnp.logical_or(position % 2 == 1, position == 0)
    sent = jnp.where(near_lead, SENDS, SENDS - RAW)
    landing = SENDS - RAW
    signals = jnp.logical_and(position > 0, position < length - 1)

    def at(send, sends=1):
        return pl.ds(pl.multiple_of(send * step, step), sends * step)

    def load(chunk):
        where = at(chunk * (SENDS // LOADS), SENDS // LOADS)
        return pltpu.make_async_copy(matrix.at[where], loaded.at[where], load_sem.at[chunk])

    def send_raw(index):
        return pairs_copy(
            loaded.at[at(SENDS - RAW + index)], raw.at[at(index)],
            raw_send.at[index], raw_recv.at[index], lead_peer,
        )

    def send_lead(send):
        return pairs_copy(
            lead.at[at(send)], keep_land.at[at(send)],
            lead_send.at[send], lead_recv.at[send], lead_peer,
        )

    def send_keep(send):
        return pairs_copy(
            keep.at[at(send)], lead_land.at[at(send)],
            keep_send.at[send], keep_recv.at[send], keep_peer,
        )

    def loop(begin, end, do):
        def body(index, carry):
            do(index)
            return carry

        lax.fori_loop(begin, end, body, 0)

    def relay_copies(source, target, send_sems, recv_sems):
        return [
            rows_copy(
                source, target.at[far], send_sems.at[far], recv_sems.at[far],
                lax.rem(me + far, count),
            )
            for far in range(1, count)
        ]

    piece = pairs_copy(mine, raw_piece, piece_send, piece_recv, lead_peer)
    piece_two = pairs_copy(mine_two, passed, pass_send, pass_recv, keep_peer)
    totals = pairs_copy(total_keep, total_lead, totals_send, totals_recv, keep_peer)
    raw_copies = relay_copies(raw_piece, gathered_raw, rest_send, rest_recv)
    lead_copies = relay_copies(passed, gathered_lead, more_send, more_recv)

    def turn(chunk):
        where = at(chunk * group, group)
        turned = dot_three(split(loaded[where, :]), (rot_high[...], rot_low[...]), 1)
        left, right = turned[:, :block], turned[:, block:]
        lead[where, :] = jnp.where(left_leads, left, right)
        keep[where, :] = jnp.where(left_leads, right, left)
        for offset in range(group):
            send = chunk * group + offset

            @pl.when(send < sent)
            def _():
                send_lead(send).start()

            @pl.when(near_keep)
            def _():
                send_keep(send).start()

    def multiply(chunk):
        where = at(chunk * group, group)
        ours, theirs = keep[where, :], keep_land[where, :]
        cross_two[...] += dot_three(split(ours), split(theirs), 0)
        add_norms(norms_two, ours, theirs)

    def take(chunk):
        for offset in range(group):
            send_lead(chunk * group + offset).wait_recv()
        multiply(chunk)

    def hand_over():
        loop(0, sent, lambda send: send_lead(send).wait_send())

        @pl.when(signals)
        def _():
            pl.semaphore_signal(
                go_sem, inc=1, device_id={"pairs": core_peer}, device_id_type=MESH
            )

    def couple_and_invert(sums, flip):
        scales = unpack(sums, coupling)
        identity = identity_of(block)
        couple(rows_all, scales, coupling, identity)
        if flip is not None:
            value = coupling[...]
            coupling[...] = jnp.where(flip, value.T, value)
        value = coupling[...]
        invert_fixed(exact_dot(value, value, 1, 1), inverse, residual, identity)
        return 2.0 * inverse[...] - identity, identity

    def prepare_both():
        straight, identity = couple_and_invert(total, None)
        upper = exact_dot(inverse[...], coupling[...])
        lower = exact_dot(coupling[...], upper, 0)
        parts = (
            (0, 0, straight),
            (0, 1, 2.0 * upper),
            (1, 0, -2.0 * upper.T),
            (1, 1, identity - 2.0 * lower),
        )
        for down, across, value in parts:
            where = (pl.ds(down * block, block), pl.ds(across * block, block))
            rot_high[where], rot_low[where] = split(value)

    def prepare(place, sums, flip, takes_first, own_out):
        straight, identity = couple_and_invert(sums, flip)
        sign = jnp.where(takes_first, -2.0, 2.0)
        crossed = sign * dot_three(split(coupling[...]), split(inverse[...]), 0)
        own = jnp.where(own_out, straight, crossed)
        landed = jnp.where(own_out, crossed, straight)
        high[place, 0], low[place, 0] = split(own)
        high[place, 1], low[place, 1] = split(landed)

    def turn_raw():
        gather_finish(count, raw_piece, gathered_raw, total_raw, raw_copies)
        left = jnp.logical_or(keep_peer % 2 == 1, keep_peer == 0)
        prepare(0, total_raw, jnp.logical_not(left), left, left)
        loop(0, RAW, lambda index: send_raw(index).wait_recv())

        def body(chunk):
            source = at(chunk * group, group)
            keep_land[at(landing + chunk * group, group), :] = dot_three(
                split(raw[source, :block]), (high[0, 0], low[0, 0]), 1
            ) + dot_three(split(raw[source, block:]), (high[0, 1], low[0, 1]), 1)
            multiply(landing // group + chunk)

        loop(0, RAW // group, body)

    def prepare_lead(place):
        prepare(
            place,
            total_lead,
            position == 0,
            jnp.logical_or(even, position == length - 1),
            position == 0,
        )

    def finish(own, landed):
        def body(chunk):
            where = at(chunk * (SENDS // OUTS), SENDS // OUTS)
            out[where, :] = two_blocks(own[where, :], landed[where, :], high, low, 0)

        loop(0, OUTS, body)

    for chunk in range(LOADS):
        load(chunk).start()
    barrier = pltpu.get_barrier_semaphore()
    for far in range(1, count):
        greet(barrier, "rows", lax.rem(me + far, count))
    for peer in (lead_peer, keep_peer, core_peer):
        greet(barrier, "pairs", peer)
    for ref in (cross, norms, cross_two, norms_two):
        ref[...] = jnp.zeros_like(ref)

    def take_first(chunk):
        where = at(chunk * (SENDS // LOADS), SENDS // LOADS)
        load(chunk).wait()
        first, second = loaded[where, :block], loaded[where, block:]
        cross[...] += dot_three(split(first), split(second), 0)
        add_norms(norms, first, second)

    loop(0, LOADS, take_first)
    pl.semaphore_wait(barrier, count + 2)

    @pl.when(far_lead)
    def _():
        loop(0, RAW_FIRST, lambda index: send_raw(index).start())

    pack(count, cross, norms, part)
    sums = scatter_start(count, part, recv, sum_send, sum_recv)
    scatter_finish(count, part, recv, mine, sums)

    @pl.when(far_lead)
    def _():
        piece.start()
        loop(RAW_FIRST, RAW, lambda index: send_raw(index).start())

    alls = gather_start(count, mine, gathered, all_send, all_recv)
    gather_finish(count, mine, gathered, total, alls)

    @pl.when(far_keep)
    def _():
        piece.wait_recv()
        for copy in raw_copies:
            copy.start()

    prepare_both()
    loop(0, CHUNKS, turn)

    @pl.when(far_keep)
    def _():
        turn_raw()

    @pl.when(far_keep)
    def _():
        loop(0, landing // group - 1, take)
        hand_over()
        pl.semaphore_wait(go_sem, 1)
        loop(0, EARLY, lambda send: send_keep(send).start())
        take(landing // group - 1)

    @pl.when(near_keep)
    def _():
        loop(0, CHUNKS, take)

    pack(count, cross_two, norms_two, part_two)
    sums_two = scatter_start(count, part_two, recv_two, sum_two_send, sum_two_recv)

    @pl.when(near_keep)
    def _():
        hand_over()

    scatter_finish(count, part_two, recv_two, mine_two, sums_two)

    @pl.when(far_keep)
    def _():
        piece_two.start()

    alls_two = gather_start(count, mine_two, gathered_two, all_two_send, all_two_recv)

    @pl.when(far_keep)
    def _():
        loop(EARLY, SENDS, lambda send: send_keep(send).start())

    @pl.when(near_lead)
    def _():
        totals.wait_recv()
        prepare_lead(0)
        loop(0, SENDS, lambda send: send_keep(send).wait_recv())
        finish(lead, lead_land)

    gather_finish(count, mine_two, gathered_two, total_keep, alls_two)

    @pl.when(near_keep)
    def _():
        totals.start()

    @pl.when(far_lead)
    def _():
        piece_two.wait_recv()
        for copy in lead_copies:
            copy.start()

    prepare(
        jnp.where(near_lead, 1, 0),
        total_keep,
        position != 1,
        jnp.logical_and(jnp.logical_not(even), position != 1),
        position == 1,
    )

    @pl.when(far_lead)
    def _():
        gather_finish(count, passed, gathered_lead, total_lead, lead_copies)
        prepare_lead(1)
        finish(keep, keep_land)
        loop(0, SENDS, lambda send: send_keep(send).wait_recv())
        for copy in lead_copies:
            copy.wait_send()

    for copy in sums + alls + sums_two + alls_two:
        copy.wait_send()

    @pl.when(near_keep)
    def _():
        totals.wait_send()

    @pl.when(far_keep)
    def _():
        piece_two.wait_send()


    @pl.when(far_keep)
    def _():
        for copy in raw_copies:
            copy.wait_send()

    @pl.when(far_lead)
    def _():
        piece.wait_send()
        loop(0, RAW, lambda index: send_raw(index).wait_send())

    loop(0, SENDS, lambda send: send_keep(send).wait_send())


def sweep(matrix):
    rows, cols = matrix.shape
    block = cols // 2
    count = lax.axis_size("rows")
    length = lax.axis_size("pairs")
    shape = (2 * (block // count) + 4, block // 2)
    slot, slots = pltpu.VMEM(shape, F32), pltpu.VMEM((count,) + shape, F32)
    square = pltpu.VMEM((block, block), F32)
    sums = [square, pltpu.VMEM((4, block // 2), F32), slots, slots, slot, slots, slots]
    vmem = pl.BlockSpec(memory_space=pltpu.VMEM)
    return pl.pallas_call(
        functools.partial(sweep_kernel, rows * count, count, length),
        out_shape=[jax.ShapeDtypeStruct((rows, block), F32)] * 5
        + [jax.ShapeDtypeStruct((2, 2, block, block), BF16)] * 2,
        in_specs=[pl.BlockSpec(memory_space=pltpu.HBM)],
        out_specs=[vmem] * 7,
        scratch_shapes=[pltpu.VMEM((rows, cols), F32)]
        + [pltpu.VMEM((RAW * (rows // SENDS), cols), F32)]
        + sums * 2
        + [slot, slots, slots] * 2
        + [square] * 3
        + [pltpu.VMEM((cols, cols), BF16)] * 2
        + [DMA((LOADS,))]
        + [DMA((SENDS,))] * 4
        + [DMA((RAW,))] * 2
        + [DMA((count,))] * 12
        + [DMA(())] * 6
        + [pltpu.SemaphoreType.REGULAR],
        name="sweep",
        compiler_params=pltpu.CompilerParams(
            collective_id=0, has_side_effects=True, vmem_limit_bytes=24 * 2**20
        ),
    )(pltpu.with_memory_space_constraint(matrix, pltpu.HBM))


def final_kernel(length, done, lead, keep, lead_land, keep_land, high, low, out, staged, sems):
    rows, block = lead.shape
    step = rows // OUTS
    position = lax.axis_index("pairs")
    near_lead = jnp.logical_or(position == 0, position == length - 1)
    even = position % 2 == 0

    def store(chunk, source, takes_lead, sem):
        column = jnp.where(takes_lead == even, 0, block)
        where = pl.ds(pl.multiple_of(chunk * step, step), step)
        return pltpu.make_async_copy(
            source.at[where],
            out.at[where, pl.ds(pl.multiple_of(column, block), block)],
            sems.at[sem, chunk],
        )

    def loop(do):
        def body(chunk, carry):
            do(chunk)
            return carry

        lax.fori_loop(0, OUTS, body, 0)

    loop(lambda chunk: store(chunk, done, near_lead, 0).start())

    def finish(own, landed):
        def body(chunk):
            where = pl.ds(pl.multiple_of(chunk * step, step), step)
            staged[where, :] = two_blocks(own[where, :], landed[where, :], high, low, 1)
            store(chunk, staged, jnp.logical_not(near_lead), 1).start()

        loop(body)

    @pl.when(near_lead)
    def _():
        finish(keep, keep_land)

    @pl.when(jnp.logical_not(near_lead))
    def _():
        finish(lead, lead_land)

    def drain(chunk):
        store(chunk, done, near_lead, 0).wait()
        store(chunk, staged, near_lead, 1).wait()

    loop(drain)


def final(done, *blocks):
    rows, block = done.shape
    return pl.pallas_call(
        functools.partial(final_kernel, lax.axis_size("pairs")),
        out_shape=jax.ShapeDtypeStruct((rows, 2 * block), F32),
        in_specs=[pl.BlockSpec(memory_space=pltpu.VMEM)] * 7,
        out_specs=pl.BlockSpec(memory_space=pl.ANY),
        scratch_shapes=[pltpu.VMEM((rows, block), F32), DMA((2, OUTS))],
        name="final",
        compiler_params=pltpu.CompilerParams(vmem_limit_bytes=16 * 2**20),
    )(done, *blocks)


def shards(matrix):
    return final(*sweep(matrix))


def solution(mesh):
    return jax.shard_map(
        shards,
        mesh=mesh,
        in_specs=(P("rows", "pairs"),),
        out_specs=P("rows", "pairs"),
        check_vma=False,
    )
```

```python
import functools

import jax
import jax.numpy as jnp
from jax import lax
from jax.experimental import pallas as pl
from jax.experimental.pallas import tpu as pltpu
from jax.sharding import PartitionSpec as P

LOADS = 4
CHUNKS = 8
SENDS = 16
OUTS = 2
EARLY = 6
RAW = 8
RAW_FIRST = 3
F32 = jnp.float32
BF16 = jnp.bfloat16
MESH = pl.DeviceIdType.MESH
DMA = pltpu.SemaphoreType.DMA


def split(value):
    high = value.astype(BF16)
    return high, (value - high.astype(F32)).astype(BF16)


def dot_bf16(left, right, left_dim):
    return lax.dot_general(
        left, right, (((left_dim,), (0,)), ((), ())), preferred_element_type=F32
    )


def dot_three(left, right, left_dim):
    return (
        dot_bf16(left[0], right[1], left_dim)
        + dot_bf16(left[1], right[0], left_dim)
        + dot_bf16(left[0], right[0], left_dim)
    )


def exact_dot(left, right, left_dim=1, right_dim=0):
    return lax.dot_general(
        left,
        right,
        (((left_dim,), (right_dim,)), ((), ())),
        precision=lax.Precision.HIGHEST,
        preferred_element_type=F32,
    )


def rows_copy(src, dst, send, recv, peer):
    return pltpu.make_async_remote_copy(
        src_ref=src,
        dst_ref=dst,
        send_sem=send,
        recv_sem=recv,
        device_id={"rows": peer},
        device_id_type=MESH,
    )


def pairs_copy(src, dst, send, recv, peer):
    return pltpu.make_async_remote_copy(
        src_ref=src,
        dst_ref=dst,
        send_sem=send,
        recv_sem=recv,
        device_id={"pairs": peer},
        device_id_type=MESH,
    )


def greet(barrier, axis, peer):
    pl.semaphore_signal(barrier, inc=1, device_id={axis: peer}, device_id_type=MESH)


def partners(position, length):
    even = position % 2 == 0
    down = jnp.where(position == 0, 1, position - 2)
    up = jnp.where(position == length - 1, length - 2, position + 2)
    lead = jnp.where(even, down, up)
    down = jnp.where(position == 1, 0, position - 2)
    up = jnp.where(position == length - 2, length - 1, position + 2)
    keep = jnp.where(even, up, down)
    return lead, keep


def add_norms(norms, first, second):
    half = norms.shape[1]
    for row, value in ((0, first), (1, second)):
        sums = jnp.sum(value * value, axis=0, keepdims=True)
        norms[row : row + 1, :] += sums[:, :half]
        norms[row + 2 : row + 3, :] += sums[:, half:]


def pack(count, cross, norms, part):
    block = cross.shape[0]
    share = block // count
    half = block // 2
    for slot in range(count):
        part[slot, :share, :] = cross[slot * share : (slot + 1) * share, :half]
        part[slot, share : 2 * share, :] = cross[slot * share : (slot + 1) * share, half:]
        part[slot, 2 * share :, :] = norms[...]


def unpack(total, cross):
    count, depth, half = total.shape
    share = (depth - 4) // 2
    for slot in range(count):
        cross[slot * share : (slot + 1) * share, :half] = total[slot, :share, :]
        cross[slot * share : (slot + 1) * share, half:] = total[slot, share : 2 * share, :]
    norms = total[0, 2 * share :, :]
    return jnp.concatenate([norms[0:2], norms[2:4]], axis=1)


def scatter_start(count, part, recv, send_sems, recv_sems):
    me = lax.axis_index("rows")
    copies = []
    for far in range(1, count):
        peer = lax.rem(me + far, count)
        copy = rows_copy(part.at[peer], recv.at[far], send_sems.at[far], recv_sems.at[far], peer)
        copy.start()
        copies.append(copy)
    return copies


def scatter_finish(count, part, recv, mine, copies):
    acc = part[lax.axis_index("rows")]
    for far in range(1, count):
        copies[far - 1].wait_recv()
        acc = acc + recv[far]
    mine[...] = acc


def gather_start(count, mine, gathered, send_sems, recv_sems):
    me = lax.axis_index("rows")
    copies = []
    for far in range(1, count):
        peer = lax.rem(me + far, count)
        copy = rows_copy(mine, gathered.at[far], send_sems.at[far], recv_sems.at[far], peer)
        copy.start()
        copies.append(copy)
    return copies


def gather_finish(count, mine, gathered, total, copies):
    me = lax.axis_index("rows")
    total[me] = mine[...]
    for far in range(1, count):
        copies[far - 1].wait_recv()
        total[lax.rem(me + count - far, count)] = gathered[far]


def invert_fixed(gram, inverse, residual, identity):
    block = identity.shape[0]
    largest = 0.25 * block * block
    ratio, trips = largest / (2.0 + largest), 0
    while ratio > 0.01:
        ratio, trips = ratio * ratio / (2.0 - ratio * ratio), trips + 1
    sums = jnp.sum(jnp.abs(gram), axis=1, keepdims=True)
    spread = jnp.max(sums, axis=0, keepdims=True)
    start = 2.0 / (2.0 + spread)
    inverse[...] = start * identity
    residual[...] = (1.0 - start) * identity - start * gram

    def grow(index, ratio):
        square = ratio * ratio
        scale = 2.0 / (2.0 - square)
        power = split(residual[...])
        more = dot_three(split(inverse[...]), power, 1)
        inverse[...] = scale * (inverse[...] + more)
        residual[...] = (1.0 - scale) * identity + scale * dot_three(power, power, 1)
        return square / (2.0 - square)

    lax.fori_loop(0, trips, grow, spread / (2.0 + spread))

    guess = inverse[...]
    error = identity - guess - exact_dot(gram, guess)
    inverse[...] = guess + dot_three(split(guess), split(error), 1)


def identity_of(block):
    row = lax.broadcasted_iota(jnp.int32, (block, block), 0)
    col = lax.broadcasted_iota(jnp.int32, (block, block), 1)
    return jnp.where(row == col, 1.0, 0.0).astype(F32)


def couple(rows_all, norms, cross, identity):
    scales = lax.rsqrt(norms / rows_all + 1e-06)
    scale_first = jnp.sum(identity * scales[0:1, :], axis=1, keepdims=True)
    cross[...] = 0.5 * cross[...] * scale_first * scales[1:2, :] / rows_all


def two_blocks(own, landed, high, low, place):
    return dot_three(split(own), (high[place, 0], low[place, 0]), 1) + dot_three(
        split(landed), (high[place, 1], low[place, 1]), 1
    )


def sweep_kernel(
    rows_all, count, length, matrix, out, lead, keep, lead_land, keep_land, high, low,
    loaded, raw,
    cross, norms, part, recv, mine, gathered, total,
    cross_two, norms_two, part_two, recv_two, mine_two, gathered_two, total_keep,
    passed, gathered_lead, total_lead, raw_piece, gathered_raw, total_raw,
    coupling, inverse, residual, rot_high, rot_low,
    load_sem, lead_send, lead_recv, keep_send, keep_recv, raw_send, raw_recv,
    sum_send, sum_recv, all_send, all_recv, sum_two_send, sum_two_recv, all_two_send, all_two_recv,
    more_send, more_recv, rest_send, rest_recv,
    pass_send, pass_recv, piece_send, piece_recv, totals_send, totals_recv, go_sem,
):
    rows, cols = loaded.shape
    block = cols // 2
    step = rows // SENDS
    group = SENDS // CHUNKS
    me = lax.axis_index("rows")
    position = lax.axis_index("pairs")
    lead_peer, keep_peer = partners(position, length)
    core_peer = position + 1 - 2 * (position % 2)
    near_keep = keep_peer == core_peer
    near_lead = lead_peer == core_peer
    far_keep = jnp.logical_not(near_keep)
    far_lead = jnp.logical_not(near_lead)
    even = position % 2 == 0
    left_leads = jnp.logical_or(position % 2 == 1, position == 0)
    sent = jnp.where(near_lead, SENDS, SENDS - RAW)
    landing = SENDS - RAW
    signals = jnp.logical_and(position > 0, position < length - 1)

    def at(send, sends=1):
        return pl.ds(pl.multiple_of(send * step, step), sends * step)

    def load(chunk):
        where = at(chunk * (SENDS // LOADS), SENDS // LOADS)
        return pltpu.make_async_copy(matrix.at[where], loaded.at[where], load_sem.at[chunk])

    def send_raw(index):
        return pairs_copy(
            loaded.at[at(SENDS - RAW + index)], raw.at[at(index)],
            raw_send.at[index], raw_recv.at[index], lead_peer,
        )

    def send_lead(send):
        return pairs_copy(
            lead.at[at(send)], keep_land.at[at(send)],
            lead_send.at[send], lead_recv.at[send], lead_peer,
        )

    def send_keep(send):
        return pairs_copy(
            keep.at[at(send)], lead_land.at[at(send)],
            keep_send.at[send], keep_recv.at[send], keep_peer,
        )

    def loop(begin, end, do):
        def body(index, carry):
            do(index)
            return carry

        lax.fori_loop(begin, end, body, 0)

    def relay_copies(source, target, send_sems, recv_sems):
        return [
            rows_copy(
                source, target.at[far], send_sems.at[far], recv_sems.at[far],
                lax.rem(me + far, count),
            )
            for far in range(1, count)
        ]

    piece = pairs_copy(mine, raw_piece, piece_send, piece_recv, lead_peer)
    piece_two = pairs_copy(mine_two, passed, pass_send, pass_recv, keep_peer)
    totals = pairs_copy(total_keep, total_lead, totals_send, totals_recv, keep_peer)
    raw_copies = relay_copies(raw_piece, gathered_raw, rest_send, rest_recv)
    lead_copies = relay_copies(passed, gathered_lead, more_send, more_recv)

    def turn(chunk):
        where = at(chunk * group, group)
        turned = dot_three(split(loaded[where, :]), (rot_high[...], rot_low[...]), 1)
        left, right = turned[:, :block], turned[:, block:]
        lead[where, :] = jnp.where(left_leads, left, right)
        keep[where, :] = jnp.where(left_leads, right, left)
        for offset in range(group):
            send = chunk * group + offset

            @pl.when(send < sent)
            def _():
                send_lead(send).start()

            @pl.when(near_keep)
            def _():
                send_keep(send).start()

    def multiply(chunk):
        where = at(chunk * group, group)
        ours, theirs = keep[where, :], keep_land[where, :]
        cross_two[...] += dot_three(split(ours), split(theirs), 0)
        add_norms(norms_two, ours, theirs)

    def take(chunk):
        for offset in range(group):
            send_lead(chunk * group + offset).wait_recv()
        multiply(chunk)

    def hand_over():
        loop(0, sent - 1, lambda send: send_lead(send).wait_send())

        @pl.when(signals)
        def _():
            pl.semaphore_signal(
                go_sem, inc=1, device_id={"pairs": core_peer}, device_id_type=MESH
            )

    def couple_and_invert(sums, flip):
        scales = unpack(sums, coupling)
        identity = identity_of(block)
        couple(rows_all, scales, coupling, identity)
        if flip is not None:
            value = coupling[...]
            coupling[...] = jnp.where(flip, value.T, value)
        value = coupling[...]
        invert_fixed(exact_dot(value, value, 1, 1), inverse, residual, identity)
        return 2.0 * inverse[...] - identity, identity

    def prepare_both():
        straight, identity = couple_and_invert(total, None)
        upper = exact_dot(inverse[...], coupling[...])
        lower = exact_dot(coupling[...], upper, 0)
        parts = (
            (0, 0, straight),
            (0, 1, 2.0 * upper),
            (1, 0, -2.0 * upper.T),
            (1, 1, identity - 2.0 * lower),
        )
        for down, across, value in parts:
            where = (pl.ds(down * block, block), pl.ds(across * block, block))
            rot_high[where], rot_low[where] = split(value)

    def prepare(place, sums, flip, takes_first, own_out):
        straight, identity = couple_and_invert(sums, flip)
        sign = jnp.where(takes_first, -2.0, 2.0)
        crossed = sign * dot_three(split(coupling[...]), split(inverse[...]), 0)
        own = jnp.where(own_out, straight, crossed)
        landed = jnp.where(own_out, crossed, straight)
        high[place, 0], low[place, 0] = split(own)
        high[place, 1], low[place, 1] = split(landed)

    def turn_raw():
        gather_finish(count, raw_piece, gathered_raw, total_raw, raw_copies)
        left = jnp.logical_or(keep_peer % 2 == 1, keep_peer == 0)
        prepare(0, total_raw, jnp.logical_not(left), left, left)
        loop(0, RAW, lambda index: send_raw(index).wait_recv())

        def body(chunk):
            source = at(chunk * group, group)
            keep_land[at(landing + chunk * group, group), :] = dot_three(
                split(raw[source, :block]), (high[0, 0], low[0, 0]), 1
            ) + dot_three(split(raw[source, block:]), (high[0, 1], low[0, 1]), 1)
            multiply(landing // group + chunk)

        loop(0, RAW // group, body)

    def prepare_lead(place):
        prepare(
            place,
            total_lead,
            position == 0,
            jnp.logical_or(even, position == length - 1),
            position == 0,
        )

    def finish(own, landed):
        def body(chunk):
            where = at(chunk * (SENDS // OUTS), SENDS // OUTS)
            out[where, :] = two_blocks(own[where, :], landed[where, :], high, low, 0)

        loop(0, OUTS, body)

    for chunk in range(LOADS):
        load(chunk).start()
    barrier = pltpu.get_barrier_semaphore()
    for far in range(1, count):
        greet(barrier, "rows", lax.rem(me + far, count))
    for peer in (lead_peer, keep_peer, core_peer):
        greet(barrier, "pairs", peer)
    for ref in (cross, norms, cross_two, norms_two):
        ref[...] = jnp.zeros_like(ref)

    def take_first(chunk):
        where = at(chunk * (SENDS // LOADS), SENDS // LOADS)
        load(chunk).wait()
        first, second = loaded[where, :block], loaded[where, block:]
        cross[...] += dot_three(split(first), split(second), 0)
        add_norms(norms, first, second)

    loop(0, LOADS, take_first)
    pl.semaphore_wait(barrier, count + 2)

    @pl.when(far_lead)
    def _():
        loop(0, RAW_FIRST, lambda index: send_raw(index).start())

    pack(count, cross, norms, part)
    sums = scatter_start(count, part, recv, sum_send, sum_recv)
    scatter_finish(count, part, recv, mine, sums)

    @pl.when(far_lead)
    def _():
        piece.start()
        loop(RAW_FIRST, RAW, lambda index: send_raw(index).start())

    alls = gather_start(count, mine, gathered, all_send, all_recv)
    gather_finish(count, mine, gathered, total, alls)

    @pl.when(far_keep)
    def _():
        piece.wait_recv()
        for copy in raw_copies:
            copy.start()

    prepare_both()
    loop(0, CHUNKS, turn)

    @pl.when(far_keep)
    def _():
        turn_raw()

    @pl.when(far_keep)
    def _():
        loop(0, landing // group - 1, take)
        hand_over()
        pl.semaphore_wait(go_sem, 1)
        loop(0, EARLY, lambda send: send_keep(send).start())
        take(landing // group - 1)

    @pl.when(near_keep)
    def _():
        loop(0, CHUNKS, take)

    pack(count, cross_two, norms_two, part_two)
    sums_two = scatter_start(count, part_two, recv_two, sum_two_send, sum_two_recv)

    @pl.when(near_keep)
    def _():
        hand_over()

    scatter_finish(count, part_two, recv_two, mine_two, sums_two)

    @pl.when(far_keep)
    def _():
        piece_two.start()

    alls_two = gather_start(count, mine_two, gathered_two, all_two_send, all_two_recv)

    @pl.when(far_keep)
    def _():
        loop(EARLY, SENDS, lambda send: send_keep(send).start())

    @pl.when(near_lead)
    def _():
        totals.wait_recv()
        prepare_lead(0)
        loop(0, SENDS, lambda send: send_keep(send).wait_recv())
        finish(lead, lead_land)

    gather_finish(count, mine_two, gathered_two, total_keep, alls_two)

    @pl.when(near_keep)
    def _():
        totals.start()

    @pl.when(far_lead)
    def _():
        piece_two.wait_recv()
        for copy in lead_copies:
            copy.start()

    prepare(
        jnp.where(near_lead, 1, 0),
        total_keep,
        position != 1,
        jnp.logical_and(jnp.logical_not(even), position != 1),
        position == 1,
    )

    @pl.when(far_lead)
    def _():
        gather_finish(count, passed, gathered_lead, total_lead, lead_copies)
        prepare_lead(1)
        finish(keep, keep_land)
        loop(0, SENDS, lambda send: send_keep(send).wait_recv())
        for copy in lead_copies:
            copy.wait_send()

    send_lead(sent - 1).wait_send()
    for copy in sums + alls + sums_two + alls_two:
        copy.wait_send()

    @pl.when(near_keep)
    def _():
        totals.wait_send()

    @pl.when(far_keep)
    def _():
        piece_two.wait_send()


    @pl.when(far_keep)
    def _():
        for copy in raw_copies:
            copy.wait_send()

    @pl.when(far_lead)
    def _():
        piece.wait_send()
        loop(0, RAW, lambda index: send_raw(index).wait_send())

    loop(0, SENDS, lambda send: send_keep(send).wait_send())


def sweep(matrix):
    rows, cols = matrix.shape
    block = cols // 2
    count = lax.axis_size("rows")
    length = lax.axis_size("pairs")
    shape = (2 * (block // count) + 4, block // 2)
    slot, slots = pltpu.VMEM(shape, F32), pltpu.VMEM((count,) + shape, F32)
    square = pltpu.VMEM((block, block), F32)
    sums = [square, pltpu.VMEM((4, block // 2), F32), slots, slots, slot, slots, slots]
    vmem = pl.BlockSpec(memory_space=pltpu.VMEM)
    return pl.pallas_call(
        functools.partial(sweep_kernel, rows * count, count, length),
        out_shape=[jax.ShapeDtypeStruct((rows, block), F32)] * 5
        + [jax.ShapeDtypeStruct((2, 2, block, block), BF16)] * 2,
        in_specs=[pl.BlockSpec(memory_space=pltpu.HBM)],
        out_specs=[vmem] * 7,
        scratch_shapes=[pltpu.VMEM((rows, cols), F32)]
        + [pltpu.VMEM((RAW * (rows // SENDS), cols), F32)]
        + sums * 2
        + [slot, slots, slots] * 2
        + [square] * 3
        + [pltpu.VMEM((cols, cols), BF16)] * 2
        + [DMA((LOADS,))]
        + [DMA((SENDS,))] * 4
        + [DMA((RAW,))] * 2
        + [DMA((count,))] * 12
        + [DMA(())] * 6
        + [pltpu.SemaphoreType.REGULAR],
        name="sweep",
        compiler_params=pltpu.CompilerParams(
            collective_id=0, has_side_effects=True, vmem_limit_bytes=24 * 2**20
        ),
    )(pltpu.with_memory_space_constraint(matrix, pltpu.HBM))


def final_kernel(length, done, lead, keep, lead_land, keep_land, high, low, out, staged, sems):
    rows, block = lead.shape
    step = rows // OUTS
    position = lax.axis_index("pairs")
    near_lead = jnp.logical_or(position == 0, position == length - 1)
    even = position % 2 == 0

    def store(chunk, source, takes_lead, sem):
        column = jnp.where(takes_lead == even, 0, block)
        where = pl.ds(pl.multiple_of(chunk * step, step), step)
        return pltpu.make_async_copy(
            source.at[where],
            out.at[where, pl.ds(pl.multiple_of(column, block), block)],
            sems.at[sem, chunk],
        )

    def loop(do):
        def body(chunk, carry):
            do(chunk)
            return carry

        lax.fori_loop(0, OUTS, body, 0)

    loop(lambda chunk: store(chunk, done, near_lead, 0).start())

    def finish(own, landed):
        def body(chunk):
            where = pl.ds(pl.multiple_of(chunk * step, step), step)
            staged[where, :] = two_blocks(own[where, :], landed[where, :], high, low, 1)
            store(chunk, staged, jnp.logical_not(near_lead), 1).start()

        loop(body)

    @pl.when(near_lead)
    def _():
        finish(keep, keep_land)

    @pl.when(jnp.logical_not(near_lead))
    def _():
        finish(lead, lead_land)

    def drain(chunk):
        store(chunk, done, near_lead, 0).wait()
        store(chunk, staged, near_lead, 1).wait()

    loop(drain)


def final(done, *blocks):
    rows, block = done.shape
    return pl.pallas_call(
        functools.partial(final_kernel, lax.axis_size("pairs")),
        out_shape=jax.ShapeDtypeStruct((rows, 2 * block), F32),
        in_specs=[pl.BlockSpec(memory_space=pltpu.VMEM)] * 7,
        out_specs=pl.BlockSpec(memory_space=pl.ANY),
        scratch_shapes=[pltpu.VMEM((rows, block), F32), DMA((2, OUTS))],
        name="final",
        compiler_params=pltpu.CompilerParams(vmem_limit_bytes=16 * 2**20),
    )(done, *blocks)


def shards(matrix):
    return final(*sweep(matrix))


def solution(mesh):
    return jax.shard_map(
        shards,
        mesh=mesh,
        in_specs=(P("rows", "pairs"),),
        out_specs=P("rows", "pairs"),
        check_vma=False,
    )
```
